512 devices in a mesh: dp: 32 (over x, z), patch: 16 (over y, core).
Axes of the slice: x: 4, y: 8, z: 8, core: 2. Of those that a mesh axis runs over, the one named last changes fastest.
Arguments:
- query_rows: bfloat16 [32, 2048, 576], P('dp', 'patch'), may hold values from -6 to 6
- key_rows: bfloat16 [32, 2048, 576], P('dp', 'patch'), may hold values from -6 to 6
- value_rows: bfloat16 [32, 2048, 576], P('dp', 'patch'), may hold values from -6 to 6
- out_weight: bfloat16 [576, 1152], replicated, may hold values from -0.25 to 0.25
- target: bfloat16 [32, 2048, 1152], P('dp', 'patch'), may hold values from -6 to 6
- lengths: int32 [32], P('dp'), may hold values from 256 to 2048
- segments: int32 [32, 2048], P('dp', 'patch'), may hold values from 0 to 7, never falling along the last dimension, each value on 1 to 1024 neighbouring positions
Outputs:
- query_grad: float32 [32, 2048, 576], P('dp', 'patch')
- key_grad: float32 [32, 2048, 576], P('dp', 'patch')
- value_grad: float32 [32, 2048, 576], P('dp', 'patch')
- weight_grad: float32 [576, 1152], P('patch', 'dp')
- loss: float32 [], replicated
The draws below stay inside these ranges and needn't reach their ends.
All inputs are finite; a program needn't handle non-finite values.
Results may differ from the reference program's by a relative error of at most 0.024.
Values may be sent and summed in bfloat16 or wider, within the bound.
A program may use at most 64 MiB of HBM per device.

```python
import math
import jax
import jax.numpy as jnp
import numpy as np
from jax import lax

WIDTH = 1152
HEADS = 8
HEAD_DIM = 72
TOK_DEV = 128
FEAT = 576
SEQ = 2048
SAMPLES = 32


def draw_rows(key, salt, chosen_rows):
    fresh_key = jax.random.fold_in(key, salt)
    sampled = jnp.clip(1.5 * jax.random.normal(fresh_key, (SAMPLES, SEQ, FEAT), jnp.float32), -6.0, 6.0)
    return sampled.astype(jnp.bfloat16)


def draw_query_rows(key, part):
    positions = jnp.arange(SEQ)
    return draw_rows(key, 1, positions % TOK_DEV == 0)


def draw_key_rows(key, part):
    positions = jnp.arange(SEQ)
    return draw_rows(key, 2, positions % TOK_DEV == 0)


def plant(entries, key, low, largest):
    longest = entries.shape.index(max(entries.shape))
    spots = []
    for shift in (0, 1):
        where = [jax.random.randint(jax.random.fold_in(key, axis), (), 0, length) for axis, length in enumerate(entries.shape)]
        where[longest] = (where[longest] + shift) % entries.shape[longest]
        spots.append(tuple(where))
    return entries.at[spots[0]].set(low).at[spots[1]].set(largest)


def steps_of(stream_key, extent, split, least, largest):
    level = 1.0
    for position, shards_of in split:
        heights = jax.random.uniform(jax.random.fold_in(jax.random.fold_in(stream_key, 6), position), (shards_of,), jnp.float32, least / len(split), largest / len(split))
        level = level * jnp.repeat(jnp.exp(heights), extent[position] // shards_of).reshape((-1,) + (1,) * (len(extent) - 1 - position))
    return level


def profile(count, total, most, skew):
    weights = [(1 << 20) // math.isqrt(rank ** skew) + 1 for rank in range(2, count + 1)]
    surplus, counts = total - most - (count - 1), [1] * (count - 1)
    while surplus > 0:
        candidates = [i for i in range(count - 1) if counts[i] < most]
        pool, remaining = sum([weights[i] for i in candidates]), surplus
        for i in candidates:
            more = min(most - counts[i], max(1, remaining * weights[i] // pool), surplus)
            counts[i] = counts[i] + more
            surplus = surplus - more
    return np.array([most] + counts)


def uneven_parts(key, number_of, total, most, skew):
    if number_of == 2:
        one = jax.random.randint(key, (), max(1, total - most), min(most, total - 1) + 1)
        return jnp.stack([one, total - one])
    tallies = jnp.asarray(profile(number_of, total, most, skew), jnp.int32)
    pairs = (number_of - 1) // 2
    donor, sink = tallies[1:1 + 2 * pairs:2], tallies[2:2 + 2 * pairs:2]
    slack = jnp.minimum(donor - 1, most - sink)
    shifted = jax.random.randint(jax.random.fold_in(key, 1), (pairs,), 0, 1 << 20) % (slack + 1)
    tallies = tallies.at[1:1 + 2 * pairs:2].set(donor - shifted).at[2:2 + 2 * pairs:2].set(sink + shifted)
    return tallies[jax.random.permutation(jax.random.fold_in(key, 2), number_of)]


def normal_values(rng, shape, spread, most, split=(), kind=jnp.bfloat16):
    array = spread * jax.random.normal(rng, shape, jnp.float32)
    if split:
        array = array * steps_of(rng, shape, split, -0.22, 0.18)
    return jnp.clip(array, -most, most).astype(kind)


def setup_inputs(seed: int = 0) -> dict:
    arg_keys = jax.random.split(jax.random.key(seed), 8)
    query_rows = draw_query_rows(jax.random.fold_in(arg_keys[7], 71), 0)
    key_rows = draw_key_rows(jax.random.fold_in(arg_keys[7], 71), 0)
    value_rows = normal_values(arg_keys[2], (SAMPLES, SEQ, FEAT), 1.0, 6.0, ((0, 32), (1, 16)))
    out_weight = normal_values(arg_keys[3], (FEAT, WIDTH), FEAT ** -0.5, 0.25)
    target = normal_values(arg_keys[4], (SAMPLES, SEQ, WIDTH), 1.0, 6.0, ((0, 32), (1, 16)))
    lengths = plant(jax.random.randint(arg_keys[5], (SAMPLES,), SEQ // 8, SEQ + 1), jax.random.fold_in(arg_keys[5], 1), SEQ // 8, SEQ).astype(jnp.int32)
    segments = jax.vmap(lambda own: jnp.searchsorted(jnp.cumsum(uneven_parts(own, 8, SEQ, SEQ // 2, 2)), jnp.arange(SEQ), side="right"))(jax.random.split(arg_keys[6], SAMPLES)).reshape((SAMPLES, SEQ)).astype(jnp.int32)
    return {"query_rows": query_rows, "key_rows": key_rows, "value_rows": value_rows, "out_weight": out_weight, "target": target, "lengths": lengths, "segments": segments}


NEG_LARGE = -1e+30

def widen(value):
    return lax.optimization_barrier(value).astype(jnp.float32)

def one_sample(packed, out_weight):
    query_rows, key_rows, value_rows, target_rows, length, segment_row = packed
    score_scale = 1.0 / math.sqrt(HEAD_DIM)
    query_heads = query_rows.astype(jnp.float32).reshape(SEQ, HEADS, HEAD_DIM)
    key_heads = key_rows.astype(jnp.float32).reshape(SEQ, HEADS, HEAD_DIM)
    value_heads = value_rows.astype(jnp.float32).reshape(SEQ, HEADS, HEAD_DIM)
    live = lax.iota(jnp.int32, SEQ) < length
    group = jnp.where(live, segment_row, -1)
    allowed = (group[:, None] == group[None, :])[None, :, :]
    scores = jnp.einsum('qhe,khe->hqk', query_heads, key_heads) * score_scale
    masked = jnp.where(allowed, scores, NEG_LARGE)
    row_max = lax.optimization_barrier(jnp.max(masked, axis=2))
    probs = jnp.where(allowed, jnp.exp(masked - row_max[:, :, None]), 0.0)
    denom = lax.optimization_barrier(jnp.sum(probs, axis=2))
    weights = widen(probs.astype(jnp.bfloat16))
    accum = jnp.einsum('hqk,khe->qhe', weights, value_heads)
    attn = (accum / denom.T[:, :, None]).reshape(SEQ, FEAT).astype(jnp.bfloat16)
    log_norm = row_max + jnp.log(denom)
    output = jnp.dot(attn, out_weight, preferred_element_type=jnp.float32)
    error = jnp.where(live[:, None], output - target_rows.astype(jnp.float32), 0.0)
    grad_out = (2.0 * error).astype(jnp.bfloat16)
    attn_wide = widen(attn)
    grad_wide = widen(grad_out)
    weight_part = jnp.einsum('tf,td->fd', attn_wide, grad_wide)
    grad_attn = jnp.einsum('td,fd->tf', grad_wide, out_weight.astype(jnp.float32)).astype(jnp.bfloat16)
    grad_attn_wide = widen(grad_attn)
    delta = lax.optimization_barrier(jnp.sum((grad_attn_wide * attn_wide).reshape(SEQ, HEADS, HEAD_DIM), axis=2)).T
    back_probs = jnp.where(allowed, jnp.exp(masked - log_norm[:, :, None]), 0.0)
    grad_heads = grad_attn_wide.reshape(SEQ, HEADS, HEAD_DIM)
    dprobs = jnp.einsum('qhe,khe->hqk', grad_heads, value_heads)
    dscores = widen((back_probs * (dprobs - delta[:, :, None])).astype(jnp.bfloat16))
    query_raw = jnp.einsum('hqk,khe->qhe', dscores, key_heads) * score_scale
    key_raw = jnp.einsum('hqk,qhe->khe', dscores, query_heads) * score_scale
    back_weights = widen(back_probs.astype(jnp.bfloat16))
    value_raw = jnp.einsum('hqk,qhe->khe', back_weights, grad_heads)
    return (query_raw.reshape(SEQ, FEAT), key_raw.reshape(SEQ, FEAT), value_raw.reshape(SEQ, FEAT), weight_part, jnp.sum(error * error))

def reference(query_rows, key_rows, value_rows, out_weight, target, lengths, segments):

    def per_sample(packed):
        return one_sample(packed, out_weight)
    results = lax.map(per_sample, (query_rows, key_rows, value_rows, target, lengths, segments))
    count = jnp.sum(lengths).astype(jnp.float32)
    ratio = jnp.float32(SAMPLES * SEQ) / count
    query_grad = ratio * results[0]
    key_grad = ratio * results[1]
    value_grad = ratio * results[2]
    weight_grad = lax.optimization_barrier(jnp.sum(results[3], axis=0)) * (ratio / SEQ)
    loss = jnp.sum(results[4]) / (count * WIDTH)
    return (query_grad, key_grad, value_grad, weight_grad, loss)
```

```python
import functools
import math

import jax
import jax.numpy as jnp
from jax import lax
from jax.experimental import pallas as pl
from jax.experimental.pallas import tpu as pltpu
from jax.sharding import Mesh
from jax.sharding import PartitionSpec as P

WIDTH = 1152
HEADS = 8
HEAD_DIM = 72
FEAT = 576
ROWS = 128
PAD = 80
PATCH = ("patch_0", "patch_1")
DP = ("dp_0", "dp_1")
BF = jnp.bfloat16
F32 = jnp.float32
FAR = (4, 3, 5, 2, 6, 1, 7)
MASK = 2.0**50


def dot(a, b, ca, cb):
    return lax.dot_general(a, b, (((ca,), (cb,)), ((), ())), preferred_element_type=F32)


def body(
    nx,
    nz,
    q_ref,
    k_ref,
    v_ref,
    seg_ref,
    len_ref,
    w_hbm,
    t_hbm,
    dq_out,
    dk_out,
    dv_out,
    wg_out,
    st_out,
    w_s,
    t_s,
    send1,
    recv1,
    ktok,
    vtok,
    qtok,
    dtok,
    p_s,
    ds_s,
    rinv_s,
    send2,
    recv2,
    at_s,
    send3,
    recv3,
    dof_s,
    dkv,
    drecv,
    send4,
    recv4,
    g_s,
    pg_s,
    pa_s,
    xsend,
    xrecv,
    zsend,
    zrecv,
    ysend,
    yrecv,
    stat_s,
    load_sem,
    s1,
    r1,
    d1s,
    d1r,
    s2,
    r2,
    s3,
    r3,
    dks,
    dkr,
    s4,
    r4,
    gs,
    gr,
    xs,
    xr,
    zs,
    zr,
    ys,
    yr,
    sts,
    strr,
):
    x = lax.axis_index("dp_0")
    z = lax.axis_index("dp_1")
    y = lax.axis_index("patch_0")
    k = lax.axis_index("patch_1")
    other = 1 - k
    p = 2 * y + k
    zh = nz // 2
    scale = 1.0 / math.sqrt(HEAD_DIM)

    load_w = pltpu.make_async_copy(w_hbm, w_s, load_sem.at[0])
    load_t = pltpu.make_async_copy(t_hbm, t_s, load_sem.at[1])
    load_w.start()
    load_t.start()

    barrier = pltpu.get_barrier_semaphore()
    for i in range(1, 8):
        peer = lax.rem(y + i, 8)
        pl.semaphore_signal(barrier, inc=1, device_id={"patch_0": peer})
        pl.semaphore_signal(barrier, inc=1, device_id={"patch_0": peer, "patch_1": other})
    pl.semaphore_signal(barrier, inc=1, device_id={"patch_1": other})
    for i in range(1, nx):
        pl.semaphore_signal(barrier, inc=1, device_id={"dp_0": lax.rem(x + i, nx)})
    for i in range(1, nz):
        pl.semaphore_signal(barrier, inc=1, device_id={"dp_1": lax.rem(z + i, nz)})

    def remote(src, dst, ssem, rsem, **where):
        return pltpu.make_async_remote_copy(
            src_ref=src, dst_ref=dst, send_sem=ssem, recv_sem=rsem, device_id=where
        )

    row = lax.broadcasted_iota(jnp.int32, (8, ROWS), 0)
    lane = lax.broadcasted_iota(jnp.int32, (8, ROWS), 1)
    length = len_ref[0]
    live_t = p * ROWS + lane < length
    code = jnp.where(live_t, jnp.broadcast_to(seg_ref[...], (8, ROWS)), 8)
    low = jnp.bitwise_and(row, 3)
    weight = jnp.where(low == 0, 1, jnp.where(low == 1, 2, jnp.where(low == 2, 4, 8)))
    bit = jnp.where(jnp.bitwise_and(code, weight) != 0, 1.0, 0.0).astype(F32)
    mine = jnp.where(row < 4, bit, 1.0 - bit)
    q_mask = -MASK * mine
    k_mask = MASK * (1.0 - mine)
    v_ones = jnp.where(row == 0, 1.0, 0.0).astype(F32)
    for at, (ref, extra) in enumerate(((q_ref, q_mask), (k_ref, k_mask), (v_ref, v_ones))):
        whole = ref[0].astype(F32).T
        for h in range(HEADS):
            block = jnp.concatenate([whole[HEAD_DIM * h : HEAD_DIM * (h + 1)], extra], axis=0)
            send1[h, PAD * at : PAD * (at + 1), :] = block.astype(BF)
    recv1[p] = send1[y]

    pl.semaphore_wait(barrier, 15 + (nx - 1) + (nz - 1))

    first = [None] * 8
    for i in FAR:
        h = lax.rem(y + i, 8)
        first[i] = remote(send1.at[h], recv1.at[p], s1.at[i], r1.at[i], patch_0=h)
        first[i].start()
    kv = pl.ds(PAD, 2 * PAD)

    def pass_on(i):
        b = 2 * lax.rem(y - i + 8, 8) + k
        return remote(
            recv1.at[b, kv], recv1.at[b, kv], d1s.at[i], d1r.at[i], patch_1=other
        )

    def prepare(b):
        at = pl.ds(pl.multiple_of(b * ROWS, ROWS), ROWS)
        both = recv1[b, PAD : 3 * PAD, :].astype(F32)
        ktok[at, :] = both[:PAD].T.astype(BF)
        vtok[at, :] = both[PAD:].T.astype(BF)

    def prepare_q(src):
        at = pl.ds(pl.multiple_of(src * ROWS, ROWS), ROWS)
        qtok[at, :] = recv1[2 * src + k, 0:PAD, :].astype(F32).T.astype(BF)

    passed = [pass_on(i) for i in range(8)]
    passed[0].start()
    prepare(p)
    prepare_q(y)
    for i in (1, 7, 2, 6, 3, 5, 4):
        first[i].wait_recv()
        passed[i].start()
        src = lax.rem(y - i + 8, 8)
        prepare(2 * src + k)
        prepare_q(src)
    for i in (0, 1, 7, 2, 6, 3, 5, 4):
        passed[i].wait_recv()
        prepare(2 * lax.rem(y - i + 8, 8) + other)

    factor = scale * math.log2(math.e)

    def queries(j, part):
        return jnp.concatenate(
            [recv1[4 * j + k, part, :], recv1[4 * j + 2 + k, part, :]], axis=1
        )

    def forward(j, carry):
        scores = dot(ktok[...], queries(j, slice(0, PAD)), 1, 0)
        top = jnp.max(scores, axis=0, keepdims=True)
        probs = jnp.exp2((scores - top) * factor).astype(BF)
        p_s[j] = probs
        values = jnp.concatenate([recv1[b, 2 * PAD : 3 * PAD, :] for b in range(16)], axis=1)
        accum = dot(values, probs, 1, 0)
        rinv = 1.0 / accum[HEAD_DIM : HEAD_DIM + 1, :]
        rinv_s[j] = jnp.broadcast_to(rinv, (8, 2 * ROWS))
        attn = (accum * rinv).astype(BF)
        send2[2 * j] = attn[:, :ROWS]
        send2[2 * j + 1] = attn[:, ROWS:]
        return carry

    lax.fori_loop(0, 4, forward, 0)
    second = [None] * 8
    for i in FAR:
        to = lax.rem(y + i, 8)
        second[i] = remote(send2.at[to], recv2.at[y], s2.at[i], r2.at[i], patch_0=to)
        second[i].start()
    recv2[y] = send2[y]

    load_w.wait()
    load_t.wait()
    for i in (1, 7, 2, 6, 3, 5, 4):
        second[i].wait_recv()
    for h in range(HEADS):
        at_s[HEAD_DIM * h : HEAD_DIM * (h + 1), :] = recv2[h].astype(F32)[:HEAD_DIM]
    attn_t = at_s[...].astype(BF)
    pa_s[0] = attn_t
    output = dot(attn_t, w_s[...], 0, 0)
    token = lax.broadcasted_iota(jnp.int32, (ROWS, WIDTH), 0)
    live = p * ROWS + token < length
    error = jnp.where(live, output - t_s[0].astype(F32), 0.0)
    grad_out = (2.0 * error).astype(BF)
    grad_attn = dot(w_s[...], grad_out, 1, 1)
    for h in range(HEADS):
        block = jnp.concatenate(
            [grad_attn[HEAD_DIM * h : HEAD_DIM * (h + 1)], jnp.zeros((8, ROWS), F32)], axis=0
        )
        send3[h] = block.astype(BF)
    third = [None] * 8
    for i in FAR:
        to = lax.rem(y + i, 8)
        third[i] = remote(send3.at[to], recv3.at[y], s3.at[i], r3.at[i], patch_0=to)
        third[i].start()
    recv3[y] = send3[y]

    grad_t = (2.0 * error).T.astype(BF)
    part = WIDTH // (2 * nx)
    for half in range(2):
        for xx in range(nx):
            at = (2 * xx + half) * part
            g_s[half, part * xx : part * (xx + 1), :] = grad_t[at : at + part]
    swap = [
        remote(g_s.at[other], pg_s, gs.at[0], gr.at[0], patch_1=other),
        remote(pa_s.at[0], pa_s.at[1], gs.at[1], gr.at[1], patch_1=other),
    ]
    for c in swap:
        c.start()
    squares = jnp.sum(error * error)
    cell = lax.broadcasted_iota(jnp.int32, (8, ROWS), 1)
    stat_s[0] = jnp.where(
        cell == 0, squares, jnp.where(cell == 1, length.astype(F32), 0.0)
    )

    def stat_copies(stage, base, n, me, to):
        return [
            remote(
                stat_s.at[stage],
                stat_s.at[base + i],
                sts.at[base + i],
                strr.at[base + i],
                **to(lax.rem(me + i, n)),
            )
            for i in range(1, n)
        ]

    stat_y = stat_copies(0, 3, 16, p, lambda t: {"patch_0": t // 2, "patch_1": lax.rem(t, 2)})
    for c in stat_y:
        c.start()
    for c in swap:
        c.wait_recv()
    left = jnp.concatenate([g_s[k], pg_s[...]], axis=1)
    right = jnp.concatenate([pa_s[0], pa_s[1]], axis=1)
    partial = dot(left, right, 1, 1)
    for xx in range(nx):
        xsend[xx] = partial[part * xx : part * (xx + 1)].astype(BF)
    xcopies = [None] * nx
    for i in range(1, nx):
        to = lax.rem(x + i, nx)
        xcopies[i] = remote(xsend.at[to], xrecv.at[i], xs.at[i], xr.at[i], dp_0=to)
        xcopies[i].start()

    for i in (1, 7, 2, 6, 3, 5, 4):
        third[i].wait_recv()

    def fold(s, carry):
        rinv = rinv_s[s // 2, 0:1, pl.ds(pl.multiple_of(lax.rem(s, 2) * ROWS, ROWS), ROWS)]
        folded = recv3[s].astype(F32) * rinv
        dof_s[s] = folded.astype(BF)
        dtok[pl.ds(pl.multiple_of(s * ROWS, ROWS), ROWS), :] = folded.T.astype(BF)
        return carry

    lax.fori_loop(0, 8, fold, 0)

    def backward(j, carry):
        grads = jnp.concatenate([dof_s[2 * j], dof_s[2 * j + 1]], axis=1)
        attn = jnp.concatenate([send2[2 * j], send2[2 * j + 1]], axis=1)
        delta = jnp.sum(grads.astype(F32) * attn.astype(F32), axis=0, keepdims=True)
        dprobs = dot(vtok[...], grads, 1, 0)
        dscores = (p_s[j].astype(F32) * (dprobs - delta)).astype(BF)
        ds_s[j] = dscores
        keys = jnp.concatenate([recv1[b, PAD : 2 * PAD, :] for b in range(16)], axis=1)
        dq = (dot(keys, dscores, 1, 0) * scale).astype(BF)
        send4[2 * j, 0:PAD, :] = dq[:, :ROWS]
        send4[2 * j + 1, 0:PAD, :] = dq[:, ROWS:]
        return carry

    lax.fori_loop(0, 4, backward, 0)

    def keyside(t, carry):
        at = pl.ds(pl.multiple_of(t * 2 * ROWS, 2 * ROWS), 2 * ROWS)
        ds_rows = jnp.concatenate([ds_s[j, at, :] for j in range(4)], axis=1)
        p_rows = jnp.concatenate([p_s[j, at, :] for j in range(4)], axis=1)
        dk = (dot(ds_rows, qtok[...], 1, 0) * scale).T.astype(BF)
        dv = dot(p_rows, dtok[...], 1, 0).T.astype(BF)
        for c in range(2):
            dkv[c, t, 0:PAD, :] = dk[:, ROWS * c : ROWS * (c + 1)]
            dkv[c, t, PAD : 2 * PAD, :] = dv[:, ROWS * c : ROWS * (c + 1)]
        return carry

    lax.fori_loop(0, 8, keyside, 0)
    cross = remote(dkv.at[other], drecv, dks.at[0], dkr.at[0], patch_1=other)
    cross.start()

    for i in range(1, nx):
        xcopies[i].wait_recv()
    total = partial[0:part] * 0.0
    total = xsend[x].astype(F32)
    for i in range(1, nx):
        total = total + xrecv[i].astype(F32)
    cols = part // zh
    for j in range(zh):
        zsend[j, 0:cols, :] = total[cols * j : cols * (j + 1)].astype(BF)
    zcopies = [None] * zh
    for j in range(zh):
        to = zh * k + j
        away = lax.rem(to - z + nz, nz)
        zcopies[j] = remote(zsend.at[j], zrecv.at[away], zs.at[j], zr.at[away], dp_1=to)

        @pl.when(to != z)
        def _():
            zcopies[j].start()

    active = z // zh == k

    @pl.when(active)
    def _():
        zrecv[0] = zsend[lax.rem(z, zh)]

    for i in range(15):
        stat_y[i].wait_recv()
    acc = stat_s[0]
    for i in range(1, 16):
        acc = acc + stat_s[3 + i]
    stat_s[1] = acc
    stat_x = stat_copies(1, 19, nx, x, lambda t: {"dp_0": t})
    for c in stat_x:
        c.start()

    cross.wait_recv()

    def join(s, carry):
        send4[s, PAD : 3 * PAD, :] = (
            dkv[k, s].astype(F32) + drecv[s].astype(F32)
        ).astype(BF)
        return carry

    lax.fori_loop(0, 8, join, 0)
    fourth = [None] * 8
    for i in FAR:
        to = lax.rem(y + i, 8)
        fourth[i] = remote(send4.at[to], recv4.at[y], s4.at[i], r4.at[i], patch_0=to)
        fourth[i].start()
    recv4[y] = send4[y]

    for c in stat_x:
        c.wait_recv()
    acc = stat_s[1]
    for i in range(1, nx):
        acc = acc + stat_s[19 + i]
    stat_s[2] = acc
    stat_z = stat_copies(2, 19 + nx, nz, z, lambda t: {"dp_1": t})
    for c in stat_z:
        c.start()

    def z_in(i):
        return remote(zsend.at[0], zrecv.at[i], zs.at[0], zr.at[i], dp_1=z)

    @pl.when(active)
    def _():
        for i in range(1, nz):
            z_in(i).wait_recv()
        summed = zrecv[0].astype(F32)
        for i in range(1, nz):
            summed = summed + zrecv[i].astype(F32)
        for t in range(16):
            ysend[t, 0:cols, 0:36] = summed[0:cols, 36 * t : 36 * (t + 1)]

    def y_out(t):
        return remote(
            ysend.at[t], yrecv.at[y], ys.at[t], yr.at[y], patch_0=t // 2, patch_1=t % 2
        )

    for t in range(16):

        @pl.when(active & (p != t))
        def _():
            y_out(t).start()

    @pl.when(active)
    def _():
        yrecv[y] = ysend[p]

    for c in stat_z:
        c.wait_recv()
    acc = stat_s[2]
    for i in range(1, nz):
        acc = acc + stat_s[19 + nx + i]
    st_out[...] = acc

    for i in (1, 7, 2, 6, 3, 5, 4):
        fourth[i].wait_recv()
    for at, out in enumerate((dq_out, dk_out, dv_out)):
        whole = jnp.concatenate(
            [
                recv4[h, PAD * at : PAD * (at + 1), :].astype(F32)[:HEAD_DIM]
                for h in range(HEADS)
            ],
            axis=0,
        )
        out[...] = whole.T

    for i in range(8):
        here = active & (y == i)

        @pl.when(jnp.logical_not(here))
        def _():
            remote(
                ysend.at[0], yrecv.at[i], ys.at[0], yr.at[i], patch_0=y, patch_1=k
            ).wait_recv()

    final = yrecv[0]
    for i in range(1, 8):
        final = final + yrecv[i]
    wg_out[...] = final

    for group in (first, second, third, fourth, xcopies):
        for c in group[1:]:
            c.wait_send()
    for c in passed + swap + [cross] + stat_y + stat_x + stat_z:
        c.wait_send()
    for j in range(zh):

        @pl.when(zh * k + j != z)
        def _():
            zcopies[j].wait_send()

    for t in range(16):

        @pl.when(active & (p != t))
        def _():
            y_out(t).wait_send()


def step(nx, nz, query_rows, key_rows, value_rows, out_weight, target, lengths, segments):
    part = WIDTH // (2 * nx)
    zh = nz // 2
    dma = pltpu.SemaphoreType.DMA
    scratch = [
        pltpu.VMEM((FEAT, WIDTH), BF),
        pltpu.VMEM((1, ROWS, WIDTH), BF),
        pltpu.VMEM((8, 3 * PAD, ROWS), BF),
        pltpu.VMEM((16, 3 * PAD, ROWS), BF),
        pltpu.VMEM((2048, PAD), BF),
        pltpu.VMEM((2048, PAD), BF),
        pltpu.VMEM((1024, PAD), BF),
        pltpu.VMEM((1024, PAD), BF),
        pltpu.VMEM((4, 2048, 256), BF),
        pltpu.VMEM((4, 2048, 256), BF),
        pltpu.VMEM((4, 8, 256), F32),
        pltpu.VMEM((8, PAD, ROWS), BF),
        pltpu.VMEM((8, PAD, ROWS), BF),
        pltpu.VMEM((FEAT, ROWS), F32),
        pltpu.VMEM((8, PAD, ROWS), BF),
        pltpu.VMEM((8, PAD, ROWS), BF),
        pltpu.VMEM((8, PAD, ROWS), BF),
        pltpu.VMEM((2, 8, 2 * PAD, ROWS), BF),
        pltpu.VMEM((8, 2 * PAD, ROWS), BF),
        pltpu.VMEM((8, 3 * PAD, ROWS), BF),
        pltpu.VMEM((8, 3 * PAD, ROWS), BF),
        pltpu.VMEM((2, FEAT, ROWS), BF),
        pltpu.VMEM((FEAT, ROWS), BF),
        pltpu.VMEM((2, FEAT, ROWS), BF),
        pltpu.VMEM((nx, part, FEAT), BF),
        pltpu.VMEM((nx, part, FEAT), BF),
        pltpu.VMEM((zh, 48, FEAT), BF),
        pltpu.VMEM((nz, 48, FEAT), BF),
        pltpu.VMEM((16, 40, 128), F32),
        pltpu.VMEM((8, 40, 128), F32),
        pltpu.VMEM((19 + nx + nz, 8, ROWS), F32),
    ]
    sems = [2, 8, 8, 8, 8, 8, 8, 8, 8, 1, 1, 8, 8, 2, 2, nx, nx, zh, nz, 16, 8]
    sems += [19 + nx + nz] * 2
    vmem = pl.BlockSpec(memory_space=pltpu.VMEM)
    hbm = pl.BlockSpec(memory_space=pl.ANY)
    wide = jax.ShapeDtypeStruct((ROWS, FEAT), F32)
    dq, dk, dv, wg, st = pl.pallas_call(
        functools.partial(body, nx, nz),
        out_shape=(
            wide,
            wide,
            wide,
            jax.ShapeDtypeStruct((40, 128), F32),
            jax.ShapeDtypeStruct((8, ROWS), F32),
        ),
        in_specs=[vmem] * 4 + [pl.BlockSpec(memory_space=pltpu.SMEM), hbm, hbm],
        out_specs=(vmem,) * 5,
        scratch_shapes=scratch + [dma((n,)) for n in sems],
        compiler_params=pltpu.CompilerParams(
            collective_id=0, has_side_effects=True, vmem_limit_bytes=60 * 1024 * 1024
        ),
    )(query_rows, key_rows, value_rows, segments, lengths, out_weight, target)
    slots = 16 * ROWS
    count = st[0, 1] / 16.0
    ratio = jnp.float32(nx * nz * slots) / count
    return (
        (ratio * dq)[None],
        (ratio * dk)[None],
        (ratio * dv)[None],
        wg[:36, :36].T * (ratio / slots),
        st[0, 0] / (count * WIDTH),
    )


def solution(mesh):
    torus = Mesh(mesh.devices.reshape(4, 8, 8, 2), ("dp_0", "dp_1", "patch_0", "patch_1"))
    return jax.shard_map(
        functools.partial(step, 4, 8),
        mesh=torus,
        in_specs=(
            P(DP, PATCH, None),
            P(DP, PATCH, None),
            P(DP, PATCH, None),
            P(),
            P(DP, PATCH, None),
            P(DP),
            P(DP, PATCH),
        ),
        out_specs=(P(DP, PATCH, None), P(DP, PATCH, None), P(DP, PATCH, None), P(PATCH, DP), P()),
        check_vma=False,
    )
```

```python
import functools
import math

import jax
import jax.numpy as jnp
from jax import lax
from jax.experimental import pallas as pl
from jax.experimental.pallas import tpu as pltpu
from jax.sharding import Mesh
from jax.sharding import PartitionSpec as P

WIDTH = 1152
HEADS = 8
HEAD_DIM = 72
FEAT = 576
ROWS = 128
PAD = 80
PATCH = ("patch_0", "patch_1")
DP = ("dp_0", "dp_1")
BF = jnp.bfloat16
F32 = jnp.float32
FAR = (4, 3, 5, 2, 6, 1, 7)
MASK = 2.0**50


def dot(a, b, ca, cb):
    return lax.dot_general(a, b, (((ca,), (cb,)), ((), ())), preferred_element_type=F32)


def body(
    nx,
    nz,
    q_ref,
    k_ref,
    v_ref,
    seg_ref,
    len_ref,
    w_hbm,
    t_hbm,
    dq_out,
    dk_out,
    dv_out,
    wg_out,
    st_out,
    w_s,
    t_s,
    send1,
    recv1,
    ktok,
    vtok,
    qtok,
    dtok,
    p_s,
    ds_s,
    rinv_s,
    send2,
    recv2,
    at_s,
    send3,
    recv3,
    dof_s,
    dkv,
    drecv,
    send4,
    recv4,
    g_s,
    pg_s,
    pa_s,
    xsend,
    xrecv,
    zsend,
    zrecv,
    ysend,
    yrecv,
    stat_s,
    load_sem,
    s1,
    r1,
    d1s,
    d1r,
    s2,
    r2,
    s3,
    r3,
    dks,
    dkr,
    s4,
    r4,
    gs,
    gr,
    xs,
    xr,
    zs,
    zr,
    ys,
    yr,
    sts,
    strr,
):
    x = lax.axis_index("dp_0")
    z = lax.axis_index("dp_1")
    y = lax.axis_index("patch_0")
    k = lax.axis_index("patch_1")
    other = 1 - k
    p = 2 * y + k
    zh = nz // 2
    scale = 1.0 / math.sqrt(HEAD_DIM)

    load_w = pltpu.make_async_copy(w_hbm, w_s, load_sem.at[0])
    load_t = pltpu.make_async_copy(t_hbm, t_s, load_sem.at[1])
    load_w.start()
    load_t.start()

    barrier = pltpu.get_barrier_semaphore()
    for i in range(1, 8):
        peer = lax.rem(y + i, 8)
        pl.semaphore_signal(barrier, inc=1, device_id={"patch_0": peer})
        pl.semaphore_signal(barrier, inc=1, device_id={"patch_0": peer, "patch_1": other})
    pl.semaphore_signal(barrier, inc=1, device_id={"patch_1": other})
    for i in range(1, nx):
        pl.semaphore_signal(barrier, inc=1, device_id={"dp_0": lax.rem(x + i, nx)})
    for i in range(1, nz):
        pl.semaphore_signal(barrier, inc=1, device_id={"dp_1": lax.rem(z + i, nz)})

    def remote(src, dst, ssem, rsem, **where):
        return pltpu.make_async_remote_copy(
            src_ref=src, dst_ref=dst, send_sem=ssem, recv_sem=rsem, device_id=where
        )

    row = lax.broadcasted_iota(jnp.int32, (8, ROWS), 0)
    lane = lax.broadcasted_iota(jnp.int32, (8, ROWS), 1)
    length = len_ref[0]
    live_t = p * ROWS + lane < length
    code = jnp.where(live_t, jnp.broadcast_to(seg_ref[...], (8, ROWS)), 8)
    low = jnp.bitwise_and(row, 3)
    weight = jnp.where(low == 0, 1, jnp.where(low == 1, 2, jnp.where(low == 2, 4, 8)))
    bit = jnp.where(jnp.bitwise_and(code, weight) != 0, 1.0, 0.0).astype(F32)
    mine = jnp.where(row < 4, bit, 1.0 - bit)
    q_mask = -MASK * mine
    k_mask = MASK * (1.0 - mine)
    v_ones = jnp.where(row == 0, 1.0, 0.0).astype(F32)
    for at, (ref, extra) in enumerate(((q_ref, q_mask), (k_ref, k_mask), (v_ref, v_ones))):
        whole = ref[0].astype(F32)
        for h in range(HEADS):
            block = jnp.concatenate([whole[HEAD_DIM * h : HEAD_DIM * (h + 1)], extra], axis=0)
            send1[h, PAD * at : PAD * (at + 1), :] = block.astype(BF)
    recv1[p] = send1[y]

    pl.semaphore_wait(barrier, 15 + (nx - 1) + (nz - 1))

    first = [None] * 8
    for i in FAR:
        h = lax.rem(y + i, 8)
        first[i] = remote(send1.at[h], recv1.at[p], s1.at[i], r1.at[i], patch_0=h)
        first[i].start()
    kv = pl.ds(PAD, 2 * PAD)

    def pass_on(i):
        b = 2 * lax.rem(y - i + 8, 8) + k
        return remote(
            recv1.at[b, kv], recv1.at[b, kv], d1s.at[i], d1r.at[i], patch_1=other
        )

    def prepare(b):
        at = pl.ds(pl.multiple_of(b * ROWS, ROWS), ROWS)
        both = recv1[b, PAD : 3 * PAD, :].astype(F32)
        ktok[at, :] = both[:PAD].T.astype(BF)
        vtok[at, :] = both[PAD:].T.astype(BF)

    def prepare_q(src):
        at = pl.ds(pl.multiple_of(src * ROWS, ROWS), ROWS)
        qtok[at, :] = recv1[2 * src + k, 0:PAD, :].astype(F32).T.astype(BF)

    passed = [pass_on(i) for i in range(8)]
    passed[0].start()
    prepare(p)
    prepare_q(y)
    for i in (1, 7, 2, 6, 3, 5, 4):
        first[i].wait_recv()
        passed[i].start()
        src = lax.rem(y - i + 8, 8)
        prepare(2 * src + k)
        prepare_q(src)
    for i in (0, 1, 7, 2, 6, 3, 5, 4):
        passed[i].wait_recv()
        prepare(2 * lax.rem(y - i + 8, 8) + other)

    factor = scale * math.log2(math.e)

    def queries(j, part):
        return jnp.concatenate(
            [recv1[4 * j + k, part, :], recv1[4 * j + 2 + k, part, :]], axis=1
        )

    def forward(j, carry):
        scores = dot(ktok[...], queries(j, slice(0, PAD)), 1, 0)
        top = jnp.max(scores, axis=0, keepdims=True)
        probs = jnp.exp2((scores - top) * factor).astype(BF)
        p_s[j] = probs
        values = jnp.concatenate([recv1[b, 2 * PAD : 3 * PAD, :] for b in range(16)], axis=1)
        accum = dot(values, probs, 1, 0)
        rinv = 1.0 / accum[HEAD_DIM : HEAD_DIM + 1, :]
        rinv_s[j] = jnp.broadcast_to(rinv, (8, 2 * ROWS))
        attn = (accum * rinv).astype(BF)
        send2[2 * j] = attn[:, :ROWS]
        send2[2 * j + 1] = attn[:, ROWS:]
        return carry

    lax.fori_loop(0, 4, forward, 0)
    second = [None] * 8
    for i in FAR:
        to = lax.rem(y + i, 8)
        second[i] = remote(send2.at[to], recv2.at[y], s2.at[i], r2.at[i], patch_0=to)
        second[i].start()
    recv2[y] = send2[y]

    load_w.wait()
    load_t.wait()
    for i in (1, 7, 2, 6, 3, 5, 4):
        second[i].wait_recv()
    for h in range(HEADS):
        at_s[HEAD_DIM * h : HEAD_DIM * (h + 1), :] = recv2[h].astype(F32)[:HEAD_DIM]
    attn_t = at_s[...].astype(BF)
    pa_s[0] = attn_t
    output = dot(attn_t, w_s[...], 0, 0)
    token = lax.broadcasted_iota(jnp.int32, (ROWS, WIDTH), 0)
    live = p * ROWS + token < length
    error = jnp.where(live, output - t_s[0].astype(F32), 0.0)
    grad_out = (2.0 * error).astype(BF)
    grad_attn = dot(w_s[...], grad_out, 1, 1)
    for h in range(HEADS):
        block = jnp.concatenate(
            [grad_attn[HEAD_DIM * h : HEAD_DIM * (h + 1)], jnp.zeros((8, ROWS), F32)], axis=0
        )
        send3[h] = block.astype(BF)
    third = [None] * 8
    for i in FAR:
        to = lax.rem(y + i, 8)
        third[i] = remote(send3.at[to], recv3.at[y], s3.at[i], r3.at[i], patch_0=to)
        third[i].start()
    recv3[y] = send3[y]

    grad_t = (2.0 * error).T.astype(BF)
    part = WIDTH // (2 * nx)
    for half in range(2):
        for xx in range(nx):
            at = (2 * xx + half) * part
            g_s[half, part * xx : part * (xx + 1), :] = grad_t[at : at + part]
    swap = [
        remote(g_s.at[other], pg_s, gs.at[0], gr.at[0], patch_1=other),
        remote(pa_s.at[0], pa_s.at[1], gs.at[1], gr.at[1], patch_1=other),
    ]
    for c in swap:
        c.start()
    squares = jnp.sum(error * error)
    cell = lax.broadcasted_iota(jnp.int32, (8, ROWS), 1)
    stat_s[0] = jnp.where(
        cell == 0, squares, jnp.where(cell == 1, length.astype(F32), 0.0)
    )

    def stat_copies(stage, base, n, me, to):
        return [
            remote(
                stat_s.at[stage],
                stat_s.at[base + i],
                sts.at[base + i],
                strr.at[base + i],
                **to(lax.rem(me + i, n)),
            )
            for i in range(1, n)
        ]

    stat_y = stat_copies(0, 3, 16, p, lambda t: {"patch_0": t // 2, "patch_1": lax.rem(t, 2)})
    for c in stat_y:
        c.start()
    for c in swap:
        c.wait_recv()
    left = jnp.concatenate([g_s[k], pg_s[...]], axis=1)
    right = jnp.concatenate([pa_s[0], pa_s[1]], axis=1)
    partial = dot(left, right, 1, 1)
    for xx in range(nx):
        xsend[xx] = partial[part * xx : part * (xx + 1)].astype(BF)
    xcopies = [None] * nx
    for i in range(1, nx):
        to = lax.rem(x + i, nx)
        xcopies[i] = remote(xsend.at[to], xrecv.at[i], xs.at[i], xr.at[i], dp_0=to)
        xcopies[i].start()

    for i in (1, 7, 2, 6, 3, 5, 4):
        third[i].wait_recv()

    def fold(s, carry):
        rinv = rinv_s[s // 2, 0:1, pl.ds(pl.multiple_of(lax.rem(s, 2) * ROWS, ROWS), ROWS)]
        folded = recv3[s].astype(F32) * rinv
        dof_s[s] = folded.astype(BF)
        dtok[pl.ds(pl.multiple_of(s * ROWS, ROWS), ROWS), :] = folded.T.astype(BF)
        return carry

    lax.fori_loop(0, 8, fold, 0)

    def backward(j, carry):
        grads = jnp.concatenate([dof_s[2 * j], dof_s[2 * j + 1]], axis=1)
        attn = jnp.concatenate([send2[2 * j], send2[2 * j + 1]], axis=1)
        delta = jnp.sum(grads.astype(F32) * attn.astype(F32), axis=0, keepdims=True)
        dprobs = dot(vtok[...], grads, 1, 0)
        dscores = (p_s[j].astype(F32) * (dprobs - delta)).astype(BF)
        ds_s[j] = dscores
        keys = jnp.concatenate([recv1[b, PAD : 2 * PAD, :] for b in range(16)], axis=1)
        dq = (dot(keys, dscores, 1, 0) * scale).astype(BF)
        send4[2 * j, 0:PAD, :] = dq[:, :ROWS]
        send4[2 * j + 1, 0:PAD, :] = dq[:, ROWS:]
        return carry

    lax.fori_loop(0, 4, backward, 0)

    def keyside(t, carry):
        at = pl.ds(pl.multiple_of(t * 2 * ROWS, 2 * ROWS), 2 * ROWS)
        ds_rows = jnp.concatenate([ds_s[j, at, :] for j in range(4)], axis=1)
        p_rows = jnp.concatenate([p_s[j, at, :] for j in range(4)], axis=1)
        dk = (dot(ds_rows, qtok[...], 1, 0) * scale).T.astype(BF)
        dv = dot(p_rows, dtok[...], 1, 0).T.astype(BF)
        for c in range(2):
            dkv[c, t, 0:PAD, :] = dk[:, ROWS * c : ROWS * (c + 1)]
            dkv[c, t, PAD : 2 * PAD, :] = dv[:, ROWS * c : ROWS * (c + 1)]
        return carry

    lax.fori_loop(0, 8, keyside, 0)
    cross = remote(dkv.at[other], drecv, dks.at[0], dkr.at[0], patch_1=other)
    cross.start()

    for i in range(1, nx):
        xcopies[i].wait_recv()
    total = partial[0:part] * 0.0
    total = xsend[x].astype(F32)
    for i in range(1, nx):
        total = total + xrecv[i].astype(F32)
    cols = part // zh
    for j in range(zh):
        zsend[j, 0:cols, :] = total[cols * j : cols * (j + 1)].astype(BF)
    zcopies = [None] * zh
    for j in range(zh):
        to = zh * k + j
        away = lax.rem(to - z + nz, nz)
        zcopies[j] = remote(zsend.at[j], zrecv.at[away], zs.at[j], zr.at[away], dp_1=to)

        @pl.when(to != z)
        def _():
            zcopies[j].start()

    active = z // zh == k

    @pl.when(active)
    def _():
        zrecv[0] = zsend[lax.rem(z, zh)]

    for i in range(15):
        stat_y[i].wait_recv()
    acc = stat_s[0]
    for i in range(1, 16):
        acc = acc + stat_s[3 + i]
    stat_s[1] = acc
    stat_x = stat_copies(1, 19, nx, x, lambda t: {"dp_0": t})
    for c in stat_x:
        c.start()

    cross.wait_recv()

    def join(s, carry):
        send4[s, PAD : 3 * PAD, :] = (
            dkv[k, s].astype(F32) + drecv[s].astype(F32)
        ).astype(BF)
        return carry

    lax.fori_loop(0, 8, join, 0)
    fourth = [None] * 8
    for i in FAR:
        to = lax.rem(y + i, 8)
        fourth[i] = remote(send4.at[to], recv4.at[y], s4.at[i], r4.at[i], patch_0=to)
        fourth[i].start()
    recv4[y] = send4[y]

    for c in stat_x:
        c.wait_recv()
    acc = stat_s[1]
    for i in range(1, nx):
        acc = acc + stat_s[19 + i]
    stat_s[2] = acc
    stat_z = stat_copies(2, 19 + nx, nz, z, lambda t: {"dp_1": t})
    for c in stat_z:
        c.start()

    def z_in(i):
        return remote(zsend.at[0], zrecv.at[i], zs.at[0], zr.at[i], dp_1=z)

    @pl.when(active)
    def _():
        for i in range(1, nz):
            z_in(i).wait_recv()
        summed = zrecv[0].astype(F32)
        for i in range(1, nz):
            summed = summed + zrecv[i].astype(F32)
        for t in range(16):
            ysend[t, 0:cols, 0:36] = summed[0:cols, 36 * t : 36 * (t + 1)]

    def y_out(t):
        return remote(
            ysend.at[t], yrecv.at[y], ys.at[t], yr.at[y], patch_0=t // 2, patch_1=t % 2
        )

    for t in range(16):

        @pl.when(active & (p != t))
        def _():
            y_out(t).start()

    @pl.when(active)
    def _():
        yrecv[y] = ysend[p]

    for c in stat_z:
        c.wait_recv()
    acc = stat_s[2]
    for i in range(1, nz):
        acc = acc + stat_s[19 + nx + i]
    count = acc[0:1, 1:2] / 16.0
    ratio = (nx * nz * 16.0 * ROWS) / count
    st_out[...] = acc[0:1, 0:1] / (count * WIDTH)

    for i in (1, 7, 2, 6, 3, 5, 4):
        fourth[i].wait_recv()
    for at, out in enumerate((dq_out, dk_out, dv_out)):
        whole = jnp.concatenate(
            [
                recv4[h, PAD * at : PAD * (at + 1), :].astype(F32)[:HEAD_DIM]
                for h in range(HEADS)
            ],
            axis=0,
        )
        out[0] = whole * ratio

    for i in range(8):
        here = active & (y == i)

        @pl.when(jnp.logical_not(here))
        def _():
            remote(
                ysend.at[0], yrecv.at[i], ys.at[0], yr.at[i], patch_0=y, patch_1=k
            ).wait_recv()

    final = yrecv[0]
    for i in range(1, 8):
        final = final + yrecv[i]
    wg_out[...] = final.T[0:36, 0:36] * (ratio / (16.0 * ROWS))

    for group in (first, second, third, fourth, xcopies):
        for c in group[1:]:
            c.wait_send()
    for c in passed + swap + [cross] + stat_y + stat_x + stat_z:
        c.wait_send()
    for j in range(zh):

        @pl.when(zh * k + j != z)
        def _():
            zcopies[j].wait_send()

    for t in range(16):

        @pl.when(active & (p != t))
        def _():
            y_out(t).wait_send()


def step(nx, nz, query_rows, key_rows, value_rows, out_weight, target, lengths, segments):
    part = WIDTH // (2 * nx)
    zh = nz // 2
    dma = pltpu.SemaphoreType.DMA
    scratch = [
        pltpu.VMEM((FEAT, WIDTH), BF),
        pltpu.VMEM((1, ROWS, WIDTH), BF),
        pltpu.VMEM((8, 3 * PAD, ROWS), BF),
        pltpu.VMEM((16, 3 * PAD, ROWS), BF),
        pltpu.VMEM((2048, PAD), BF),
        pltpu.VMEM((2048, PAD), BF),
        pltpu.VMEM((1024, PAD), BF),
        pltpu.VMEM((1024, PAD), BF),
        pltpu.VMEM((4, 2048, 256), BF),
        pltpu.VMEM((4, 2048, 256), BF),
        pltpu.VMEM((4, 8, 256), F32),
        pltpu.VMEM((8, PAD, ROWS), BF),
        pltpu.VMEM((8, PAD, ROWS), BF),
        pltpu.VMEM((FEAT, ROWS), F32),
        pltpu.VMEM((8, PAD, ROWS), BF),
        pltpu.VMEM((8, PAD, ROWS), BF),
        pltpu.VMEM((8, PAD, ROWS), BF),
        pltpu.VMEM((2, 8, 2 * PAD, ROWS), BF),
        pltpu.VMEM((8, 2 * PAD, ROWS), BF),
        pltpu.VMEM((8, 3 * PAD, ROWS), BF),
        pltpu.VMEM((8, 3 * PAD, ROWS), BF),
        pltpu.VMEM((2, FEAT, ROWS), BF),
        pltpu.VMEM((FEAT, ROWS), BF),
        pltpu.VMEM((2, FEAT, ROWS), BF),
        pltpu.VMEM((nx, part, FEAT), BF),
        pltpu.VMEM((nx, part, FEAT), BF),
        pltpu.VMEM((zh, 48, FEAT), BF),
        pltpu.VMEM((nz, 48, FEAT), BF),
        pltpu.VMEM((16, 40, 128), F32),
        pltpu.VMEM((8, 40, 128), F32),
        pltpu.VMEM((19 + nx + nz, 8, ROWS), F32),
    ]
    sems = [2, 8, 8, 8, 8, 8, 8, 8, 8, 1, 1, 8, 8, 2, 2, nx, nx, zh, nz, 16, 8]
    sems += [19 + nx + nz] * 2
    vmem = pl.BlockSpec(memory_space=pltpu.VMEM)
    hbm = pl.BlockSpec(memory_space=pl.ANY)
    wide = jax.ShapeDtypeStruct((1, FEAT, ROWS), F32)
    dq, dk, dv, wg, st = pl.pallas_call(
        functools.partial(body, nx, nz),
        out_shape=(
            wide,
            wide,
            wide,
            jax.ShapeDtypeStruct((36, 36), F32),
            jax.ShapeDtypeStruct((1, 1), F32),
        ),
        in_specs=[vmem] * 4 + [pl.BlockSpec(memory_space=pltpu.SMEM), hbm, hbm],
        out_specs=(vmem,) * 5,
        scratch_shapes=scratch + [dma((n,)) for n in sems],
        compiler_params=pltpu.CompilerParams(
            collective_id=0, has_side_effects=True, vmem_limit_bytes=60 * 1024 * 1024
        ),
    )(
        jnp.swapaxes(query_rows, 1, 2),
        jnp.swapaxes(key_rows, 1, 2),
        jnp.swapaxes(value_rows, 1, 2),
        segments,
        lengths,
        out_weight,
        target,
    )
    return (
        jnp.swapaxes(dq, 1, 2),
        jnp.swapaxes(dk, 1, 2),
        jnp.swapaxes(dv, 1, 2),
        wg,
        st[0, 0],
    )


def solution(mesh):
    torus = Mesh(mesh.devices.reshape(4, 8, 8, 2), ("dp_0", "dp_1", "patch_0", "patch_1"))
    return jax.shard_map(
        functools.partial(step, 4, 8),
        mesh=torus,
        in_specs=(
            P(DP, PATCH, None),
            P(DP, PATCH, None),
            P(DP, PATCH, None),
            P(),
            P(DP, PATCH, None),
            P(DP),
            P(DP, PATCH),
        ),
        out_specs=(P(DP, PATCH, None), P(DP, PATCH, None), P(DP, PATCH, None), P(PATCH, DP), P()),
        check_vma=False,
    )
```

```python
import functools
import math

import jax
import jax.numpy as jnp
from jax import lax
from jax.experimental import pallas as pl
from jax.experimental.pallas import tpu as pltpu
from jax.sharding import Mesh
from jax.sharding import PartitionSpec as P

WIDTH = 1152
HEADS = 8
HEAD_DIM = 72
FEAT = 576
ROWS = 128
PAD = 80
PATCH = ("patch_0", "patch_1")
DP = ("dp_0", "dp_1")
BF = jnp.bfloat16
F32 = jnp.float32
FAR = (4, 3, 5, 2, 6, 1, 7)
NEAR = (1, 7, 2, 6, 3, 5, 4)
LAG = 3
MASK = 2.0**50


def dot(a, b, ca, cb):
    return lax.dot_general(a, b, (((ca,), (cb,)), ((), ())), preferred_element_type=F32)


def body(
    nx,
    nz,
    q_hbm,
    k_hbm,
    v_hbm,
    seg_hbm,
    len_ref,
    w_hbm,
    t_hbm,
    dq_out,
    dk_out,
    dv_out,
    wg_out,
    st_out,
    q_s,
    k_s,
    v_s,
    seg_s,
    w_s,
    t_s,
    send1,
    recv1,
    ktok,
    vtok,
    qtok,
    dtok,
    p_s,
    ds_s,
    rinv_s,
    send2,
    recv2,
    at_s,
    send3,
    recv3,
    dkv,
    drecv,
    send4,
    recv4,
    g_s,
    pg_s,
    pa_s,
    xsend,
    xrecv,
    zsend,
    zrecv,
    ysend,
    yrecv,
    stat_s,
    load_sem,
    s1,
    r1,
    s1v,
    r1v,
    d1s,
    d1r,
    d1vs,
    d1vr,
    s2,
    r2,
    s3,
    r3,
    dks,
    dkr,
    s4q,
    r4q,
    s4,
    r4,
    gs,
    gr,
    xs,
    xr,
    zs,
    zr,
    ys,
    yr,
    sts,
    strr,
):
    x = lax.axis_index("dp_0")
    z = lax.axis_index("dp_1")
    y = lax.axis_index("patch_0")
    k = lax.axis_index("patch_1")
    other = 1 - k
    p = 2 * y + k
    zh = nz // 2
    scale = 1.0 / math.sqrt(HEAD_DIM)

    loads = [
        pltpu.make_async_copy(src, dst, load_sem.at[n])
        for n, (src, dst) in enumerate(
            (
                (q_hbm, q_s),
                (k_hbm, k_s),
                (seg_hbm, seg_s),
                (v_hbm, v_s),
                (w_hbm, w_s),
                (t_hbm, t_s),
            )
        )
    ]
    for c in loads:
        c.start()

    barrier = pltpu.get_barrier_semaphore()
    for i in range(1, 8):
        peer = lax.rem(y + i, 8)
        pl.semaphore_signal(barrier, inc=1, device_id={"patch_0": peer})
        pl.semaphore_signal(barrier, inc=1, device_id={"patch_0": peer, "patch_1": other})
    pl.semaphore_signal(barrier, inc=1, device_id={"patch_1": other})
    for i in range(1, nx):
        pl.semaphore_signal(barrier, inc=1, device_id={"dp_0": lax.rem(x + i, nx)})
    for i in range(1, nz):
        pl.semaphore_signal(barrier, inc=1, device_id={"dp_1": lax.rem(z + i, nz)})

    def remote(src, dst, ssem, rsem, **where):
        return pltpu.make_async_remote_copy(
            src_ref=src, dst_ref=dst, send_sem=ssem, recv_sem=rsem, device_id=where
        )

    row = lax.broadcasted_iota(jnp.int32, (8, ROWS), 0)
    lane = lax.broadcasted_iota(jnp.int32, (8, ROWS), 1)
    length = len_ref[0]
    live_t = p * ROWS + lane < length
    for c in loads[:4]:
        c.wait()
    code = jnp.where(live_t, jnp.broadcast_to(seg_s[...], (8, ROWS)), 8)
    low = jnp.bitwise_and(row, 3)
    weight = jnp.where(low == 0, 1, jnp.where(low == 1, 2, jnp.where(low == 2, 4, 8)))
    bit = jnp.where(jnp.bitwise_and(code, weight) != 0, 1.0, 0.0).astype(F32)
    mine = jnp.where(row < 4, bit, 1.0 - bit)
    q_mask = -MASK * mine
    k_mask = MASK * (1.0 - mine)
    v_ones = jnp.where(row == 0, 1.0, 0.0).astype(F32)
    for at, (ref, extra) in enumerate(((q_s, q_mask), (k_s, k_mask), (v_s, v_ones))):
        whole = ref[0].astype(F32)
        for h in range(HEADS):
            block = jnp.concatenate([whole[HEAD_DIM * h : HEAD_DIM * (h + 1)], extra], axis=0)
            send1[h, PAD * at : PAD * (at + 1), :] = block.astype(BF)
    recv1[p] = send1[y]

    pl.semaphore_wait(barrier, 15 + (nx - 1) + (nz - 1))

    qk = pl.ds(0, 2 * PAD)
    ko = pl.ds(PAD, PAD)
    vo = pl.ds(2 * PAD, PAD)

    def spread(rows, ssem, rsem):
        out = [None] * 8
        for i in FAR:
            h = lax.rem(y + i, 8)
            out[i] = remote(
                send1.at[h, rows], recv1.at[p, rows], ssem.at[i], rsem.at[i], patch_0=h
            )
            out[i].start()
        return out

    first = spread(qk, s1, r1)
    first_v = spread(vo, s1v, r1v)

    def source(i):
        return lax.rem(y - i + 8, 8)

    def pass_on(i, rows, ssem, rsem):
        ref = recv1.at[2 * source(i) + k, rows]
        return remote(ref, ref, ssem.at[i], rsem.at[i], patch_1=other)

    def token_major(dst, b, part, at):
        at = pl.ds(pl.multiple_of(at * ROWS, ROWS), ROWS)
        dst[at, :] = recv1[b, PAD * part : PAD * (part + 1), :].astype(F32).T.astype(BF)

    passed = [pass_on(i, ko, d1s, d1r) for i in range(8)]
    passed_v = [pass_on(i, vo, d1vs, d1vr) for i in range(8)]
    passed[0].start()
    passed_v[0].start()
    token_major(ktok, p, 1, p)
    for i in NEAR:
        first[i].wait_recv()
        passed[i].start()
        b = 2 * source(i) + k
        token_major(ktok, b, 1, b)
    for i in (0,) + NEAR:
        passed[i].wait_recv()
        b = 2 * source(i) + other
        token_major(ktok, b, 1, b)

    factor = scale * math.log2(math.e)
    pair = y // 2
    mate = y + 1 - 2 * lax.rem(y, 2)

    def forward(j, carry):
        queries = jnp.concatenate([recv1[4 * j + k, 0:PAD, :], recv1[4 * j + 2 + k, 0:PAD, :]], axis=1)
        scores = dot(ktok[...], queries, 1, 0)
        top = jnp.max(scores, axis=0, keepdims=True)
        p_s[j] = jnp.exp2((scores - top) * factor).astype(BF)
        return carry

    lax.fori_loop(0, 4, forward, 0)
    for i in NEAR:
        first_v[i].wait_recv()
        passed_v[i].start()
    for i in (0,) + NEAR:
        passed_v[i].wait_recv()

    def send_attn(s):
        i = lax.rem(s - y + 8, 8)
        return remote(send2.at[s], recv2.at[y], s2.at[i], r2.at[i], patch_0=s)

    for step_at in (2, 1, 3, 0):
        j = lax.rem(pair + step_at, 4)
        values = jnp.concatenate([recv1[b, 2 * PAD : 3 * PAD, :] for b in range(16)], axis=1)
        accum = dot(values, p_s[j], 1, 0)
        rinv = 1.0 / accum[HEAD_DIM : HEAD_DIM + 1, :]
        rinv_s[j] = jnp.broadcast_to(rinv, (8, 2 * ROWS))
        attn = (accum * rinv).astype(BF)
        send2[2 * j] = attn[:, :ROWS]
        send2[2 * j + 1] = attn[:, ROWS:]
        if step_at:
            send_attn(2 * j).start()
            send_attn(2 * j + 1).start()
        else:
            send_attn(mate).start()
    recv2[y] = send2[y]

    def backward_layouts(b, carry):
        token_major(vtok, b, 2, b)
        return carry

    lax.fori_loop(0, 16, backward_layouts, 0)

    def query_layouts(src, carry):
        token_major(qtok, 2 * src + k, 0, src)
        return carry

    lax.fori_loop(0, 8, query_layouts, 0)

    loads[4].wait()
    loads[5].wait()
    for i in NEAR:
        remote(send2.at[y], recv2.at[source(i)], s2.at[i], r2.at[i], patch_0=source(i)).wait_recv()
    for h in range(HEADS):
        at_s[HEAD_DIM * h : HEAD_DIM * (h + 1), :] = recv2[h].astype(F32)[:HEAD_DIM]
    attn_t = at_s[...].astype(BF)
    pa_s[0] = attn_t
    swap_a = remote(pa_s.at[0], pa_s.at[1], gs.at[1], gr.at[1], patch_1=other)
    swap_a.start()
    output = dot(attn_t, w_s[...], 0, 0)
    token = lax.broadcasted_iota(jnp.int32, (ROWS, WIDTH), 0)
    live = p * ROWS + token < length
    error = jnp.where(live, output - t_s[0].astype(F32), 0.0)
    grad_out = (2.0 * error).astype(BF)
    grad_attn = dot(w_s[...], grad_out, 1, 1)
    for h in range(HEADS):
        block = jnp.concatenate(
            [grad_attn[HEAD_DIM * h : HEAD_DIM * (h + 1)], jnp.zeros((8, ROWS), F32)], axis=0
        )
        send3[h] = block.astype(BF)
    third = [None] * 8
    for i in FAR:
        to = lax.rem(y + i, 8)
        third[i] = remote(send3.at[to], recv3.at[y], s3.at[i], r3.at[i], patch_0=to)
        third[i].start()
    recv3[y] = send3[y]

    grad_t = (2.0 * error).T.astype(BF)
    part = WIDTH // (2 * nx)
    for half in range(2):
        for xx in range(nx):
            at = (2 * xx + half) * part
            g_s[half, part * xx : part * (xx + 1), :] = grad_t[at : at + part]
    swap_g = remote(g_s.at[other], pg_s, gs.at[0], gr.at[0], patch_1=other)
    swap_g.start()
    squares = jnp.sum(error * error)
    cell = lax.broadcasted_iota(jnp.int32, (8, ROWS), 1)
    stat_s[0] = jnp.where(
        cell == 0, squares, jnp.where(cell == 1, length.astype(F32), 0.0)
    )

    def stat_copies(stage, base, n, me, to):
        return [
            remote(
                stat_s.at[stage],
                stat_s.at[base + i],
                sts.at[base + i],
                strr.at[base + i],
                **to(lax.rem(me + i, n)),
            )
            for i in range(1, n)
        ]

    def stat_sum(stage, base, n, copies):
        for c in copies:
            c.wait_recv()
        acc = stat_s[stage]
        for i in range(1, n):
            acc = acc + stat_s[base + i]
        return acc

    stat_y = stat_copies(0, 3, 16, p, lambda t: {"patch_0": t // 2, "patch_1": lax.rem(t, 2)})
    for c in stat_y:
        c.start()
    swap_a.wait_recv()
    swap_g.wait_recv()
    left = jnp.concatenate([g_s[k], pg_s[...]], axis=1)
    right = jnp.concatenate([pa_s[0], pa_s[1]], axis=1)
    partial = dot(left, right, 1, 1)
    for xx in range(nx):
        xsend[xx] = partial[part * xx : part * (xx + 1)].astype(BF)
    xcopies = [None] * nx
    for i in range(1, nx):
        to = lax.rem(x + i, nx)
        xcopies[i] = remote(xsend.at[to], xrecv.at[i], xs.at[i], xr.at[i], dp_0=to)
        xcopies[i].start()

    def send_grad(s, rows, ssem, rsem):
        i = lax.rem(s - y + 8, 8)
        return remote(
            send4.at[s, rows], recv4.at[y, rows], ssem.at[i], rsem.at[i], patch_0=s
        )

    qo = pl.ds(0, PAD)
    kvo = pl.ds(PAD, 2 * PAD)

    def third_in(s):
        i = lax.rem(y - s + 8, 8)
        remote(send3.at[y], recv3.at[s], s3.at[i], r3.at[i], patch_0=s).wait_recv()

    for step_at in (0, 1, 3, 2):
        j = lax.rem(pair + step_at, 4)
        if step_at:
            third_in(2 * j)
            third_in(2 * j + 1)
        else:
            third_in(mate)
        grads = jnp.concatenate([recv3[2 * j], recv3[2 * j + 1]], axis=1).astype(F32)
        folded = grads * rinv_s[j, 0:1, :]
        dtok[pl.ds(pl.multiple_of(j * 2 * ROWS, 2 * ROWS), 2 * ROWS), :] = folded.T.astype(BF)
        folded = folded.astype(BF)
        attn = jnp.concatenate([send2[2 * j], send2[2 * j + 1]], axis=1)
        delta = jnp.sum(folded.astype(F32) * attn.astype(F32), axis=0, keepdims=True)
        dprobs = dot(vtok[...], folded, 1, 0)
        dscores = (p_s[j].astype(F32) * (dprobs - delta)).astype(BF)
        ds_s[j] = dscores
        keys = jnp.concatenate([recv1[b, PAD : 2 * PAD, :] for b in range(16)], axis=1)
        dq = (dot(keys, dscores, 1, 0) * scale).astype(BF)
        send4[2 * j, 0:PAD, :] = dq[:, :ROWS]
        send4[2 * j + 1, 0:PAD, :] = dq[:, ROWS:]
        if step_at:
            send_grad(2 * j, qo, s4q, r4q).start()
            send_grad(2 * j + 1, qo, s4q, r4q).start()
        else:
            send_grad(mate, qo, s4q, r4q).start()

    stat_s[1] = stat_sum(0, 3, 16, stat_y)
    stat_x = stat_copies(1, 19, nx, x, lambda t: {"dp_0": t})
    for c in stat_x:
        c.start()

    def crossing(t):
        i = lax.rem(t - y + 8, 8)
        return remote(dkv.at[other, t], drecv.at[t], dks.at[i], dkr.at[i], patch_1=other)

    def join(t, away):
        crossing(t).wait_recv()
        send4[t, PAD : 3 * PAD, :] = (
            dkv[k, t].astype(F32) + drecv[t].astype(F32)
        ).astype(BF)
        if away:
            send_grad(t, kvo, s4, r4).start()

    order = FAR + (0,)
    for n, i in enumerate(order):
        t = lax.rem(y + i, 8)
        at = pl.ds(pl.multiple_of(t * 2 * ROWS, 2 * ROWS), 2 * ROWS)
        ds_rows = jnp.concatenate([ds_s[j, at, :] for j in range(4)], axis=1)
        p_rows = jnp.concatenate([p_s[j, at, :] for j in range(4)], axis=1)
        dk = (dot(ds_rows, qtok[...], 1, 0) * scale).T.astype(BF)
        dv = dot(p_rows, dtok[...], 1, 0).T.astype(BF)
        for c in range(2):
            dkv[c, t, 0:PAD, :] = dk[:, ROWS * c : ROWS * (c + 1)]
            dkv[c, t, PAD : 2 * PAD, :] = dv[:, ROWS * c : ROWS * (c + 1)]
        crossing(t).start()
        if n >= LAG:
            join(lax.rem(y + order[n - LAG], 8), order[n - LAG])
    for i in order[8 - LAG :]:
        join(lax.rem(y + i, 8), i)

    for i in range(1, nx):
        xcopies[i].wait_recv()
    total = xsend[x].astype(F32)
    for i in range(1, nx):
        total = total + xrecv[i].astype(F32)
    cols = part // zh
    for j in range(zh):
        zsend[j, 0:cols, :] = total[cols * j : cols * (j + 1)].astype(BF)
    zcopies = [None] * zh
    for j in range(zh):
        to = zh * k + j
        away = lax.rem(to - z + nz, nz)
        zcopies[j] = remote(zsend.at[j], zrecv.at[away], zs.at[j], zr.at[away], dp_1=to)

        @pl.when(to != z)
        def _():
            zcopies[j].start()

    active = z // zh == k

    @pl.when(active)
    def _():
        zrecv[0] = zsend[lax.rem(z, zh)]

    stat_s[2] = stat_sum(1, 19, nx, stat_x)
    stat_z = stat_copies(2, 19 + nx, nz, z, lambda t: {"dp_1": t})
    for c in stat_z:
        c.start()
    recv4[y] = send4[y]

    def z_in(i):
        return remote(zsend.at[0], zrecv.at[i], zs.at[0], zr.at[i], dp_1=z)

    @pl.when(active)
    def _():
        for i in range(1, nz):
            z_in(i).wait_recv()
        summed = zrecv[0].astype(F32)
        for i in range(1, nz):
            summed = summed + zrecv[i].astype(F32)
        for t in range(16):
            ysend[t, 0:cols, 0:36] = summed[0:cols, 36 * t : 36 * (t + 1)]

    def y_out(t):
        return remote(
            ysend.at[t], yrecv.at[y], ys.at[t], yr.at[y], patch_0=t // 2, patch_1=t % 2
        )

    for t in range(16):

        @pl.when(active & (p != t))
        def _():
            y_out(t).start()

    @pl.when(active)
    def _():
        yrecv[y] = ysend[p]

    acc = stat_sum(2, 19 + nx, nz, stat_z)
    count = acc[0:1, 1:2] / 16.0
    ratio = (nx * nz * 16.0 * ROWS) / count
    st_out[...] = acc[0:1, 0:1] / (count * WIDTH)

    def grad_in(i, rows, ssem, rsem):
        remote(
            send4.at[y, rows], recv4.at[source(i), rows], ssem.at[i], rsem.at[i], patch_0=y
        ).wait_recv()

    def emit(at, out):
        whole = jnp.concatenate(
            [
                recv4[h, PAD * at : PAD * (at + 1), :].astype(F32)[:HEAD_DIM]
                for h in range(HEADS)
            ],
            axis=0,
        )
        out[0] = whole * ratio

    for i in NEAR:
        grad_in(i, qo, s4q, r4q)
    emit(0, dq_out)
    for i in NEAR:
        grad_in(i, kvo, s4, r4)
    emit(1, dk_out)
    emit(2, dv_out)

    for i in range(8):
        here = active & (y == i)

        @pl.when(jnp.logical_not(here))
        def _():
            remote(
                ysend.at[0], yrecv.at[i], ys.at[0], yr.at[i], patch_0=y, patch_1=k
            ).wait_recv()

    final = yrecv[0]
    for i in range(1, 8):
        final = final + yrecv[i]
    wg_out[...] = final.T[0:36, 0:36] * (ratio / (16.0 * ROWS))

    for group in (first, first_v, third, xcopies):
        for c in group[1:]:
            c.wait_send()
    for i in range(1, 8):
        to = lax.rem(y + i, 8)
        send_attn(to).wait_send()
        send_grad(to, qo, s4q, r4q).wait_send()
        send_grad(to, kvo, s4, r4).wait_send()
    for i in range(8):
        crossing(lax.rem(y + i, 8)).wait_send()
    for c in passed + passed_v + [swap_a, swap_g] + stat_y + stat_x + stat_z:
        c.wait_send()
    for j in range(zh):

        @pl.when(zh * k + j != z)
        def _():
            zcopies[j].wait_send()

    for t in range(16):

        @pl.when(active & (p != t))
        def _():
            y_out(t).wait_send()


def write_out(*refs):
    n = len(refs) // 2
    copies = [
        pltpu.make_async_copy(refs[i], refs[n + i], refs[-1].at[i]) for i in range(n)
    ]
    for c in copies:
        c.start()
    for c in copies:
        c.wait()


def step(nx, nz, query_rows, key_rows, value_rows, out_weight, target, lengths, segments):
    part = WIDTH // (2 * nx)
    zh = nz // 2
    dma = pltpu.SemaphoreType.DMA
    scratch = [
        pltpu.VMEM((1, FEAT, ROWS), BF),
        pltpu.VMEM((1, FEAT, ROWS), BF),
        pltpu.VMEM((1, FEAT, ROWS), BF),
        pltpu.VMEM((1, ROWS), jnp.int32),
        pltpu.VMEM((FEAT, WIDTH), BF),
        pltpu.VMEM((1, ROWS, WIDTH), BF),
        pltpu.VMEM((8, 3 * PAD, ROWS), BF),
        pltpu.VMEM((16, 3 * PAD, ROWS), BF),
        pltpu.VMEM((2048, PAD), BF),
        pltpu.VMEM((2048, PAD), BF),
        pltpu.VMEM((1024, PAD), BF),
        pltpu.VMEM((1024, PAD), BF),
        pltpu.VMEM((4, 2048, 256), BF),
        pltpu.VMEM((4, 2048, 256), BF),
        pltpu.VMEM((4, 8, 256), F32),
        pltpu.VMEM((8, PAD, ROWS), BF),
        pltpu.VMEM((8, PAD, ROWS), BF),
        pltpu.VMEM((FEAT, ROWS), F32),
        pltpu.VMEM((8, PAD, ROWS), BF),
        pltpu.VMEM((8, PAD, ROWS), BF),
        pltpu.VMEM((2, 8, 2 * PAD, ROWS), BF),
        pltpu.VMEM((8, 2 * PAD, ROWS), BF),
        pltpu.VMEM((8, 3 * PAD, ROWS), BF),
        pltpu.VMEM((8, 3 * PAD, ROWS), BF),
        pltpu.VMEM((2, FEAT, ROWS), BF),
        pltpu.VMEM((FEAT, ROWS), BF),
        pltpu.VMEM((2, FEAT, ROWS), BF),
        pltpu.VMEM((nx, part, FEAT), BF),
        pltpu.VMEM((nx, part, FEAT), BF),
        pltpu.VMEM((zh, 48, FEAT), BF),
        pltpu.VMEM((nz, 48, FEAT), BF),
        pltpu.VMEM((16, 40, 128), F32),
        pltpu.VMEM((8, 40, 128), F32),
        pltpu.VMEM((19 + nx + nz, 8, ROWS), F32),
    ]
    sems = [6] + [8] * 18 + [2, 2, nx, nx, zh, nz, 16, 8]
    sems += [19 + nx + nz] * 2
    vmem = pl.BlockSpec(memory_space=pltpu.VMEM)
    hbm = pl.BlockSpec(memory_space=pltpu.HBM)
    wide = jax.ShapeDtypeStruct((1, FEAT, ROWS), F32)
    results = (
        wide,
        wide,
        wide,
        jax.ShapeDtypeStruct((36, 36), F32),
        jax.ShapeDtypeStruct((1, 1), F32),
    )
    far = lambda a: pltpu.with_memory_space_constraint(a, pltpu.HBM)
    grads = pl.pallas_call(
        functools.partial(body, nx, nz),
        out_shape=results,
        in_specs=[hbm] * 4 + [pl.BlockSpec(memory_space=pltpu.SMEM), hbm, hbm],
        out_specs=(vmem,) * 5,
        scratch_shapes=scratch + [dma((n,)) for n in sems],
        compiler_params=pltpu.CompilerParams(
            collective_id=0, has_side_effects=True, vmem_limit_bytes=40 * 1024 * 1024
        ),
    )(
        far(jnp.swapaxes(query_rows, 1, 2)),
        far(jnp.swapaxes(key_rows, 1, 2)),
        far(jnp.swapaxes(value_rows, 1, 2)),
        far(segments),
        lengths,
        far(out_weight),
        far(target),
    )
    dq, dk, dv, wg, st = pl.pallas_call(
        write_out,
        out_shape=results,
        in_specs=[pl.BlockSpec(memory_space=pl.ANY)] * 5,
        out_specs=(hbm,) * 5,
        scratch_shapes=[dma((5,))],
        compiler_params=pltpu.CompilerParams(vmem_limit_bytes=2 * 1024 * 1024),
    )(*grads)
    return (
        jnp.swapaxes(dq, 1, 2),
        jnp.swapaxes(dk, 1, 2),
        jnp.swapaxes(dv, 1, 2),
        wg,
        st[0, 0],
    )


def solution(mesh):
    torus = Mesh(mesh.devices.reshape(4, 8, 8, 2), ("dp_0", "dp_1", "patch_0", "patch_1"))
    return jax.shard_map(
        functools.partial(step, 4, 8),
        mesh=torus,
        in_specs=(
            P(DP, PATCH, None),
            P(DP, PATCH, None),
            P(DP, PATCH, None),
            P(),
            P(DP, PATCH, None),
            P(DP),
            P(DP, PATCH),
        ),
        out_specs=(P(DP, PATCH, None), P(DP, PATCH, None), P(DP, PATCH, None), P(PATCH, DP), P()),
        check_vma=False,
    )
```

```python
import functools
import math

import jax
import jax.numpy as jnp
from jax import lax
from jax.experimental import pallas as pl
from jax.experimental.pallas import tpu as pltpu
from jax.sharding import Mesh
from jax.sharding import PartitionSpec as P

WIDTH = 1152
HEADS = 8
HEAD_DIM = 72
FEAT = 576
ROWS = 128
PAD = 80
PATCH = ("patch_0", "patch_1")
DP = ("dp_0", "dp_1")
BF = jnp.bfloat16
F32 = jnp.float32
FAR = (4, 3, 5, 2, 6, 1, 7)
NEAR = (1, 7, 2, 6, 3, 5, 4)
LAG = 3
XAT = 3
ZROWS = 48
MASK = 2.0**50


def dot(a, b, ca, cb):
    return lax.dot_general(a, b, (((ca,), (cb,)), ((), ())), preferred_element_type=F32)


def body(
    nx,
    nz,
    q_hbm,
    k_hbm,
    v_hbm,
    seg_hbm,
    len_ref,
    w_hbm,
    t_hbm,
    dq_out,
    dk_out,
    dv_out,
    wg_out,
    st_out,
    q_s,
    k_s,
    v_s,
    seg_s,
    w_s,
    t_s,
    send1,
    recv1,
    ktok,
    vtok,
    qtok,
    dtok,
    p_s,
    ds_s,
    rinv_s,
    send2,
    recv2,
    at_s,
    send3,
    recv3,
    dkv,
    drecv,
    send4,
    recv4,
    g_s,
    pg_s,
    pa_s,
    xsend,
    xrel,
    xacc,
    xin,
    zsend,
    zrecv,
    ysend,
    yrecv,
    stat_s,
    relay,
    load_sem,
    snd,
    rcv,
    r1,
    r1v,
    rls,
    rlr,
    d1r,
    d1vr,
    r3,
    dkr,
    xs,
    xr,
):
    x = lax.axis_index("dp_0")
    z = lax.axis_index("dp_1")
    y = lax.axis_index("patch_0")
    k = lax.axis_index("patch_1")
    other = 1 - k
    p = 2 * y + k
    zh = nz // 2
    scale = 1.0 / math.sqrt(HEAD_DIM)

    loads = [
        pltpu.make_async_copy(src, dst, load_sem.at[n])
        for n, (src, dst) in enumerate(
            (
                (q_hbm, q_s),
                (k_hbm, k_s),
                (seg_hbm, seg_s),
                (v_hbm, v_s),
                (w_hbm, w_s),
                (t_hbm, t_s),
            )
        )
    ]
    for c in loads:
        c.start()

    barrier = pltpu.get_barrier_semaphore()
    for i in range(1, 8):
        peer = lax.rem(y + i, 8)
        pl.semaphore_signal(barrier, inc=1, device_id={"patch_0": peer})
        pl.semaphore_signal(barrier, inc=1, device_id={"patch_0": peer, "patch_1": other})
    pl.semaphore_signal(barrier, inc=1, device_id={"patch_1": other})
    for i in range(1, nx):
        pl.semaphore_signal(barrier, inc=1, device_id={"dp_0": lax.rem(x + i, nx)})
    for i in range(1, nz):
        pl.semaphore_signal(barrier, inc=1, device_id={"dp_1": lax.rem(z + i, nz)})

    def remote(src, dst, ssem, rsem, **where):
        return pltpu.make_async_remote_copy(
            src_ref=src, dst_ref=dst, send_sem=ssem, recv_sem=rsem, device_id=where
        )

    row = lax.broadcasted_iota(jnp.int32, (8, ROWS), 0)
    lane = lax.broadcasted_iota(jnp.int32, (8, ROWS), 1)
    length = len_ref[0]
    live_t = p * ROWS + lane < length
    for c in loads[:4]:
        c.wait()
    code = jnp.where(live_t, jnp.broadcast_to(seg_s[...], (8, ROWS)), 8)
    low = jnp.bitwise_and(row, 3)
    weight = jnp.where(low == 0, 1, jnp.where(low == 1, 2, jnp.where(low == 2, 4, 8)))
    bit = jnp.where(jnp.bitwise_and(code, weight) != 0, 1.0, 0.0).astype(F32)
    mine = jnp.where(row < 4, bit, 1.0 - bit)
    q_mask = -MASK * mine
    k_mask = MASK * (1.0 - mine)
    v_ones = jnp.where(row == 0, 1.0, 0.0).astype(F32)
    for at, (ref, extra) in enumerate(((q_s, q_mask), (k_s, k_mask), (v_s, v_ones))):
        whole = ref[0].astype(F32)
        for h in range(HEADS):
            block = jnp.concatenate([whole[HEAD_DIM * h : HEAD_DIM * (h + 1)], extra], axis=0)
            send1[h, PAD * at : PAD * (at + 1), :] = block.astype(BF)
    recv1[p] = send1[y]

    pl.semaphore_wait(barrier, 15 + (nx - 1) + (nz - 1))

    qk = pl.ds(0, 2 * PAD)
    ko = pl.ds(PAD, PAD)
    vo = pl.ds(2 * PAD, PAD)

    two_on = lax.rem(y + 2, 8)

    def spread(rows, n, rsem):
        for i in FAR:
            h = lax.rem(y + i, 8)
            direct = remote(
                send1.at[h, rows], recv1.at[p, rows], snd.at[n], rsem.at[i], patch_0=h
            )
            if i != 4:
                direct.start()
                continue

            @pl.when(k == 0)
            def _():
                direct.start()

            @pl.when(k == 1)
            def _():
                remote(
                    send1.at[h, rows], relay.at[rows], snd.at[n], rlr.at[n], patch_0=two_on
                ).start()

    def relay_on(rows, n, rsem):
        at = recv1.at[2 * lax.rem(y + 6, 8) + k, rows]
        return remote(relay.at[rows], at, rls.at[n], rsem.at[4], patch_0=two_on)

    def relay_in(rows, n, rsem):
        @pl.when(k == 1)
        def _():
            remote(relay.at[rows], relay.at[rows], rls.at[n], rlr.at[n], patch_0=y).wait_recv()
            relay_on(rows, n, rsem).start()

    def block_in(i, rows, rsem):
        b = recv1.at[2 * source(i) + k, rows]
        remote(b, b, snd.at[0], rsem.at[i], patch_0=y).wait_recv()

    spread(qk, 0, r1)
    spread(vo, 1, r1v)

    def source(i):
        return lax.rem(y - i + 8, 8)

    def pass_on(i, rows, n, rsem):
        ref = recv1.at[2 * source(i) + k, rows]
        return remote(ref, ref, snd.at[n], rsem.at[i], patch_1=other)

    def token_major(dst, b, part, at):
        at = pl.ds(pl.multiple_of(at * ROWS, ROWS), ROWS)
        dst[at, :] = recv1[b, PAD * part : PAD * (part + 1), :].astype(F32).T.astype(BF)

    passed = [pass_on(i, ko, 2, d1r) for i in range(8)]
    passed_v = [pass_on(i, vo, 3, d1vr) for i in range(8)]
    passed[0].start()
    passed_v[0].start()
    token_major(ktok, p, 1, p)
    for i in NEAR:
        if i == 2:
            relay_in(qk, 0, r1)
        block_in(i, qk, r1)
        passed[i].start()
        b = 2 * source(i) + k
        token_major(ktok, b, 1, b)
    relay_in(vo, 1, r1v)
    for i in (0,) + NEAR:
        passed[i].wait_recv()
        b = 2 * source(i) + other
        token_major(ktok, b, 1, b)

    factor = scale * math.log2(math.e)
    pair = y // 2
    mate = y + 1 - 2 * lax.rem(y, 2)

    def forward(j, carry):
        queries = jnp.concatenate([recv1[4 * j + k, 0:PAD, :], recv1[4 * j + 2 + k, 0:PAD, :]], axis=1)
        scores = dot(ktok[...], queries, 1, 0)
        top = jnp.max(scores, axis=0, keepdims=True)
        p_s[j] = jnp.exp2((scores - top) * factor).astype(BF)
        return carry

    lax.fori_loop(0, 4, forward, 0)
    for i in NEAR:
        block_in(i, vo, r1v)
        passed_v[i].start()
    for i in (0,) + NEAR:
        passed_v[i].wait_recv()

    def send_attn(s):
        return remote(send2.at[s], recv2.at[y], snd.at[4], rcv.at[0], patch_0=s)

    for step_at in (2, 1, 3, 0):
        j = lax.rem(pair + step_at, 4)
        values = jnp.concatenate([recv1[b, 2 * PAD : 3 * PAD, :] for b in range(16)], axis=1)
        accum = dot(values, p_s[j], 1, 0)
        rinv = 1.0 / accum[HEAD_DIM : HEAD_DIM + 1, :]
        rinv_s[j] = jnp.broadcast_to(rinv, (8, 2 * ROWS))
        attn = (accum * rinv).astype(BF)
        send2[2 * j] = attn[:, :ROWS]
        send2[2 * j + 1] = attn[:, ROWS:]
        if step_at:
            send_attn(2 * j).start()
            send_attn(2 * j + 1).start()
        else:
            send_attn(mate).start()
    recv2[y] = send2[y]

    def backward_layouts(b, carry):
        token_major(vtok, b, 2, b)
        return carry

    lax.fori_loop(0, 16, backward_layouts, 0)

    def query_layouts(src, carry):
        token_major(qtok, 2 * src + k, 0, src)
        return carry

    lax.fori_loop(0, 8, query_layouts, 0)

    loads[4].wait()
    loads[5].wait()
    seven = pl.ds(0, 7)
    remote(send2.at[seven], recv2.at[seven], snd.at[4], rcv.at[0], patch_0=y).wait_recv()
    for h in range(HEADS):
        at_s[HEAD_DIM * h : HEAD_DIM * (h + 1), :] = recv2[h].astype(F32)[:HEAD_DIM]
    attn_t = at_s[...].astype(BF)
    pa_s[0] = attn_t
    swap_a = remote(pa_s.at[0], pa_s.at[1], snd.at[5], rcv.at[1], patch_1=other)
    swap_a.start()
    output = dot(attn_t, w_s[...], 0, 0)
    token = lax.broadcasted_iota(jnp.int32, (ROWS, WIDTH), 0)
    live = p * ROWS + token < length
    error = jnp.where(live, output - t_s[0].astype(F32), 0.0)
    grad_out = (2.0 * error).astype(BF)
    grad_attn = dot(w_s[...], grad_out, 1, 1)
    for h in range(HEADS):
        block = jnp.concatenate(
            [grad_attn[HEAD_DIM * h : HEAD_DIM * (h + 1)], jnp.zeros((8, ROWS), F32)], axis=0
        )
        send3[h] = block.astype(BF)
    for i in FAR:
        to = lax.rem(y + i, 8)
        remote(send3.at[to], recv3.at[y], snd.at[6], r3.at[i], patch_0=to).start()
    recv3[y] = send3[y]

    grad_t = (2.0 * error).T.astype(BF)
    part = WIDTH // (2 * nx)
    for half in range(2):
        for xx in range(nx):
            at = (2 * xx + half) * part
            g_s[half, part * xx : part * (xx + 1), :] = grad_t[at : at + part]
    swap_g = remote(g_s.at[other], pg_s, snd.at[7], rcv.at[2], patch_1=other)
    swap_g.start()
    squares = jnp.sum(error * error)
    cell = lax.broadcasted_iota(jnp.int32, (8, ROWS), 1)
    stat_s[0] = jnp.where(
        cell == 0, squares, jnp.where(cell == 1, length.astype(F32), 0.0)
    )

    def stat_send(stage, base, n, me, to):
        for i in range(1, n):
            remote(
                stat_s.at[stage],
                stat_s.at[base + i],
                snd.at[8 + stage],
                rcv.at[3 + stage],
                **to(lax.rem(me + i, n)),
            ).start()

    def stat_all(stage, base, n):
        slots = stat_s.at[pl.ds(base + 1, n - 1)]
        return remote(slots, slots, snd.at[8 + stage], rcv.at[3 + stage], patch_0=y)

    def stat_sum(stage, base, n):
        stat_all(stage, base, n).wait_recv()
        acc = stat_s[stage]
        for i in range(1, n):
            acc = acc + stat_s[base + i]
        return acc

    stat_send(0, 3, 16, p, lambda t: {"patch_0": t // 2, "patch_1": lax.rem(t, 2)})
    swap_a.wait_recv()
    swap_g.wait_recv()
    left = jnp.concatenate([g_s[k], pg_s[...]], axis=1)
    right = jnp.concatenate([pa_s[0], pa_s[1]], axis=1)
    partial = dot(left, right, 1, 1)
    for xx in range(nx):
        xsend[xx] = partial[part * xx : part * (xx + 1)].astype(BF)
    lo, hi = pl.ds(0, 80), pl.ds(80, 64)
    up, down, across = lax.rem(x + 1, 4), lax.rem(x + 3, 4), lax.rem(x + 2, 4)
    xring = [
        remote(xsend.at[across, lo], xrel.at[lo], xs.at[0], xr.at[0], dp_0=up),
        remote(xsend.at[across, hi], xrel.at[hi], xs.at[1], xr.at[1], dp_0=down),
        remote(xsend.at[up, hi], xin.at[0, hi], xs.at[2], xr.at[2], dp_0=up),
        remote(xsend.at[down, lo], xin.at[1, lo], xs.at[3], xr.at[3], dp_0=down),
        remote(xacc.at[lo], xin.at[0, lo], xs.at[4], xr.at[4], dp_0=up),
        remote(xacc.at[hi], xin.at[1, hi], xs.at[5], xr.at[5], dp_0=down),
    ]
    for c in xring[:4]:
        c.start()

    def x_relay():
        for n, (rows, size, to) in enumerate(((0, 80, up), (80, 64, down))):
            xring[n].wait_recv()
            xacc[rows : rows + size, :] = (
                xsend[to, rows : rows + size, :].astype(F32)
                + xrel[rows : rows + size, :].astype(F32)
            ).astype(BF)
            xring[4 + n].start()

    def send_grad(s, rows, n):
        return remote(
            send4.at[s, rows], recv4.at[y, rows], snd.at[n], rcv.at[n], patch_0=s
        )

    qo = pl.ds(0, PAD)
    kvo = pl.ds(PAD, 2 * PAD)

    def third_in(s):
        i = lax.rem(y - s + 8, 8)
        remote(send3.at[y], recv3.at[s], snd.at[6], r3.at[i], patch_0=y).wait_recv()

    for step_at in (0, 1, 3, 2):
        j = lax.rem(pair + step_at, 4)
        if step_at:
            third_in(2 * j)
            third_in(2 * j + 1)
        else:
            third_in(mate)
        grads = jnp.concatenate([recv3[2 * j], recv3[2 * j + 1]], axis=1).astype(F32)
        folded = grads * rinv_s[j, 0:1, :]
        dtok[pl.ds(pl.multiple_of(j * 2 * ROWS, 2 * ROWS), 2 * ROWS), :] = folded.T.astype(BF)
        folded = folded.astype(BF)
        attn = jnp.concatenate([send2[2 * j], send2[2 * j + 1]], axis=1)
        delta = jnp.sum(folded.astype(F32) * attn.astype(F32), axis=0, keepdims=True)
        dprobs = dot(vtok[...], folded, 1, 0)
        dscores = (p_s[j].astype(F32) * (dprobs - delta)).astype(BF)
        ds_s[j] = dscores
        keys = jnp.concatenate([recv1[b, PAD : 2 * PAD, :] for b in range(16)], axis=1)
        dq = (dot(keys, dscores, 1, 0) * scale).astype(BF)
        send4[2 * j, 0:PAD, :] = dq[:, :ROWS]
        send4[2 * j + 1, 0:PAD, :] = dq[:, ROWS:]
        if step_at:
            send_grad(2 * j, qo, 11).start()
            send_grad(2 * j + 1, qo, 11).start()
        else:
            send_grad(mate, qo, 11).start()
        if step_at == 1:
            x_relay()

    stat_s[1] = stat_sum(0, 3, 16)
    stat_send(1, 19, nx, x, lambda t: {"dp_0": t})

    def crossing(t):
        i = lax.rem(t - y + 8, 8)
        return remote(dkv.at[other, t], drecv.at[t], snd.at[13], dkr.at[i], patch_1=other)

    def join(t, away):
        crossing(t).wait_recv()
        send4[t, PAD : 3 * PAD, :] = (
            dkv[k, t].astype(F32) + drecv[t].astype(F32)
        ).astype(BF)
        if away:
            send_grad(t, kvo, 12).start()

    cols = part // zh
    active = z // zh == k

    def x_done():
        stat_s[2] = stat_sum(1, 19, nx)
        stat_send(2, 19 + nx, nz, z, lambda t: {"dp_1": t})
        for c in xring[2:]:
            c.wait_recv()
        total = xsend[x].astype(F32) + xin[0].astype(F32) + xin[1].astype(F32)
        for j in range(zh):
            zsend[j, 0:cols, :] = total[cols * j : cols * (j + 1)].astype(BF)
        for j in range(zh):
            to = zh * k + j
            away = lax.rem(to - z + nz, nz)

            @pl.when(to != z)
            def _():
                remote(
                    zsend.at[j, zrows], zrecv.at[away, zrows], snd.at[14], rcv.at[6], dp_1=to
                ).start()

        @pl.when(active)
        def _():
            zrecv[0] = zsend[lax.rem(z, zh)]

    zrows = pl.ds(0, ZROWS)
    order = FAR + (0,)
    for n, i in enumerate(order):
        t = lax.rem(y + i, 8)
        at = pl.ds(pl.multiple_of(t * 2 * ROWS, 2 * ROWS), 2 * ROWS)
        ds_rows = jnp.concatenate([ds_s[j, at, :] for j in range(4)], axis=1)
        p_rows = jnp.concatenate([p_s[j, at, :] for j in range(4)], axis=1)
        dk = (dot(ds_rows, qtok[...], 1, 0) * scale).T.astype(BF)
        dv = dot(p_rows, dtok[...], 1, 0).T.astype(BF)
        for c in range(2):
            dkv[c, t, 0:PAD, :] = dk[:, ROWS * c : ROWS * (c + 1)]
            dkv[c, t, PAD : 2 * PAD, :] = dv[:, ROWS * c : ROWS * (c + 1)]
        crossing(t).start()
        if n == XAT:
            x_done()
        if n >= LAG:
            join(lax.rem(y + order[n - LAG], 8), order[n - LAG])
    for i in order[8 - LAG :]:
        join(lax.rem(y + i, 8), i)

    recv4[y] = send4[y]

    @pl.when(active)
    def _():
        z_all = zrecv.at[pl.ds(1, nz - 1), zrows]
        remote(z_all, z_all, snd.at[14], rcv.at[6], patch_0=y).wait_recv()
        summed = zrecv[0].astype(F32)
        for i in range(1, nz):
            summed = summed + zrecv[i].astype(F32)
        for t in range(16):
            piece = summed[:, 36 * t : 36 * (t + 1)]
            ysend[t, :, 0:108] = jnp.concatenate(
                [piece[0:16], piece[16:32], piece[32:48]], axis=1
            )

    for t in range(16):

        @pl.when(active & (p != t))
        def _():
            remote(
                ysend.at[t], yrecv.at[y], snd.at[15], rcv.at[7], patch_0=t // 2, patch_1=t % 2
            ).start()

    @pl.when(active)
    def _():
        yrecv[y] = ysend[p]

    acc = stat_sum(2, 19 + nx, nz)
    count = acc[0:1, 1:2] / 16.0
    ratio = (nx * nz * 16.0 * ROWS) / count
    st_out[...] = acc[0:1, 0:1] / (count * WIDTH)

    def grad_all(rows, n):
        blocks = recv4.at[seven, rows]
        return remote(blocks, blocks, snd.at[n], rcv.at[n], patch_0=y)

    def emit(at, out):
        whole = jnp.concatenate(
            [
                recv4[h, PAD * at : PAD * (at + 1), :].astype(F32)[:HEAD_DIM]
                for h in range(HEADS)
            ],
            axis=0,
        )
        out[0] = whole * ratio

    grad_all(qo, 11).wait_recv()
    emit(0, dq_out)
    grad_all(kvo, 12).wait_recv()
    emit(1, dk_out)
    emit(2, dv_out)

    def y_all(n):
        blocks = yrecv.at[pl.ds(0, n)]
        return remote(blocks, blocks, snd.at[15], rcv.at[7], patch_0=y)

    @pl.when(active)
    def _():
        y_all(7).wait_recv()

    @pl.when(jnp.logical_not(active))
    def _():
        y_all(8).wait_recv()

    final = yrecv[0]
    for i in range(1, 8):
        final = final + yrecv[i]
    final = jnp.concatenate([final[:, 0:36], final[:, 36:72], final[:, 72:108]], axis=0)
    wg_out[...] = final.T[0:36, 0:36] * (ratio / (16.0 * ROWS))

    def drain(ref, n):
        remote(ref, ref, snd.at[n], rcv.at[0], patch_0=y).wait_send()

    drain(send1.at[seven, qk], 0)
    drain(send1.at[seven, vo], 1)
    drain(send1.at[:, ko], 2)
    drain(send1.at[:, vo], 3)
    drain(send2.at[seven], 4)
    drain(pa_s.at[0], 5)
    drain(send3.at[seven], 6)
    drain(pg_s, 7)
    stat_all(0, 3, 16).wait_send()
    stat_all(1, 19, nx).wait_send()
    stat_all(2, 19 + nx, nz).wait_send()
    drain(send4.at[seven, qo], 11)
    drain(send4.at[seven, kvo], 12)
    drain(drecv, 13)
    for c in xring:
        c.wait_send()

    @pl.when(k == 1)
    def _():
        relay_on(qk, 0, r1).wait_send()
        relay_on(vo, 1, r1v).wait_send()

    @pl.when(active)
    def _():
        drain(zsend.at[pl.ds(0, zh - 1), zrows], 14)
        drain(ysend.at[pl.ds(0, 15)], 15)

    @pl.when(jnp.logical_not(active))
    def _():
        drain(zsend.at[:, zrows], 14)


def write_out(*refs):
    n = len(refs) // 2
    copies = [
        pltpu.make_async_copy(refs[i], refs[n + i], refs[-1].at[i]) for i in range(n)
    ]
    for c in copies:
        c.start()
    for c in copies:
        c.wait()


def step(nx, nz, query_rows, key_rows, value_rows, out_weight, target, lengths, segments):
    part = WIDTH // (2 * nx)
    zh = nz // 2
    dma = pltpu.SemaphoreType.DMA
    scratch = [
        pltpu.VMEM((1, FEAT, ROWS), BF),
        pltpu.VMEM((1, FEAT, ROWS), BF),
        pltpu.VMEM((1, FEAT, ROWS), BF),
        pltpu.VMEM((1, ROWS), jnp.int32),
        pltpu.VMEM((FEAT, WIDTH), BF),
        pltpu.VMEM((1, ROWS, WIDTH), BF),
        pltpu.VMEM((8, 3 * PAD, ROWS), BF),
        pltpu.VMEM((16, 3 * PAD, ROWS), BF),
        pltpu.VMEM((2048, PAD), BF),
        pltpu.VMEM((2048, PAD), BF),
        pltpu.VMEM((1024, PAD), BF),
        pltpu.VMEM((1024, PAD), BF),
        pltpu.VMEM((4, 2048, 256), BF),
        pltpu.VMEM((4, 2048, 256), BF),
        pltpu.VMEM((4, 8, 256), F32),
        pltpu.VMEM((8, PAD, ROWS), BF),
        pltpu.VMEM((8, PAD, ROWS), BF),
        pltpu.VMEM((FEAT, ROWS), F32),
        pltpu.VMEM((8, PAD, ROWS), BF),
        pltpu.VMEM((8, PAD, ROWS), BF),
        pltpu.VMEM((2, 8, 2 * PAD, ROWS), BF),
        pltpu.VMEM((8, 2 * PAD, ROWS), BF),
        pltpu.VMEM((8, 3 * PAD, ROWS), BF),
        pltpu.VMEM((8, 3 * PAD, ROWS), BF),
        pltpu.VMEM((2, FEAT, ROWS), BF),
        pltpu.VMEM((FEAT, ROWS), BF),
        pltpu.VMEM((2, FEAT, ROWS), BF),
        pltpu.VMEM((nx, part, FEAT), BF),
        pltpu.VMEM((part, FEAT), BF),
        pltpu.VMEM((part, FEAT), BF),
        pltpu.VMEM((2, part, FEAT), BF),
        pltpu.VMEM((zh, 48, FEAT), BF),
        pltpu.VMEM((nz, 48, FEAT), BF),
        pltpu.VMEM((16, 16, 128), F32),
        pltpu.VMEM((8, 16, 128), F32),
        pltpu.VMEM((19 + nx + nz, 8, ROWS), F32),
        pltpu.VMEM((3 * PAD, ROWS), BF),
    ]
    sems = [6, 16, 13, 8, 8, 2, 2, 8, 8, 8, 8, 6, 6]
    vmem = pl.BlockSpec(memory_space=pltpu.VMEM)
    hbm = pl.BlockSpec(memory_space=pltpu.HBM)
    wide = jax.ShapeDtypeStruct((1, FEAT, ROWS), F32)
    results = (
        wide,
        wide,
        wide,
        jax.ShapeDtypeStruct((36, 36), F32),
        jax.ShapeDtypeStruct((1, 1), F32),
    )
    far = lambda a: pltpu.with_memory_space_constraint(a, pltpu.HBM)
    grads = pl.pallas_call(
        functools.partial(body, nx, nz),
        out_shape=results,
        in_specs=[hbm] * 4 + [pl.BlockSpec(memory_space=pltpu.SMEM), hbm, hbm],
        out_specs=(vmem,) * 5,
        scratch_shapes=scratch + [dma((n,)) for n in sems],
        compiler_params=pltpu.CompilerParams(
            collective_id=0, has_side_effects=True, vmem_limit_bytes=40 * 1024 * 1024
        ),
    )(
        far(jnp.swapaxes(query_rows, 1, 2)),
        far(jnp.swapaxes(key_rows, 1, 2)),
        far(jnp.swapaxes(value_rows, 1, 2)),
        far(segments),
        lengths,
        far(out_weight),
        far(target),
    )
    dq, dk, dv, wg, st = pl.pallas_call(
        write_out,
        out_shape=results,
        in_specs=[pl.BlockSpec(memory_space=pl.ANY)] * 5,
        out_specs=(hbm,) * 5,
        scratch_shapes=[dma((5,))],
        compiler_params=pltpu.CompilerParams(vmem_limit_bytes=2 * 1024 * 1024),
    )(*grads)
    return (
        jnp.swapaxes(dq, 1, 2),
        jnp.swapaxes(dk, 1, 2),
        jnp.swapaxes(dv, 1, 2),
        wg,
        st[0, 0],
    )


def solution(mesh):
    torus = Mesh(mesh.devices.reshape(4, 8, 8, 2), ("dp_0", "dp_1", "patch_0", "patch_1"))
    return jax.shard_map(
        functools.partial(step, 4, 8),
        mesh=torus,
        in_specs=(
            P(DP, PATCH, None),
            P(DP, PATCH, None),
            P(DP, PATCH, None),
            P(),
            P(DP, PATCH, None),
            P(DP),
            P(DP, PATCH),
        ),
        out_specs=(P(DP, PATCH, None), P(DP, PATCH, None), P(DP, PATCH, None), P(PATCH, DP), P()),
        check_vma=False,
    )
```

```python
import functools
import math

import jax
import jax.numpy as jnp
from jax import lax
from jax.experimental import pallas as pl
from jax.experimental.pallas import tpu as pltpu
from jax.sharding import Mesh
from jax.sharding import PartitionSpec as P

WIDTH = 1152
HEADS = 8
HEAD_DIM = 72
FEAT = 576
ROWS = 128
PAD = 80
PATCH = ("patch_0", "patch_1")
DP = ("dp_0", "dp_1")
BF = jnp.bfloat16
F32 = jnp.float32
FAR = (4, 3, 5, 2, 6, 1, 7)
NEAR = (1, 7, 2, 6, 3, 5, 4)
XAT = 2
MASK = 2.0**50


def dot(a, b, ca, cb):
    return lax.dot_general(a, b, (((ca,), (cb,)), ((), ())), preferred_element_type=F32)


def body(
    nx,
    nz,
    q_hbm,
    k_hbm,
    v_hbm,
    seg_hbm,
    len_ref,
    w_hbm,
    t_hbm,
    dq_out,
    dk_out,
    dv_out,
    wg_out,
    st_out,
    q_s,
    k_s,
    v_s,
    seg_s,
    w_s,
    t_s,
    send1,
    recv1,
    ktok,
    vtok,
    qtok,
    dtok,
    p_s,
    ds_s,
    rinv_s,
    send2,
    recv2,
    at_s,
    send3,
    recv3,
    dkv,
    drecv,
    send4,
    recv4,
    g_s,
    pg_s,
    pa_s,
    xsend,
    xrel,
    xacc,
    xin,
    zsend,
    zrecv,
    ysend,
    yrecv,
    stat_s,
    s_s,
    top_s,
    acc_s,
    load_sem,
    snd,
    rcv,
    r1,
    r1v,
    d1r,
    d1vr,
    r3,
    dkr,
    xs,
    xr,
):
    x = lax.axis_index("dp_0")
    z = lax.axis_index("dp_1")
    y = lax.axis_index("patch_0")
    k = lax.axis_index("patch_1")
    other = 1 - k
    p = 2 * y + k
    zh = nz // 2
    scale = 1.0 / math.sqrt(HEAD_DIM)

    loads = [
        pltpu.make_async_copy(src, dst, load_sem.at[n])
        for n, (src, dst) in enumerate(
            (
                (q_hbm, q_s),
                (k_hbm, k_s),
                (seg_hbm, seg_s),
                (v_hbm, v_s),
                (w_hbm, w_s),
                (t_hbm, t_s),
            )
        )
    ]
    for c in loads:
        c.start()

    barrier = pltpu.get_barrier_semaphore()
    for i in range(1, 8):
        peer = lax.rem(y + i, 8)
        pl.semaphore_signal(barrier, inc=1, device_id={"patch_0": peer})
        pl.semaphore_signal(barrier, inc=1, device_id={"patch_0": peer, "patch_1": other})
    pl.semaphore_signal(barrier, inc=1, device_id={"patch_1": other})
    for i in range(1, nx):
        pl.semaphore_signal(barrier, inc=1, device_id={"dp_0": lax.rem(x + i, nx)})
    for i in range(1, nz):
        pl.semaphore_signal(barrier, inc=1, device_id={"dp_1": lax.rem(z + i, nz)})

    def remote(src, dst, ssem, rsem, **where):
        return pltpu.make_async_remote_copy(
            src_ref=src, dst_ref=dst, send_sem=ssem, recv_sem=rsem, device_id=where
        )

    row = lax.broadcasted_iota(jnp.int32, (8, ROWS), 0)
    lane = lax.broadcasted_iota(jnp.int32, (8, ROWS), 1)
    length = len_ref[0]
    live_t = p * ROWS + lane < length
    for c in loads[:4]:
        c.wait()
    code = jnp.where(live_t, jnp.broadcast_to(seg_s[...], (8, ROWS)), 8)
    low = jnp.bitwise_and(row, 3)
    weight = jnp.where(low == 0, 1, jnp.where(low == 1, 2, jnp.where(low == 2, 4, 8)))
    bit = jnp.where(jnp.bitwise_and(code, weight) != 0, 1.0, 0.0).astype(F32)
    mine = jnp.where(row < 4, bit, 1.0 - bit)
    q_mask = -MASK * mine
    k_mask = MASK * (1.0 - mine)
    v_ones = jnp.where(row == 0, 1.0, 0.0).astype(F32)
    for at, (ref, extra) in enumerate(((q_s, q_mask), (k_s, k_mask), (v_s, v_ones))):
        whole = ref[0].astype(F32)
        for h in range(HEADS):
            block = jnp.concatenate([whole[HEAD_DIM * h : HEAD_DIM * (h + 1)], extra], axis=0)
            send1[h, PAD * at : PAD * (at + 1), :] = block.astype(BF)
    recv1[0, y] = send1[y]

    recv3[...] = jnp.zeros_like(recv3)
    pl.semaphore_wait(barrier, 15 + (nx - 1) + (nz - 1))

    qk = pl.ds(0, 2 * PAD)
    ko = pl.ds(PAD, PAD)
    vo = pl.ds(2 * PAD, PAD)

    def spread(rows, n, rsem):
        for i in FAR:
            h = lax.rem(y + i, 8)
            remote(
                send1.at[h, rows], recv1.at[0, y, rows], snd.at[n], rsem.at[i], patch_0=h
            ).start()

    def block_in(i, rows, rsem):
        b = recv1.at[0, source(i), rows]
        remote(b, b, snd.at[0], rsem.at[i], patch_0=y).wait_recv()

    spread(qk, 0, r1)
    spread(vo, 1, r1v)

    def source(i):
        return lax.rem(y - i + 8, 8)

    def pass_on(i, rows, n, rsem):
        return remote(
            recv1.at[0, source(i), rows],
            recv1.at[1, source(i), rows],
            snd.at[n],
            rsem.at[i],
            patch_1=other,
        )

    def token_major(dst, c, src, part):
        at = pl.ds(pl.multiple_of((8 * c + src) * ROWS, ROWS), ROWS)
        dst[at, :] = recv1[c, src, PAD * part : PAD * (part + 1), :].astype(F32).T.astype(BF)

    passed = [pass_on(i, ko, 2, d1r) for i in range(8)]
    passed_v = [pass_on(i, vo, 3, d1vr) for i in range(8)]
    passed[0].start()
    passed_v[0].start()
    token_major(ktok, 0, y, 1)
    for i in NEAR:
        block_in(i, qk, r1)
        passed[i].start()
        token_major(ktok, 0, source(i), 1)

    factor = scale * math.log2(math.e)
    pair = y // 2
    mate = y + 1 - 2 * lax.rem(y, 2)
    half = 8 * ROWS

    def queries(j):
        return jnp.concatenate([recv1[0, 2 * j, 0:PAD, :], recv1[0, 2 * j + 1, 0:PAD, :]], axis=1)

    def forward_own(j, carry):
        scores = dot(ktok[0:half, :], queries(j), 1, 0)
        s_s[j] = scores
        top_s[j] = jnp.broadcast_to(jnp.max(scores, axis=0, keepdims=True), (8, 2 * ROWS))
        return carry

    lax.fori_loop(0, 4, forward_own, 0)
    for i in (0,) + NEAR:
        passed[i].wait_recv()
        token_major(ktok, 1, source(i), 1)

    def forward_other(j, carry):
        scores = dot(ktok[half : 2 * half, :], queries(j), 1, 0)
        top = jnp.maximum(top_s[j, 0:1, :], jnp.max(scores, axis=0, keepdims=True))
        p_s[j, half : 2 * half, :] = jnp.exp2((scores - top) * factor).astype(BF)
        p_s[j, 0:half, :] = jnp.exp2((s_s[j] - top) * factor).astype(BF)
        return carry

    lax.fori_loop(0, 4, forward_other, 0)
    for i in NEAR:
        block_in(i, vo, r1v)
        passed_v[i].start()

    def lanes(c, part):
        return jnp.concatenate(
            [recv1[c, src, PAD * part : PAD * (part + 1), :] for src in range(8)], axis=1
        )

    def values_own(j, carry):
        acc_s[j] = dot(lanes(0, 2), p_s[j, 0:half, :], 1, 0)
        return carry

    lax.fori_loop(0, 4, values_own, 0)
    for i in (0,) + NEAR:
        passed_v[i].wait_recv()

    head = pl.ds(0, HEAD_DIM)

    def send_attn(s):
        return remote(
            send2.at[s, head], recv2.at[y, head], snd.at[4], rcv.at[0], patch_0=s
        )

    for step_at in (2, 1, 3, 0):
        j = lax.rem(pair + step_at, 4)
        accum = acc_s[j] + dot(lanes(1, 2), p_s[j, half : 2 * half, :], 1, 0)
        rinv = 1.0 / accum[HEAD_DIM : HEAD_DIM + 1, :]
        rinv_s[j] = jnp.broadcast_to(rinv, (8, 2 * ROWS))
        attn = (accum * rinv).astype(BF)
        send2[2 * j] = attn[:, :ROWS]
        send2[2 * j + 1] = attn[:, ROWS:]
        if step_at:
            send_attn(2 * j).start()
            send_attn(2 * j + 1).start()
        else:
            send_attn(mate).start()
    recv2[y] = send2[y]

    def backward_layouts(src, carry):
        token_major(vtok, 0, src, 2)
        token_major(vtok, 1, src, 2)
        token_major(qtok, 0, src, 0)
        return carry

    lax.fori_loop(0, 8, backward_layouts, 0)

    loads[4].wait()
    loads[5].wait()
    seven = pl.ds(0, 7)
    remote(
        send2.at[seven, head], recv2.at[seven, head], snd.at[4], rcv.at[0], patch_0=y
    ).wait_recv()
    for h in range(HEADS):
        at_s[HEAD_DIM * h : HEAD_DIM * (h + 1), :] = recv2[h].astype(F32)[:HEAD_DIM]
    attn_t = at_s[...].astype(BF)
    pa_s[0] = attn_t
    swap_a = remote(pa_s.at[0], pa_s.at[1], snd.at[5], rcv.at[1], patch_1=other)
    swap_a.start()
    output = dot(attn_t, w_s[...], 0, 0)
    token = lax.broadcasted_iota(jnp.int32, (ROWS, WIDTH), 0)
    live = p * ROWS + token < length
    error = jnp.where(live, output - t_s[0].astype(F32), 0.0)
    grad_out = (2.0 * error).astype(BF)
    grad_t = (2.0 * error).T.astype(BF)
    part = WIDTH // (2 * nx)
    for zhalf in range(2):
        for xx in range(nx):
            at = (2 * xx + zhalf) * part
            g_s[zhalf, part * xx : part * (xx + 1), :] = grad_t[at : at + part]
    swap_g = remote(g_s.at[other], pg_s, snd.at[7], rcv.at[2], patch_1=other)
    swap_g.start()
    grad_attn = dot(w_s[...], grad_t, 1, 0)
    for h in range(HEADS):
        block = jnp.concatenate(
            [grad_attn[HEAD_DIM * h : HEAD_DIM * (h + 1)], jnp.zeros((8, ROWS), F32)], axis=0
        )
        send3[h] = block.astype(BF)
    for i in FAR:
        to = lax.rem(y + i, 8)
        remote(
            send3.at[to, head], recv3.at[y, head], snd.at[6], r3.at[i], patch_0=to
        ).start()
    recv3[y, 0:HEAD_DIM, :] = send3[y, 0:HEAD_DIM, :]

    squares = jnp.sum(error * error)
    cell = lax.broadcasted_iota(jnp.int32, (8, ROWS), 1)
    stat_s[0] = jnp.where(
        cell == 0, squares, jnp.where(cell == 1, length.astype(F32), 0.0)
    )

    def stat_send(stage, base, n, me, to):
        for i in range(1, n):
            remote(
                stat_s.at[stage],
                stat_s.at[base + i],
                snd.at[8 + stage],
                rcv.at[3 + stage],
                **to(lax.rem(me + i, n)),
            ).start()

    def stat_all(stage, base, n):
        slots = stat_s.at[pl.ds(base + 1, n - 1)]
        return remote(slots, slots, snd.at[8 + stage], rcv.at[3 + stage], patch_0=y)

    def stat_sum(stage, base, n):
        stat_all(stage, base, n).wait_recv()
        acc = stat_s[stage]
        for i in range(1, n):
            acc = acc + stat_s[base + i]
        return acc

    stat_send(0, 3, 16, p, lambda t: {"patch_0": t // 2, "patch_1": lax.rem(t, 2)})
    swap_a.wait_recv()
    swap_g.wait_recv()
    left = jnp.concatenate([g_s[k], pg_s[...]], axis=1)
    right = jnp.concatenate([pa_s[0], pa_s[1]], axis=1)
    partial = dot(left, right, 1, 1)
    for xx in range(nx):
        chunk = partial[part * xx : part * (xx + 1)]
        rest = jnp.concatenate([chunk[: part // 2, 512:], chunk[part // 2 :, 512:]], axis=1)
        for g in range(4):
            xsend[xx, part * g : part * (g + 1), :] = chunk[:, ROWS * g : ROWS * (g + 1)].astype(BF)
        xsend[xx, 4 * part :, :] = jnp.concatenate([rest, jnp.zeros((8, ROWS), F32)], axis=0).astype(BF)
    lo, hi = pl.ds(0, 336), pl.ds(336, 320)
    up, down, across = lax.rem(x + 1, 4), lax.rem(x + 3, 4), lax.rem(x + 2, 4)
    xring = [
        remote(xsend.at[across, lo], xrel.at[lo], xs.at[0], xr.at[0], dp_0=up),
        remote(xsend.at[across, hi], xrel.at[hi], xs.at[1], xr.at[1], dp_0=down),
        remote(xsend.at[up, hi], xin.at[0, hi], xs.at[2], xr.at[2], dp_0=up),
        remote(xsend.at[down, lo], xin.at[1, lo], xs.at[3], xr.at[3], dp_0=down),
        remote(xacc.at[lo], xin.at[0, lo], xs.at[4], xr.at[4], dp_0=up),
        remote(xacc.at[hi], xin.at[1, hi], xs.at[5], xr.at[5], dp_0=down),
    ]
    for c in xring[:4]:
        c.start()

    def x_relay():
        for n, (rows, size, to) in enumerate(((0, 336, up), (336, 320, down))):
            xring[n].wait_recv()
            xacc[rows : rows + size, :] = (
                xsend[to, rows : rows + size, :].astype(F32)
                + xrel[rows : rows + size, :].astype(F32)
            ).astype(BF)
            xring[4 + n].start()

    def send_grad(s, rows, n):
        return remote(
            send4.at[s, rows], recv4.at[y, rows], snd.at[n], rcv.at[n], patch_0=s
        )

    qo = pl.ds(0, HEAD_DIM)
    kvo = pl.ds(PAD, 2 * HEAD_DIM)

    def third_in(s):
        i = lax.rem(y - s + 8, 8)
        remote(
            send3.at[y, head], recv3.at[s, head], snd.at[6], r3.at[i], patch_0=y
        ).wait_recv()

    for step_at in (0, 1, 3, 2):
        j = lax.rem(pair + step_at, 4)
        if step_at:
            third_in(2 * j)
            third_in(2 * j + 1)
        else:
            third_in(mate)
        grads = jnp.concatenate([recv3[2 * j], recv3[2 * j + 1]], axis=1).astype(F32)
        folded = grads * rinv_s[j, 0:1, :]
        dtok[pl.ds(pl.multiple_of(j * 2 * ROWS, 2 * ROWS), 2 * ROWS), :] = folded.T.astype(BF)
        folded = folded.astype(BF)
        attn = jnp.concatenate([send2[2 * j], send2[2 * j + 1]], axis=1)
        delta = jnp.sum(folded.astype(F32) * attn.astype(F32), axis=0, keepdims=True)
        dprobs = dot(vtok[...], folded, 1, 0)
        dscores = (p_s[j].astype(F32) * (dprobs - delta)).astype(BF)
        ds_s[j] = dscores
        keys = jnp.concatenate([lanes(0, 1), lanes(1, 1)], axis=1)
        dq = (dot(keys, dscores, 1, 0) * scale).astype(BF)
        send4[2 * j, 0:PAD, :] = dq[:, :ROWS]
        send4[2 * j + 1, 0:PAD, :] = dq[:, ROWS:]
        if step_at:
            send_grad(2 * j, qo, 11).start()
            send_grad(2 * j + 1, qo, 11).start()
        else:
            send_grad(mate, qo, 11).start()
        if step_at == 1:
            x_relay()

    stat_s[1] = stat_sum(0, 3, 16)
    stat_send(1, 19, nx, x, lambda t: {"dp_0": t})

    def crossing(u):
        two = pl.ds(2 * u, 2)
        return remote(dkv.at[two], drecv.at[two], snd.at[13], dkr.at[u], patch_1=other)

    def key_grads(c, u):
        at = pl.ds(pl.multiple_of((8 * c + 2 * u) * ROWS, 2 * ROWS), 2 * ROWS)
        ds_rows = jnp.concatenate([ds_s[j, at, :] for j in range(4)], axis=1)
        p_rows = jnp.concatenate([p_s[j, at, :] for j in range(4)], axis=1)
        dk = (dot(ds_rows, qtok[...], 1, 0) * scale).T
        dv = dot(p_rows, dtok[...], 1, 0).T
        return jnp.concatenate([dk[:HEAD_DIM], dv[:HEAD_DIM]], axis=0)

    cols = part // zh
    active = z // zh == k

    def x_done():
        stat_s[2] = stat_sum(1, 19, nx)
        stat_send(2, 19 + nx, nz, z, lambda t: {"dp_1": t})
        for c in xring[2:]:
            c.wait_recv()
        total = xsend[x].astype(F32) + xin[0].astype(F32) + xin[1].astype(F32)
        for j in range(zh):
            rest = total[4 * part + cols * (j % 2) : 4 * part + cols * (j % 2 + 1)]
            rest = rest[:, 64 * (j // 2) : 64 * (j // 2 + 1)]
            rows = [total[part * g + cols * j : part * g + cols * (j + 1)] for g in range(4)]
            rows += [
                jnp.concatenate([rest[: cols // 2], rest[cols // 2 :]], axis=1),
                jnp.zeros((14, ROWS), F32),
            ]
            zsend[j] = jnp.concatenate(rows, axis=0).astype(BF)
        for j in range(zh):
            to = zh * k + j
            away = lax.rem(to - z + nz, nz)

            @pl.when(to != z)
            def _():
                remote(
                    zsend.at[j], zrecv.at[away], snd.at[14], rcv.at[6], dp_1=to
                ).start()

        @pl.when(active)
        def _():
            zrecv[0] = zsend[lax.rem(z, zh)]

    for step_at in (2, 1, 3, 0):
        u = lax.rem(pair + step_at, 4)
        both = key_grads(1, u).astype(BF)
        dkv[2 * u] = both[:, :ROWS]
        dkv[2 * u + 1] = both[:, ROWS:]
        crossing(u).start()
    for step_at in (2, 1, 3, 0):
        u = lax.rem(pair + step_at, 4)
        both = key_grads(0, u)
        crossing(u).wait_recv()
        for c in range(2):
            mine = both[:, ROWS * c : ROWS * (c + 1)]
            send4[2 * u + c, PAD:, :] = (mine + drecv[2 * u + c].astype(F32)).astype(BF)
        if step_at:
            send_grad(2 * u, kvo, 12).start()
            send_grad(2 * u + 1, kvo, 12).start()
        else:
            send_grad(mate, kvo, 12).start()
        if step_at == XAT:
            x_done()

    recv4[y] = send4[y]

    @pl.when(active)
    def _():
        z_all = zrecv.at[pl.ds(1, nz - 1)]
        remote(z_all, z_all, snd.at[14], rcv.at[6], patch_0=y).wait_recv()
        summed = zrecv[0].astype(F32)
        for i in range(1, nz):
            summed = summed + zrecv[i].astype(F32)
        rest = summed[4 * cols : 4 * cols + cols // 2]
        summed = jnp.concatenate(
            [summed[cols * g : cols * (g + 1)] for g in range(4)]
            + [jnp.concatenate([rest[:, :64], rest[:, 64:]], axis=0)],
            axis=1,
        )
        summed = jnp.concatenate([summed, jnp.zeros((48 - cols, FEAT), F32)], axis=0)
        for t in range(16):
            piece = summed[:, 36 * t : 36 * (t + 1)]
            ysend[t, :, 0:108] = jnp.concatenate(
                [piece[0:16], piece[16:32], piece[32:48]], axis=1
            )

    for t in range(16):

        @pl.when(active & (p != t))
        def _():
            remote(
                ysend.at[t], yrecv.at[y], snd.at[15], rcv.at[7], patch_0=t // 2, patch_1=t % 2
            ).start()

    @pl.when(active)
    def _():
        yrecv[y] = ysend[p]

    acc = stat_sum(2, 19 + nx, nz)
    count = acc[0:1, 1:2] / 16.0
    ratio = (nx * nz * 16.0 * ROWS) / count
    st_out[...] = acc[0:1, 0:1] / (count * WIDTH)

    def grad_all(rows, n):
        blocks = recv4.at[seven, rows]
        return remote(blocks, blocks, snd.at[n], rcv.at[n], patch_0=y)

    def emit(start, out):
        rows = slice(start // 16 * 16, (start // 16 + 5) * 16)
        skip = start % 16
        whole = jnp.concatenate(
            [recv4[h, rows, :].astype(F32)[skip : skip + HEAD_DIM] for h in range(HEADS)],
            axis=0,
        )
        out[0] = whole * ratio

    grad_all(qo, 11).wait_recv()
    emit(0, dq_out)
    grad_all(kvo, 12).wait_recv()
    emit(PAD, dk_out)
    emit(PAD + HEAD_DIM, dv_out)

    def y_all(n):
        blocks = yrecv.at[pl.ds(0, n)]
        return remote(blocks, blocks, snd.at[15], rcv.at[7], patch_0=y)

    @pl.when(active)
    def _():
        y_all(7).wait_recv()

    @pl.when(jnp.logical_not(active))
    def _():
        y_all(8).wait_recv()

    final = yrecv[0]
    for i in range(1, 8):
        final = final + yrecv[i]
    final = jnp.concatenate([final[:, 0:36], final[:, 36:72], final[:, 72:108]], axis=0)
    wg_out[...] = final.T[0:36, 0:36] * (ratio / (16.0 * ROWS))

    def drain(ref, n):
        remote(ref, ref, snd.at[n], rcv.at[0], patch_0=y).wait_send()

    drain(send1.at[seven, qk], 0)
    drain(send1.at[seven, vo], 1)
    drain(send1.at[:, ko], 2)
    drain(send1.at[:, vo], 3)
    drain(send2.at[seven, head], 4)
    drain(pa_s.at[0], 5)
    drain(send3.at[seven, head], 6)
    drain(pg_s, 7)
    stat_all(0, 3, 16).wait_send()
    stat_all(1, 19, nx).wait_send()
    stat_all(2, 19 + nx, nz).wait_send()
    drain(send4.at[seven, qo], 11)
    drain(send4.at[seven, kvo], 12)
    drain(drecv, 13)
    for c in xring:
        c.wait_send()

    @pl.when(active)
    def _():
        drain(zsend.at[pl.ds(0, zh - 1)], 14)
        drain(ysend.at[pl.ds(0, 15)], 15)

    @pl.when(jnp.logical_not(active))
    def _():
        drain(zsend, 14)


def write_out(*refs):
    n = len(refs) // 2
    copies = [
        pltpu.make_async_copy(refs[i], refs[n + i], refs[-1].at[i]) for i in range(n)
    ]
    for c in copies:
        c.start()
    for c in copies:
        c.wait()


def step(nx, nz, query_rows, key_rows, value_rows, out_weight, target, lengths, segments):
    part = WIDTH // (2 * nx)
    zh = nz // 2
    dma = pltpu.SemaphoreType.DMA
    scratch = [
        pltpu.VMEM((1, FEAT, ROWS), BF),
        pltpu.VMEM((1, FEAT, ROWS), BF),
        pltpu.VMEM((1, FEAT, ROWS), BF),
        pltpu.VMEM((1, ROWS), jnp.int32),
        pltpu.VMEM((FEAT, WIDTH), BF),
        pltpu.VMEM((1, ROWS, WIDTH), BF),
        pltpu.VMEM((8, 3 * PAD, ROWS), BF),
        pltpu.VMEM((2, 8, 3 * PAD, ROWS), BF),
        pltpu.VMEM((2048, PAD), BF),
        pltpu.VMEM((2048, PAD), BF),
        pltpu.VMEM((1024, PAD), BF),
        pltpu.VMEM((1024, PAD), BF),
        pltpu.VMEM((4, 2048, 256), BF),
        pltpu.VMEM((4, 2048, 256), BF),
        pltpu.VMEM((4, 8, 256), F32),
        pltpu.VMEM((8, PAD, ROWS), BF),
        pltpu.VMEM((8, PAD, ROWS), BF),
        pltpu.VMEM((FEAT, ROWS), F32),
        pltpu.VMEM((8, PAD, ROWS), BF),
        pltpu.VMEM((8, PAD, ROWS), BF),
        pltpu.VMEM((8, 2 * HEAD_DIM, ROWS), BF),
        pltpu.VMEM((8, 2 * HEAD_DIM, ROWS), BF),
        pltpu.VMEM((8, PAD + 2 * HEAD_DIM, ROWS), BF),
        pltpu.VMEM((8, PAD + 2 * HEAD_DIM, ROWS), BF),
        pltpu.VMEM((2, FEAT, ROWS), BF),
        pltpu.VMEM((FEAT, ROWS), BF),
        pltpu.VMEM((2, FEAT, ROWS), BF),
        pltpu.VMEM((nx, 656, ROWS), BF),
        pltpu.VMEM((656, ROWS), BF),
        pltpu.VMEM((656, ROWS), BF),
        pltpu.VMEM((2, 656, ROWS), BF),
        pltpu.VMEM((zh, 176, ROWS), BF),
        pltpu.VMEM((nz, 176, ROWS), BF),
        pltpu.VMEM((16, 16, 128), F32),
        pltpu.VMEM((8, 16, 128), F32),
        pltpu.VMEM((19 + nx + nz, 8, ROWS), F32),
        pltpu.VMEM((4, 1024, 256), F32),
        pltpu.VMEM((4, 8, 256), F32),
        pltpu.VMEM((4, PAD, 256), F32),
    ]
    sems = [6, 16, 13, 8, 8, 8, 8, 8, 4, 6, 6]
    vmem = pl.BlockSpec(memory_space=pltpu.VMEM)
    hbm = pl.BlockSpec(memory_space=pltpu.HBM)
    wide = jax.ShapeDtypeStruct((1, FEAT, ROWS), F32)
    results = (
        wide,
        wide,
        wide,
        jax.ShapeDtypeStruct((36, 36), F32),
        jax.ShapeDtypeStruct((1, 1), F32),
    )
    far = lambda a: pltpu.with_memory_space_constraint(a, pltpu.HBM)
    grads = pl.pallas_call(
        functools.partial(body, nx, nz),
        out_shape=results,
        in_specs=[hbm] * 4 + [pl.BlockSpec(memory_space=pltpu.SMEM), hbm, hbm],
        out_specs=(vmem,) * 5,
        scratch_shapes=scratch + [dma((n,)) for n in sems],
        compiler_params=pltpu.CompilerParams(
            collective_id=0, has_side_effects=True, vmem_limit_bytes=40 * 1024 * 1024
        ),
    )(
        far(jnp.swapaxes(query_rows, 1, 2)),
        far(jnp.swapaxes(key_rows, 1, 2)),
        far(jnp.swapaxes(value_rows, 1, 2)),
        far(segments),
        lengths,
        far(out_weight),
        far(target),
    )
    dq, dk, dv, wg, st = pl.pallas_call(
        write_out,
        out_shape=results,
        in_specs=[pl.BlockSpec(memory_space=pl.ANY)] * 5,
        out_specs=(hbm,) * 5,
        scratch_shapes=[dma((5,))],
        compiler_params=pltpu.CompilerParams(vmem_limit_bytes=2 * 1024 * 1024),
    )(*grads)
    return (
        jnp.swapaxes(dq, 1, 2),
        jnp.swapaxes(dk, 1, 2),
        jnp.swapaxes(dv, 1, 2),
        wg,
        st[0, 0],
    )


def solution(mesh):
    torus = Mesh(mesh.devices.reshape(4, 8, 8, 2), ("dp_0", "dp_1", "patch_0", "patch_1"))
    return jax.shard_map(
        functools.partial(step, 4, 8),
        mesh=torus,
        in_specs=(
            P(DP, PATCH, None),
            P(DP, PATCH, None),
            P(DP, PATCH, None),
            P(),
            P(DP, PATCH, None),
            P(DP),
            P(DP, PATCH),
        ),
        out_specs=(P(DP, PATCH, None), P(DP, PATCH, None), P(DP, PATCH, None), P(PATCH, DP), P()),
        check_vma=False,
    )
```

```python
import functools
import math

import jax
import jax.numpy as jnp
from jax import lax
from jax.experimental import pallas as pl
from jax.experimental.pallas import tpu as pltpu
from jax.sharding import Mesh
from jax.sharding import PartitionSpec as P

WIDTH = 1152
HEADS = 8
HEAD_DIM = 72
FEAT = 576
ROWS = 128
PAD = 80
PATCH = ("patch_0", "patch_1")
DP = ("dp_0", "dp_1")
BF = jnp.bfloat16
F32 = jnp.float32
FAR = (4, 3, 5, 2, 6, 1, 7)
NEAR = (1, 7, 2, 6, 3, 5, 4)
MASK = 2.0**50


def dot(a, b, ca, cb):
    return lax.dot_general(a, b, (((ca,), (cb,)), ((), ())), preferred_element_type=F32)


def body(
    nx,
    nz,
    q_hbm,
    k_hbm,
    v_hbm,
    seg_hbm,
    len_ref,
    w_hbm,
    t_hbm,
    dq_out,
    dk_out,
    dv_out,
    wg_out,
    st_out,
    q_s,
    k_s,
    v_s,
    seg_s,
    w_s,
    t_s,
    send1,
    recv1,
    ktok,
    vtok,
    qtok,
    dtok,
    p_s,
    ds_s,
    rinv_s,
    send2,
    recv2,
    at_s,
    send3,
    recv3,
    dkv,
    drecv,
    send4,
    recv4,
    g_s,
    pg_s,
    pa_s,
    xsend,
    xrel,
    xacc,
    xin,
    zsend,
    zrecv,
    ysend,
    yrecv,
    stat_s,
    s_s,
    top_s,
    acc_s,
    load_sem,
    snd,
    rcv,
    r1,
    r1v,
    d1r,
    r3,
    dkr,
    xs,
    xr,
):
    x = lax.axis_index("dp_0")
    z = lax.axis_index("dp_1")
    y = lax.axis_index("patch_0")
    k = lax.axis_index("patch_1")
    other = 1 - k
    p = 2 * y + k
    zh = nz // 2
    scale = 1.0 / math.sqrt(HEAD_DIM)

    loads = [
        pltpu.make_async_copy(src, dst, load_sem.at[n])
        for n, (src, dst) in enumerate(
            (
                (q_hbm, q_s),
                (k_hbm, k_s),
                (seg_hbm, seg_s),
                (v_hbm, v_s),
                (w_hbm, w_s),
                (t_hbm, t_s),
            )
        )
    ]
    for c in loads:
        c.start()

    barrier = pltpu.get_barrier_semaphore()
    for i in range(1, 8):
        peer = lax.rem(y + i, 8)
        pl.semaphore_signal(barrier, inc=1, device_id={"patch_0": peer})
        pl.semaphore_signal(barrier, inc=1, device_id={"patch_0": peer, "patch_1": other})
    pl.semaphore_signal(barrier, inc=1, device_id={"patch_1": other})
    for i in range(1, nx):
        pl.semaphore_signal(barrier, inc=1, device_id={"dp_0": lax.rem(x + i, nx)})
    for i in range(1, nz):
        pl.semaphore_signal(barrier, inc=1, device_id={"dp_1": lax.rem(z + i, nz)})

    def remote(src, dst, ssem, rsem, **where):
        return pltpu.make_async_remote_copy(
            src_ref=src, dst_ref=dst, send_sem=ssem, recv_sem=rsem, device_id=where
        )

    row = lax.broadcasted_iota(jnp.int32, (8, ROWS), 0)
    lane = lax.broadcasted_iota(jnp.int32, (8, ROWS), 1)
    length = len_ref[0]
    live_t = p * ROWS + lane < length
    for c in loads[:4]:
        c.wait()
    code = jnp.where(live_t, jnp.broadcast_to(seg_s[...], (8, ROWS)), 8)
    low = jnp.bitwise_and(row, 3)
    weight = jnp.where(low == 0, 1, jnp.where(low == 1, 2, jnp.where(low == 2, 4, 8)))
    bit = jnp.where(jnp.bitwise_and(code, weight) != 0, 1.0, 0.0).astype(F32)
    mine = jnp.where(row < 4, bit, 1.0 - bit)
    q_mask = -MASK * mine
    k_mask = MASK * (1.0 - mine)
    v_ones = jnp.where(row == 0, 1.0, 0.0).astype(F32)
    for at, (ref, extra) in enumerate(((q_s, q_mask), (k_s, k_mask), (v_s, v_ones))):
        whole = ref[0].astype(F32)
        for h in range(HEADS):
            block = jnp.concatenate([whole[HEAD_DIM * h : HEAD_DIM * (h + 1)], extra], axis=0)
            send1[h, PAD * at : PAD * (at + 1), :] = block.astype(BF)
    recv1[0, y] = send1[y]

    recv3[...] = jnp.zeros_like(recv3)
    pl.semaphore_wait(barrier, 15 + (nx - 1) + (nz - 1))

    qk = pl.ds(0, 2 * PAD)
    ko = pl.ds(PAD, PAD)
    vo = pl.ds(2 * PAD, PAD)

    def spread(rows, n, rsem):
        for i in FAR:
            h = lax.rem(y + i, 8)
            remote(
                send1.at[h, rows], recv1.at[0, y, rows], snd.at[n], rsem.at[i], patch_0=h
            ).start()

    def block_in(i, rows, rsem):
        b = recv1.at[0, source(i), rows]
        remote(b, b, snd.at[0], rsem.at[i], patch_0=y).wait_recv()

    spread(qk, 0, r1)
    spread(vo, 1, r1v)

    def source(i):
        return lax.rem(y - i + 8, 8)

    def pass_on(i, rows, n, rsem):
        return remote(
            recv1.at[0, source(i), rows],
            recv1.at[1, source(i), rows],
            snd.at[n],
            rsem,
            patch_1=other,
        )

    def token_major(dst, c, src, part):
        at = pl.ds(pl.multiple_of((8 * c + src) * ROWS, ROWS), ROWS)
        dst[at, :] = recv1[c, src, PAD * part : PAD * (part + 1), :].astype(F32).T.astype(BF)

    def pass_keys(i):
        at = pl.multiple_of(source(i) * ROWS, ROWS)
        return remote(
            ktok.at[pl.ds(at, ROWS)],
            ktok.at[pl.ds(8 * ROWS + at, ROWS)],
            snd.at[16],
            d1r.at[i],
            patch_1=other,
        )

    passed = [pass_on(i, ko, 2, rcv.at[8]) for i in range(8)]
    passed_v = [pass_on(i, vo, 3, rcv.at[9]) for i in range(8)]
    token_major(ktok, 0, y, 1)
    pass_keys(0).start()
    passed[0].start()
    passed_v[0].start()
    for i in NEAR:
        block_in(i, qk, r1)
        token_major(ktok, 0, source(i), 1)
        pass_keys(i).start()
        passed[i].start()

    factor = scale * math.log2(math.e)
    pair = y // 2
    mate = y + 1 - 2 * lax.rem(y, 2)
    half = 8 * ROWS

    def queries(j):
        return jnp.concatenate([recv1[0, 2 * j, 0:PAD, :], recv1[0, 2 * j + 1, 0:PAD, :]], axis=1)

    def forward_own(j, carry):
        scores = dot(ktok[0:half, :], queries(j), 1, 0)
        s_s[j] = scores
        top_s[j] = jnp.broadcast_to(jnp.max(scores, axis=0, keepdims=True), (8, 2 * ROWS))
        return carry

    lax.fori_loop(0, 4, forward_own, 0)
    for i in (0,) + NEAR:
        pass_keys(i).wait_recv()

    def forward_other(j, carry):
        scores = dot(ktok[half : 2 * half, :], queries(j), 1, 0)
        top = jnp.maximum(top_s[j, 0:1, :], jnp.max(scores, axis=0, keepdims=True))
        p_s[j, half : 2 * half, :] = jnp.exp2((scores - top) * factor).astype(BF)
        p_s[j, 0:half, :] = jnp.exp2((s_s[j] - top) * factor).astype(BF)
        return carry

    lax.fori_loop(0, 4, forward_other, 0)
    for i in NEAR:
        block_in(i, vo, r1v)
        passed_v[i].start()

    def lanes(c, part):
        return jnp.concatenate(
            [recv1[c, src, PAD * part : PAD * (part + 1), :] for src in range(8)], axis=1
        )

    def values_own(j, carry):
        acc_s[j] = dot(lanes(0, 2), p_s[j, 0:half, :], 1, 0)
        return carry

    lax.fori_loop(0, 4, values_own, 0)
    crossed = recv1.at[1, :, vo]
    remote(crossed, crossed, snd.at[3], rcv.at[9], patch_0=y).wait_recv()

    head = pl.ds(0, HEAD_DIM)

    def send_attn(s):
        return remote(
            send2.at[s, head], recv2.at[y, head], snd.at[4], rcv.at[0], patch_0=s
        )

    for step_at in (2, 1, 3, 0):
        j = lax.rem(pair + step_at, 4)
        accum = acc_s[j] + dot(lanes(1, 2), p_s[j, half : 2 * half, :], 1, 0)
        rinv = 1.0 / accum[HEAD_DIM : HEAD_DIM + 1, :]
        rinv_s[j] = jnp.broadcast_to(rinv, (8, 2 * ROWS))
        attn = (accum * rinv).astype(BF)
        send2[2 * j] = attn[:, :ROWS]
        send2[2 * j + 1] = attn[:, ROWS:]
        if step_at:
            send_attn(2 * j).start()
            send_attn(2 * j + 1).start()
        else:
            send_attn(mate).start()
    recv2[y] = send2[y]

    def backward_layouts(src, carry):
        token_major(vtok, 0, src, 2)
        token_major(vtok, 1, src, 2)
        token_major(qtok, 0, src, 0)
        return carry

    lax.fori_loop(0, 8, backward_layouts, 0)

    loads[4].wait()
    loads[5].wait()
    seven = pl.ds(0, 7)
    remote(
        send2.at[seven, head], recv2.at[seven, head], snd.at[4], rcv.at[0], patch_0=y
    ).wait_recv()
    for h in range(HEADS):
        at_s[HEAD_DIM * h : HEAD_DIM * (h + 1), :] = recv2[h].astype(F32)[:HEAD_DIM]
    attn_t = at_s[...].astype(BF)
    pa_s[0] = attn_t
    swap_a = remote(pa_s.at[0], pa_s.at[1], snd.at[5], rcv.at[1], patch_1=other)
    swap_a.start()
    output = dot(attn_t, w_s[...], 0, 0)
    token = lax.broadcasted_iota(jnp.int32, (ROWS, WIDTH), 0)
    live = p * ROWS + token < length
    error = jnp.where(live, output - t_s[0].astype(F32), 0.0)
    grad_out = (2.0 * error).astype(BF)
    grad_t = (2.0 * error).T.astype(BF)
    part = WIDTH // (2 * nx)
    for zhalf in range(2):
        for xx in range(nx):
            at = (2 * xx + zhalf) * part
            g_s[zhalf, part * xx : part * (xx + 1), :] = grad_t[at : at + part]
    swap_g = remote(g_s.at[other], pg_s, snd.at[7], rcv.at[2], patch_1=other)
    swap_g.start()
    grad_attn = dot(w_s[...], grad_t, 1, 0)
    for h in range(HEADS):
        block = jnp.concatenate(
            [grad_attn[HEAD_DIM * h : HEAD_DIM * (h + 1)], jnp.zeros((8, ROWS), F32)], axis=0
        )
        send3[h] = block.astype(BF)
    for i in FAR:
        to = lax.rem(y + i, 8)
        remote(
            send3.at[to, head], recv3.at[y, head], snd.at[6], r3.at[i], patch_0=to
        ).start()
    recv3[y, 0:HEAD_DIM, :] = send3[y, 0:HEAD_DIM, :]

    swap_a.wait_recv()
    swap_g.wait_recv()
    left = jnp.concatenate([g_s[k], pg_s[...]], axis=1)
    right = jnp.concatenate([pa_s[0], pa_s[1]], axis=1)
    partial = dot(left, right, 1, 1)
    for xx in range(nx):
        chunk = partial[part * xx : part * (xx + 1)]
        rest = jnp.concatenate([chunk[: part // 2, 512:], chunk[part // 2 :, 512:]], axis=1)
        for g in range(4):
            xsend[xx, part * g : part * (g + 1), :] = chunk[:, ROWS * g : ROWS * (g + 1)].astype(BF)
        xsend[xx, 4 * part :, :] = jnp.concatenate([rest, jnp.zeros((8, ROWS), F32)], axis=0).astype(BF)
    lo, hi = pl.ds(0, 336), pl.ds(336, 320)
    up, down, across = lax.rem(x + 1, 4), lax.rem(x + 3, 4), lax.rem(x + 2, 4)
    xring = [
        remote(xsend.at[across, lo], xrel.at[lo], xs.at[0], xr.at[0], dp_0=up),
        remote(xsend.at[across, hi], xrel.at[hi], xs.at[1], xr.at[1], dp_0=down),
        remote(xsend.at[up, hi], xin.at[0, hi], xs.at[2], xr.at[2], dp_0=up),
        remote(xsend.at[down, lo], xin.at[1, lo], xs.at[3], xr.at[3], dp_0=down),
        remote(xacc.at[lo], xin.at[0, lo], xs.at[4], xr.at[4], dp_0=up),
        remote(xacc.at[hi], xin.at[1, hi], xs.at[5], xr.at[5], dp_0=down),
    ]
    for c in xring[:4]:
        c.start()

    def x_relay():
        for n, (rows, size, to) in enumerate(((0, 336, up), (336, 320, down))):
            xring[n].wait_recv()
            xacc[rows : rows + size, :] = (
                xsend[to, rows : rows + size, :].astype(F32)
                + xrel[rows : rows + size, :].astype(F32)
            ).astype(BF)
            xring[4 + n].start()

    squares = jnp.sum(error * error)
    cell = lax.broadcasted_iota(jnp.int32, (8, ROWS), 1)
    stat_s[0] = jnp.where(
        cell == 0, squares, jnp.where(cell == 1, length.astype(F32), 0.0)
    )

    def stat_send(stage, base, n, me, to):
        for i in range(1, n):
            remote(
                stat_s.at[stage],
                stat_s.at[base + i],
                snd.at[8 + stage],
                rcv.at[3 + stage],
                **to(lax.rem(me + i, n)),
            ).start()

    def stat_all(stage, base, n):
        slots = stat_s.at[pl.ds(base + 1, n - 1)]
        return remote(slots, slots, snd.at[8 + stage], rcv.at[3 + stage], patch_0=y)

    def stat_sum(stage, base, n):
        stat_all(stage, base, n).wait_recv()
        acc = stat_s[stage]
        for i in range(1, n):
            acc = acc + stat_s[base + i]
        return acc

    stat_send(0, 3, 16, p, lambda t: {"patch_0": t // 2, "patch_1": lax.rem(t, 2)})
    crossed = recv1.at[1, :, ko]
    remote(crossed, crossed, snd.at[2], rcv.at[8], patch_0=y).wait_recv()

    def send_grad(s, rows, n):
        return remote(
            send4.at[s, rows], recv4.at[y, rows], snd.at[n], rcv.at[n], patch_0=s
        )

    qo = pl.ds(0, HEAD_DIM)
    kvo = pl.ds(PAD, 2 * HEAD_DIM)

    def third_in(s):
        i = lax.rem(y - s + 8, 8)
        remote(
            send3.at[y, head], recv3.at[s, head], snd.at[6], r3.at[i], patch_0=y
        ).wait_recv()

    for step_at in (0, 1, 3, 2):
        j = lax.rem(pair + step_at, 4)
        if step_at:
            third_in(2 * j)
            third_in(2 * j + 1)
        else:
            third_in(mate)
        grads = jnp.concatenate([recv3[2 * j], recv3[2 * j + 1]], axis=1).astype(F32)
        folded = grads * rinv_s[j, 0:1, :]
        dtok[pl.ds(pl.multiple_of(j * 2 * ROWS, 2 * ROWS), 2 * ROWS), :] = folded.T.astype(BF)
        folded = folded.astype(BF)
        attn = jnp.concatenate([send2[2 * j], send2[2 * j + 1]], axis=1)
        delta = jnp.sum(folded.astype(F32) * attn.astype(F32), axis=0, keepdims=True)
        dprobs = dot(vtok[...], folded, 1, 0)
        dscores = (p_s[j].astype(F32) * (dprobs - delta)).astype(BF)
        ds_s[j] = dscores
        keys = jnp.concatenate([lanes(0, 1), lanes(1, 1)], axis=1)
        dq = (dot(keys, dscores, 1, 0) * scale).astype(BF)
        send4[2 * j, 0:PAD, :] = dq[:, :ROWS]
        send4[2 * j + 1, 0:PAD, :] = dq[:, ROWS:]
        if step_at:
            send_grad(2 * j, qo, 11).start()
            send_grad(2 * j + 1, qo, 11).start()
        else:
            send_grad(mate, qo, 11).start()
        if step_at == 1:
            x_relay()

    stat_s[1] = stat_sum(0, 3, 16)
    stat_send(1, 19, nx, x, lambda t: {"dp_0": t})

    def crossing(u):
        two = pl.ds(2 * u, 2)
        return remote(dkv.at[two], drecv.at[two], snd.at[13], dkr.at[u], patch_1=other)

    def key_grads(c, u):
        at = pl.ds(pl.multiple_of((8 * c + 2 * u) * ROWS, 2 * ROWS), 2 * ROWS)
        ds_rows = jnp.concatenate([ds_s[j, at, :] for j in range(4)], axis=1)
        p_rows = jnp.concatenate([p_s[j, at, :] for j in range(4)], axis=1)
        dk = (dot(ds_rows, qtok[...], 1, 0) * scale).T
        dv = dot(p_rows, dtok[...], 1, 0).T
        return jnp.concatenate([dk[:HEAD_DIM], dv[:HEAD_DIM]], axis=0)

    cols = part // zh
    active = z // zh == k

    def x_done():
        stat_s[2] = stat_sum(1, 19, nx)
        stat_send(2, 19 + nx, nz, z, lambda t: {"dp_1": t})
        for c in xring[2:]:
            c.wait_recv()
        total = xsend[x].astype(F32) + xin[0].astype(F32) + xin[1].astype(F32)
        for j in range(zh):
            rest = total[4 * part + cols * (j % 2) : 4 * part + cols * (j % 2 + 1)]
            rest = rest[:, 64 * (j // 2) : 64 * (j // 2 + 1)]
            rows = [total[part * g + cols * j : part * g + cols * (j + 1)] for g in range(4)]
            rows += [
                jnp.concatenate([rest[: cols // 2], rest[cols // 2 :]], axis=1),
                jnp.zeros((14, ROWS), F32),
            ]
            zsend[j] = jnp.concatenate(rows, axis=0).astype(BF)
        start = z + jnp.where(active, 2, 0)
        for step_at in (0, 1, 3, 2):
            j = lax.rem(start + step_at, zh)
            to = zh * k + j
            away = lax.rem(to - z + nz, nz)

            @pl.when(to != z)
            def _():
                remote(
                    zsend.at[j], zrecv.at[away], snd.at[14], rcv.at[6], dp_1=to
                ).start()

        @pl.when(active)
        def _():
            zrecv[0] = zsend[lax.rem(z, zh)]

    def other_keys(step_at):
        u = lax.rem(pair + step_at, 4)
        both = key_grads(1, u).astype(BF)
        dkv[2 * u] = both[:, :ROWS]
        dkv[2 * u + 1] = both[:, ROWS:]
        crossing(u).start()

    def own_keys(step_at):
        u = lax.rem(pair + step_at, 4)
        both = key_grads(0, u)
        crossing(u).wait_recv()
        for c in range(2):
            mine = both[:, ROWS * c : ROWS * (c + 1)]
            send4[2 * u + c, PAD:, :] = (mine + drecv[2 * u + c].astype(F32)).astype(BF)
        if step_at:
            send_grad(2 * u, kvo, 12).start()
            send_grad(2 * u + 1, kvo, 12).start()
        else:
            send_grad(mate, kvo, 12).start()

    other_keys(2)
    other_keys(1)
    own_keys(2)
    x_done()
    other_keys(3)
    own_keys(1)
    other_keys(0)
    own_keys(3)
    own_keys(0)

    recv4[y] = send4[y]

    @pl.when(active)
    def _():
        z_all = zrecv.at[pl.ds(1, nz - 1)]
        remote(z_all, z_all, snd.at[14], rcv.at[6], patch_0=y).wait_recv()
        summed = zrecv[0].astype(F32)
        for i in range(1, nz):
            summed = summed + zrecv[i].astype(F32)
        rest = summed[4 * cols : 4 * cols + cols // 2]
        summed = jnp.concatenate(
            [summed[cols * g : cols * (g + 1)] for g in range(4)]
            + [jnp.concatenate([rest[:, :64], rest[:, 64:]], axis=0)],
            axis=1,
        )
        summed = jnp.concatenate([summed, jnp.zeros((48 - cols, FEAT), F32)], axis=0)
        for t in range(16):
            piece = summed[:, 36 * t : 36 * (t + 1)]
            ysend[t, :, 0:108] = jnp.concatenate(
                [piece[0:16], piece[16:32], piece[32:48]], axis=1
            )

    @pl.when(active)
    def _():
        for i in FAR + (0,):
            for c in range(2):
                if i == 0 and c == 1:
                    continue
                to = lax.rem(y + i, 8)
                core = c if i else other
                remote(
                    ysend.at[2 * to + core],
                    yrecv.at[y],
                    snd.at[15],
                    rcv.at[7],
                    patch_0=to,
                    patch_1=core,
                ).start()

    @pl.when(active)
    def _():
        yrecv[y] = ysend[p]

    acc = stat_sum(2, 19 + nx, nz)
    count = acc[0:1, 1:2] / 16.0
    ratio = (nx * nz * 16.0 * ROWS) / count
    st_out[...] = acc[0:1, 0:1] / (count * WIDTH)

    def grad_all(rows, n):
        blocks = recv4.at[seven, rows]
        return remote(blocks, blocks, snd.at[n], rcv.at[n], patch_0=y)

    def emit(start, out):
        rows = slice(start // 16 * 16, (start // 16 + 5) * 16)
        skip = start % 16
        whole = jnp.concatenate(
            [recv4[h, rows, :].astype(F32)[skip : skip + HEAD_DIM] for h in range(HEADS)],
            axis=0,
        )
        out[0] = whole * ratio

    grad_all(qo, 11).wait_recv()
    emit(0, dq_out)
    grad_all(kvo, 12).wait_recv()
    emit(PAD, dk_out)
    emit(PAD + HEAD_DIM, dv_out)

    def y_all(n):
        blocks = yrecv.at[pl.ds(0, n)]
        return remote(blocks, blocks, snd.at[15], rcv.at[7], patch_0=y)

    @pl.when(active)
    def _():
        y_all(7).wait_recv()

    @pl.when(jnp.logical_not(active))
    def _():
        y_all(8).wait_recv()

    final = yrecv[0]
    for i in range(1, 8):
        final = final + yrecv[i]
    final = jnp.concatenate([final[:, 0:36], final[:, 36:72], final[:, 72:108]], axis=0)
    wg_out[...] = final.T[0:36, 0:36] * (ratio / (16.0 * ROWS))

    def drain(ref, n):
        remote(ref, ref, snd.at[n], rcv.at[0], patch_0=y).wait_send()

    drain(send1.at[seven, qk], 0)
    drain(send1.at[seven, vo], 1)
    drain(send1.at[:, ko], 2)
    drain(ktok.at[pl.ds(0, 8 * ROWS)], 16)
    drain(send1.at[:, vo], 3)
    drain(send2.at[seven, head], 4)
    drain(pa_s.at[0], 5)
    drain(send3.at[seven, head], 6)
    drain(pg_s, 7)
    stat_all(0, 3, 16).wait_send()
    stat_all(1, 19, nx).wait_send()
    stat_all(2, 19 + nx, nz).wait_send()
    drain(send4.at[seven, qo], 11)
    drain(send4.at[seven, kvo], 12)
    drain(drecv, 13)
    for c in xring:
        c.wait_send()

    @pl.when(active)
    def _():
        drain(zsend.at[pl.ds(0, zh - 1)], 14)
        drain(ysend.at[pl.ds(0, 15)], 15)

    @pl.when(jnp.logical_not(active))
    def _():
        drain(zsend, 14)


def write_out(*refs):
    n = len(refs) // 2
    copies = [
        pltpu.make_async_copy(refs[i], refs[n + i], refs[-1].at[i]) for i in range(n)
    ]
    for c in copies:
        c.start()
    for c in copies:
        c.wait()


def step(nx, nz, query_rows, key_rows, value_rows, out_weight, target, lengths, segments):
    part = WIDTH // (2 * nx)
    zh = nz // 2
    dma = pltpu.SemaphoreType.DMA
    scratch = [
        pltpu.VMEM((1, FEAT, ROWS), BF),
        pltpu.VMEM((1, FEAT, ROWS), BF),
        pltpu.VMEM((1, FEAT, ROWS), BF),
        pltpu.VMEM((1, ROWS), jnp.int32),
        pltpu.VMEM((FEAT, WIDTH), BF),
        pltpu.VMEM((1, ROWS, WIDTH), BF),
        pltpu.VMEM((8, 3 * PAD, ROWS), BF),
        pltpu.VMEM((2, 8, 3 * PAD, ROWS), BF),
        pltpu.VMEM((2048, PAD), BF),
        pltpu.VMEM((2048, PAD), BF),
        pltpu.VMEM((1024, PAD), BF),
        pltpu.VMEM((1024, PAD), BF),
        pltpu.VMEM((4, 2048, 256), BF),
        pltpu.VMEM((4, 2048, 256), BF),
        pltpu.VMEM((4, 8, 256), F32),
        pltpu.VMEM((8, PAD, ROWS), BF),
        pltpu.VMEM((8, PAD, ROWS), BF),
        pltpu.VMEM((FEAT, ROWS), F32),
        pltpu.VMEM((8, PAD, ROWS), BF),
        pltpu.VMEM((8, PAD, ROWS), BF),
        pltpu.VMEM((8, 2 * HEAD_DIM, ROWS), BF),
        pltpu.VMEM((8, 2 * HEAD_DIM, ROWS), BF),
        pltpu.VMEM((8, PAD + 2 * HEAD_DIM, ROWS), BF),
        pltpu.VMEM((8, PAD + 2 * HEAD_DIM, ROWS), BF),
        pltpu.VMEM((2, FEAT, ROWS), BF),
        pltpu.VMEM((FEAT, ROWS), BF),
        pltpu.VMEM((2, FEAT, ROWS), BF),
        pltpu.VMEM((nx, 656, ROWS), BF),
        pltpu.VMEM((656, ROWS), BF),
        pltpu.VMEM((656, ROWS), BF),
        pltpu.VMEM((2, 656, ROWS), BF),
        pltpu.VMEM((zh, 176, ROWS), BF),
        pltpu.VMEM((nz, 176, ROWS), BF),
        pltpu.VMEM((16, 16, 128), F32),
        pltpu.VMEM((8, 16, 128), F32),
        pltpu.VMEM((19 + nx + nz, 8, ROWS), F32),
        pltpu.VMEM((4, 1024, 256), F32),
        pltpu.VMEM((4, 8, 256), F32),
        pltpu.VMEM((4, PAD, 256), F32),
    ]
    sems = [6, 17, 13, 8, 8, 8, 8, 4, 6, 6]
    vmem = pl.BlockSpec(memory_space=pltpu.VMEM)
    hbm = pl.BlockSpec(memory_space=pltpu.HBM)
    wide = jax.ShapeDtypeStruct((1, FEAT, ROWS), F32)
    results = (
        wide,
        wide,
        wide,
        jax.ShapeDtypeStruct((36, 36), F32),
        jax.ShapeDtypeStruct((1, 1), F32),
    )
    far = lambda a: pltpu.with_memory_space_constraint(a, pltpu.HBM)
    grads = pl.pallas_call(
        functools.partial(body, nx, nz),
        out_shape=results,
        in_specs=[hbm] * 4 + [pl.BlockSpec(memory_space=pltpu.SMEM), hbm, hbm],
        out_specs=(vmem,) * 5,
        scratch_shapes=scratch + [dma((n,)) for n in sems],
        compiler_params=pltpu.CompilerParams(
            collective_id=0, has_side_effects=True, vmem_limit_bytes=40 * 1024 * 1024
        ),
    )(
        far(jnp.swapaxes(query_rows, 1, 2)),
        far(jnp.swapaxes(key_rows, 1, 2)),
        far(jnp.swapaxes(value_rows, 1, 2)),
        far(segments),
        lengths,
        far(out_weight),
        far(target),
    )
    dq, dk, dv, wg, st = pl.pallas_call(
        write_out,
        out_shape=results,
        in_specs=[pl.BlockSpec(memory_space=pl.ANY)] * 5,
        out_specs=(hbm,) * 5,
        scratch_shapes=[dma((5,))],
        compiler_params=pltpu.CompilerParams(vmem_limit_bytes=2 * 1024 * 1024),
    )(*grads)
    return (
        jnp.swapaxes(dq, 1, 2),
        jnp.swapaxes(dk, 1, 2),
        jnp.swapaxes(dv, 1, 2),
        wg,
        st[0, 0],
    )


def solution(mesh):
    torus = Mesh(mesh.devices.reshape(4, 8, 8, 2), ("dp_0", "dp_1", "patch_0", "patch_1"))
    return jax.shard_map(
        functools.partial(step, 4, 8),
        mesh=torus,
        in_specs=(
            P(DP, PATCH, None),
            P(DP, PATCH, None),
            P(DP, PATCH, None),
            P(),
            P(DP, PATCH, None),
            P(DP),
            P(DP, PATCH),
        ),
        out_specs=(P(DP, PATCH, None), P(DP, PATCH, None), P(DP, PATCH, None), P(PATCH, DP), P()),
        check_vma=False,
    )
```

```python
import functools
import math

import jax
import jax.numpy as jnp
from jax import lax
from jax.experimental import pallas as pl
from jax.experimental.pallas import tpu as pltpu
from jax.sharding import Mesh
from jax.sharding import PartitionSpec as P

WIDTH = 1152
HEADS = 8
HEAD_DIM = 72
FEAT = 576
ROWS = 128
PAD = 80
PATCH = ("patch_0", "patch_1")
DP = ("dp_0", "dp_1")
BF = jnp.bfloat16
F32 = jnp.float32
FAR = (4, 3, 5, 2, 6, 1, 7)
NEAR = (1, 7, 2, 6, 3, 5, 4)
MASK = 2.0**50


def dot(a, b, ca, cb):
    return lax.dot_general(a, b, (((ca,), (cb,)), ((), ())), preferred_element_type=F32)


def body(
    nx,
    nz,
    q_hbm,
    k_hbm,
    v_hbm,
    seg_hbm,
    len_ref,
    w_hbm,
    t_hbm,
    dq_out,
    dk_out,
    dv_out,
    wg_out,
    st_out,
    q_s,
    k_s,
    v_s,
    seg_s,
    w_s,
    t_s,
    send1,
    recv1,
    ktok,
    vtok,
    qtok,
    dtok,
    p_s,
    ds_s,
    w_half,
    send2,
    recv2,
    at_s,
    send3,
    recv3,
    dkv,
    drecv,
    send4,
    recv4,
    g_s,
    pg_s,
    pa_s,
    xsend,
    xrel,
    xacc,
    xin,
    zsend,
    zrecv,
    ysend,
    yrecv,
    stat_s,
    qf_s,
    top_s,
    acc_s,
    load_sem,
    snd,
    rcv,
    r1,
    r1v,
    d1r,
    r3,
    dkr,
    xs,
    xr,
):
    x = lax.axis_index("dp_0")
    z = lax.axis_index("dp_1")
    y = lax.axis_index("patch_0")
    k = lax.axis_index("patch_1")
    other = 1 - k
    p = 2 * y + k
    zh = nz // 2
    scale = 1.0 / math.sqrt(HEAD_DIM)

    loads = [
        pltpu.make_async_copy(src, dst, load_sem.at[n])
        for n, (src, dst) in enumerate(
            (
                (q_hbm, q_s),
                (k_hbm, k_s),
                (seg_hbm, seg_s),
                (v_hbm, v_s),
                (w_hbm, w_s),
                (t_hbm, t_s),
            )
        )
    ]
    for c in loads:
        c.start()

    barrier = pltpu.get_barrier_semaphore()
    for i in range(1, 8):
        peer = lax.rem(y + i, 8)
        pl.semaphore_signal(barrier, inc=1, device_id={"patch_0": peer})
        pl.semaphore_signal(barrier, inc=1, device_id={"patch_0": peer, "patch_1": other})
    pl.semaphore_signal(barrier, inc=1, device_id={"patch_1": other})
    for i in range(1, nx):
        pl.semaphore_signal(barrier, inc=1, device_id={"dp_0": lax.rem(x + i, nx)})
    for i in range(1, nz):
        pl.semaphore_signal(barrier, inc=1, device_id={"dp_1": lax.rem(z + i, nz)})

    def remote(src, dst, ssem, rsem, **where):
        return pltpu.make_async_remote_copy(
            src_ref=src, dst_ref=dst, send_sem=ssem, recv_sem=rsem, device_id=where
        )

    row = lax.broadcasted_iota(jnp.int32, (8, ROWS), 0)
    lane = lax.broadcasted_iota(jnp.int32, (8, ROWS), 1)
    for c in loads[:4]:
        c.wait()
    length = len_ref[0]
    live_t = p * ROWS + lane < length
    code = jnp.where(live_t, jnp.broadcast_to(seg_s[...], (8, ROWS)), 8)
    low = jnp.bitwise_and(row, 3)
    weight = jnp.where(low == 0, 1, jnp.where(low == 1, 2, jnp.where(low == 2, 4, 8)))
    bit = jnp.where(jnp.bitwise_and(code, weight) != 0, 1.0, 0.0).astype(F32)
    mine = jnp.where(row < 4, bit, 1.0 - bit)
    q_mask = -MASK * mine
    parts = [ref[0].astype(F32) for ref in (k_s, q_s, v_s)]
    for h in range(HEADS):
        keys, asks, vals = [a[HEAD_DIM * h : HEAD_DIM * (h + 1)] for a in parts]
        send1[h] = jnp.concatenate([keys, asks, q_mask, vals], axis=0).astype(BF)
    recv1[0, y] = send1[y]

    recv3[...] = jnp.zeros_like(recv3)
    pl.semaphore_wait(barrier, 15 + (nx - 1) + (nz - 1))

    qk = pl.ds(0, 2 * HEAD_DIM + 8)
    ko = pl.ds(0, HEAD_DIM)
    vo = pl.ds(2 * HEAD_DIM + 8, HEAD_DIM)
    mo = pl.ds(2 * HEAD_DIM, PAD)

    def spread(rows, n, rsem):
        for i in FAR:
            h = lax.rem(y + i, 8)
            remote(
                send1.at[h, rows], recv1.at[0, y, rows], snd.at[n], rsem.at[i], patch_0=h
            ).start()

    def block_in(i, rows, rsem):
        b = recv1.at[0, source(i), rows]
        remote(b, b, snd.at[0], rsem.at[i], patch_0=y).wait_recv()

    spread(qk, 0, r1)
    spread(vo, 1, r1v)

    def source(i):
        return lax.rem(y - i + 8, 8)

    def pass_on(i, rows, n, rsem):
        return remote(
            recv1.at[0, source(i), rows],
            recv1.at[1, source(i), rows],
            snd.at[n],
            rsem,
            patch_1=other,
        )

    def row_block(src, c=0):
        return pl.ds(pl.multiple_of((8 * c + src) * ROWS, ROWS), ROWS)

    def take(src):
        asks = recv1[0, src, HEAD_DIM : 2 * HEAD_DIM + 8, :].astype(F32)
        qf_s[src] = asks.astype(BF)
        keys = recv1[0, src, 0:HEAD_DIM, :].astype(F32)
        keys = jnp.concatenate([keys, MASK + asks[HEAD_DIM:]], axis=0)
        ktok[row_block(src), :] = keys.T.astype(BF)

    def pass_keys(i):
        at = pl.multiple_of(source(i) * ROWS, ROWS)
        return remote(
            ktok.at[pl.ds(at, ROWS)],
            ktok.at[pl.ds(8 * ROWS + at, ROWS)],
            snd.at[16],
            d1r.at[i],
            patch_1=other,
        )

    passed = [pass_on(i, ko, 2, rcv.at[8]) for i in range(8)]
    passed_v = [pass_on(i, mo, 3, rcv.at[9]) for i in range(8)]
    take(y)
    pass_keys(0).start()
    passed[0].start()
    passed_v[0].start()
    for i in NEAR:
        block_in(i, qk, r1)
        take(source(i))
        pass_keys(i).start()
        passed[i].start()

    factor = scale * math.log2(math.e)
    pair = y // 2
    mate = y + 1 - 2 * lax.rem(y, 2)
    half = 8 * ROWS

    def queries(j):
        return jnp.concatenate([qf_s[2 * j], qf_s[2 * j + 1]], axis=1)

    def forward_half(j, c):
        scores = dot(ktok[half * c : half * (c + 1), :], queries(j), 1, 0)
        top = jnp.max(scores, axis=0, keepdims=True)
        p_s[j, half * c : half * (c + 1), :] = jnp.exp2((scores - top) * factor).astype(BF)
        return top

    def forward_own(j, carry):
        top_s[j] = jnp.broadcast_to(forward_half(j, 0), (8, 2 * ROWS))
        return carry

    lax.fori_loop(0, 4, forward_own, 0)
    for i in (0,) + NEAR:
        pass_keys(i).wait_recv()

    def forward_other(j, carry):
        top = forward_half(j, 1)
        mine = top_s[j, 0:1, :]
        best = jnp.maximum(mine, top)
        for c, one in enumerate((mine, top)):
            w_half[c, j] = jnp.broadcast_to(jnp.exp2((one - best) * factor), (8, 2 * ROWS))
        return carry

    lax.fori_loop(0, 4, forward_other, 0)
    for i in NEAR:
        block_in(i, vo, r1v)
        passed_v[i].start()

    def lanes(c, start, end):
        return jnp.concatenate([recv1[c, src, start:end, :] for src in range(8)], axis=1)

    def values(c):
        return lanes(c, 2 * HEAD_DIM, 3 * HEAD_DIM + 8)

    def values_own(j, carry):
        acc_s[j] = dot(values(0), p_s[j, 0:half, :], 1, 0)
        return carry

    lax.fori_loop(0, 4, values_own, 0)
    crossed = recv1.at[1, :, mo]
    remote(crossed, crossed, snd.at[3], rcv.at[9], patch_0=y).wait_recv()

    head = pl.ds(8, HEAD_DIM)

    def send_attn(s):
        return remote(
            send2.at[s, head], recv2.at[y, head], snd.at[4], rcv.at[0], patch_0=s
        )

    for step_at in (2, 1, 3, 0):
        j = lax.rem(pair + step_at, 4)
        mine, yours = w_half[0, j, 0:1, :], w_half[1, j, 0:1, :]
        accum = acc_s[j] * mine + dot(values(1), p_s[j, half : 2 * half, :], 1, 0) * yours
        rinv = -MASK / (accum[0:1, :] + accum[4:5, :])
        w_half[0, j] = jnp.broadcast_to(mine * rinv, (8, 2 * ROWS))
        w_half[1, j] = jnp.broadcast_to(yours * rinv, (8, 2 * ROWS))
        attn = (accum * rinv).astype(BF)
        send2[2 * j] = attn[:, :ROWS]
        send2[2 * j + 1] = attn[:, ROWS:]
        if step_at:
            send_attn(2 * j).start()
            send_attn(2 * j + 1).start()
        else:
            send_attn(mate).start()
    recv2[y] = send2[y]

    def backward_layouts(src, carry):
        for c in range(2):
            vals = recv1[c, src, 2 * HEAD_DIM : 3 * HEAD_DIM + 8, :]
            vtok[row_block(src, c), :] = vals.astype(F32).T.astype(BF)
        qtok[row_block(src), :] = qf_s[src].astype(F32).T.astype(BF)
        return carry

    lax.fori_loop(0, 8, backward_layouts, 0)

    loads[4].wait()
    loads[5].wait()
    seven = pl.ds(0, 7)
    remote(
        send2.at[seven, head], recv2.at[seven, head], snd.at[4], rcv.at[0], patch_0=y
    ).wait_recv()
    for h in range(HEADS):
        at_s[HEAD_DIM * h : HEAD_DIM * (h + 1), :] = recv2[h].astype(F32)[8:]
    attn_t = at_s[...].astype(BF)
    pa_s[0] = attn_t
    swap_a = remote(pa_s.at[0], pa_s.at[1], snd.at[5], rcv.at[1], patch_1=other)
    swap_a.start()
    output = dot(attn_t, w_s[...], 0, 0)
    token = lax.broadcasted_iota(jnp.int32, (ROWS, WIDTH), 0)
    live = p * ROWS + token < length
    error = jnp.where(live, output - t_s[0].astype(F32), 0.0)
    grad_out = (2.0 * error).astype(BF)
    grad_t = (2.0 * error).T.astype(BF)
    part = WIDTH // (2 * nx)
    for zhalf in range(2):
        for xx in range(nx):
            at = (2 * xx + zhalf) * part
            g_s[zhalf, part * xx : part * (xx + 1), :] = grad_t[at : at + part]
    swap_g = remote(g_s.at[other], pg_s, snd.at[7], rcv.at[2], patch_1=other)
    swap_g.start()
    grad_attn = dot(w_s[...], grad_t, 1, 0)
    for h in range(HEADS):
        block = jnp.concatenate(
            [jnp.zeros((8, ROWS), F32), grad_attn[HEAD_DIM * h : HEAD_DIM * (h + 1)]], axis=0
        )
        send3[h] = block.astype(BF)
    for i in FAR:
        to = lax.rem(y + i, 8)
        remote(
            send3.at[to, head], recv3.at[y, head], snd.at[6], r3.at[i], patch_0=to
        ).start()
    recv3[y] = send3[y]

    swap_a.wait_recv()
    swap_g.wait_recv()
    right = jnp.concatenate([pa_s[0], pa_s[1]], axis=1)

    def x_chunk(xx):
        at = pl.ds(pl.multiple_of(part * xx, 16), part)
        chunk = dot(jnp.concatenate([g_s[k, at, :], pg_s[at, :]], axis=1), right, 1, 1)
        rest = jnp.concatenate([chunk[: part // 2, 512:], chunk[part // 2 :, 512:]], axis=1)
        for g in range(4):
            xsend[xx, part * g : part * (g + 1), :] = chunk[:, ROWS * g : ROWS * (g + 1)].astype(BF)
        xsend[xx, 4 * part :, :] = jnp.concatenate([rest, jnp.zeros((8, ROWS), F32)], axis=0).astype(BF)

    lo, hi = pl.ds(0, 336), pl.ds(336, 320)
    up, down, across = lax.rem(x + 1, 4), lax.rem(x + 3, 4), lax.rem(x + 2, 4)
    xring = [
        remote(xsend.at[across, lo], xrel.at[lo], xs.at[0], xr.at[0], dp_0=up),
        remote(xsend.at[across, hi], xrel.at[hi], xs.at[1], xr.at[1], dp_0=down),
        remote(xsend.at[up, hi], xin.at[0, hi], xs.at[2], xr.at[2], dp_0=up),
        remote(xsend.at[down, lo], xin.at[1, lo], xs.at[3], xr.at[3], dp_0=down),
        remote(xacc.at[lo], xin.at[0, lo], xs.at[4], xr.at[4], dp_0=up),
        remote(xacc.at[hi], xin.at[1, hi], xs.at[5], xr.at[5], dp_0=down),
    ]
    x_chunk(across)
    xring[0].start()
    xring[1].start()
    x_chunk(up)
    xring[2].start()
    x_chunk(down)
    xring[3].start()
    x_chunk(x)

    def x_relay():
        for n, (rows, size, to) in enumerate(((0, 336, up), (336, 320, down))):
            xring[n].wait_recv()
            xacc[rows : rows + size, :] = (
                xsend[to, rows : rows + size, :].astype(F32)
                + xrel[rows : rows + size, :].astype(F32)
            ).astype(BF)
            xring[4 + n].start()

    squares = jnp.sum(error * error)
    cell = lax.broadcasted_iota(jnp.int32, (8, ROWS), 1)
    stat_s[0] = jnp.where(
        cell == 0, squares, jnp.where(cell == 1, length.astype(F32), 0.0)
    )

    def stat_send(stage, base, n, me, to):
        for i in range(1, n):
            remote(
                stat_s.at[stage],
                stat_s.at[base + i],
                snd.at[8 + stage],
                rcv.at[3 + stage],
                **to(lax.rem(me + i, n)),
            ).start()

    def stat_all(stage, base, n):
        slots = stat_s.at[pl.ds(base + 1, n - 1)]
        return remote(slots, slots, snd.at[8 + stage], rcv.at[3 + stage], patch_0=y)

    def stat_sum(stage, base, n):
        stat_all(stage, base, n).wait_recv()
        acc = stat_s[stage]
        for i in range(1, n):
            acc = acc + stat_s[base + i]
        return acc

    stat_send(0, 3, 16, p, lambda t: {"patch_0": t // 2, "patch_1": lax.rem(t, 2)})
    crossed = recv1.at[1, :, ko]
    remote(crossed, crossed, snd.at[2], rcv.at[8], patch_0=y).wait_recv()

    def send_grad(s, rows, n):
        return remote(
            send4.at[s, rows], recv4.at[y, rows], snd.at[n], rcv.at[n], patch_0=s
        )

    qo = pl.ds(0, HEAD_DIM)
    kvo = pl.ds(PAD, 2 * HEAD_DIM)

    def third_in(s):
        i = lax.rem(y - s + 8, 8)
        remote(
            send3.at[y, head], recv3.at[s, head], snd.at[6], r3.at[i], patch_0=y
        ).wait_recv()

    for step_at in (0, 1, 3, 2):
        j = lax.rem(pair + step_at, 4)
        if step_at:
            third_in(2 * j)
            third_in(2 * j + 1)
        else:
            third_in(mate)
        grads = jnp.concatenate([recv3[2 * j], recv3[2 * j + 1]], axis=1).astype(F32)
        attn = jnp.concatenate([send2[2 * j], send2[2 * j + 1]], axis=1).astype(F32)
        at = pl.ds(pl.multiple_of(j * 2 * ROWS, 2 * ROWS), 2 * ROWS)
        for c in range(2):
            folded = grads * w_half[c, j, 0:1, :]
            dtok[c, at, :] = folded.T.astype(BF)
            folded = folded.astype(BF)
            delta = jnp.sum(folded.astype(F32) * attn, axis=0, keepdims=True)
            these = slice(half * c, half * (c + 1))
            dprobs = dot(vtok[these, :], folded, 1, 0)
            ds_s[j, these, :] = (p_s[j, these, :].astype(F32) * (dprobs - delta)).astype(BF)
        keys = jnp.concatenate([lanes(0, 0, HEAD_DIM), lanes(1, 0, HEAD_DIM)], axis=1)
        dq = dot(keys, ds_s[j], 1, 0) * scale
        dq = jnp.concatenate([dq, jnp.zeros((8, 2 * ROWS), F32)], axis=0).astype(BF)
        send4[2 * j, 0:PAD, :] = dq[:, :ROWS]
        send4[2 * j + 1, 0:PAD, :] = dq[:, ROWS:]
        if step_at:
            send_grad(2 * j, qo, 11).start()
            send_grad(2 * j + 1, qo, 11).start()
        else:
            send_grad(mate, qo, 11).start()
        if step_at == 1:
            x_relay()

    stat_s[1] = stat_sum(0, 3, 16)
    stat_send(1, 19, nx, x, lambda t: {"dp_0": t})

    def crossing(u):
        two = pl.ds(2 * u, 2)
        return remote(dkv.at[two], drecv.at[two], snd.at[13], dkr.at[u], patch_1=other)

    def key_grads(c, u):
        at = pl.ds(pl.multiple_of((8 * c + 2 * u) * ROWS, 2 * ROWS), 2 * ROWS)
        ds_rows = jnp.concatenate([ds_s[j, at, :] for j in range(4)], axis=1)
        p_rows = jnp.concatenate([p_s[j, at, :] for j in range(4)], axis=1)
        dk = (dot(ds_rows, qtok[...], 1, 0) * scale).T
        dv = dot(p_rows, dtok[c], 1, 0).T
        return jnp.concatenate([dk[:HEAD_DIM], dv[8:]], axis=0)

    cols = part // zh
    active = z // zh == k

    def x_done():
        stat_s[2] = stat_sum(1, 19, nx)
        stat_send(2, 19 + nx, nz, z, lambda t: {"dp_1": t})
        for c in xring[2:]:
            c.wait_recv()
        total = xsend[x].astype(F32) + xin[0].astype(F32) + xin[1].astype(F32)
        for j in range(zh):
            rest = total[4 * part + cols * (j % 2) : 4 * part + cols * (j % 2 + 1)]
            rest = rest[:, 64 * (j // 2) : 64 * (j // 2 + 1)]
            rows = [total[part * g + cols * j : part * g + cols * (j + 1)] for g in range(4)]
            rows += [
                jnp.concatenate([rest[: cols // 2], rest[cols // 2 :]], axis=1),
                jnp.zeros((14, ROWS), F32),
            ]
            zsend[j] = jnp.concatenate(rows, axis=0).astype(BF)
        start = z + jnp.where(active, 2, 0)
        for step_at in (0, 1, 3, 2):
            j = lax.rem(start + step_at, zh)
            to = zh * k + j
            away = lax.rem(to - z + nz, nz)

            @pl.when(to != z)
            def _():
                remote(
                    zsend.at[j], zrecv.at[away], snd.at[14], rcv.at[6], dp_1=to
                ).start()

        @pl.when(active)
        def _():
            zrecv[0] = zsend[lax.rem(z, zh)]

    def other_keys(step_at):
        u = lax.rem(pair + step_at, 4)
        both = key_grads(1, u).astype(BF)
        dkv[2 * u] = both[:, :ROWS]
        dkv[2 * u + 1] = both[:, ROWS:]
        crossing(u).start()

    def own_keys(step_at):
        u = lax.rem(pair + step_at, 4)
        both = key_grads(0, u)
        crossing(u).wait_recv()
        for c in range(2):
            mine = both[:, ROWS * c : ROWS * (c + 1)]
            send4[2 * u + c, PAD:, :] = (mine + drecv[2 * u + c].astype(F32)).astype(BF)
        if step_at:
            send_grad(2 * u, kvo, 12).start()
            send_grad(2 * u + 1, kvo, 12).start()
        else:
            send_grad(mate, kvo, 12).start()

    other_keys(2)
    other_keys(1)
    own_keys(2)
    x_done()
    other_keys(3)
    own_keys(1)
    other_keys(0)
    own_keys(3)
    own_keys(0)

    recv4[y] = send4[y]

    @pl.when(active)
    def _():
        z_all = zrecv.at[pl.ds(1, nz - 1)]
        remote(z_all, z_all, snd.at[14], rcv.at[6], patch_0=y).wait_recv()
        summed = zrecv[0].astype(F32)
        for i in range(1, nz):
            summed = summed + zrecv[i].astype(F32)
        rest = summed[4 * cols : 4 * cols + cols // 2]
        summed = jnp.concatenate(
            [summed[cols * g : cols * (g + 1)] for g in range(4)]
            + [jnp.concatenate([rest[:, :64], rest[:, 64:]], axis=0)],
            axis=1,
        )
        summed = jnp.concatenate([summed, jnp.zeros((48 - cols, FEAT), F32)], axis=0)
        for t in range(16):
            piece = summed[:, 36 * t : 36 * (t + 1)]
            ysend[t, :, 0:108] = jnp.concatenate(
                [piece[0:16], piece[16:32], piece[32:48]], axis=1
            )

    @pl.when(active)
    def _():
        for i in FAR + (0,):
            for c in range(2):
                if i == 0 and c == 1:
                    continue
                to = lax.rem(y + i, 8)
                core = c if i else other
                remote(
                    ysend.at[2 * to + core],
                    yrecv.at[y],
                    snd.at[15],
                    rcv.at[7],
                    patch_0=to,
                    patch_1=core,
                ).start()

    @pl.when(active)
    def _():
        yrecv[y] = ysend[p]

    acc = stat_sum(2, 19 + nx, nz)
    count = acc[0:1, 1:2] / 16.0
    ratio = (nx * nz * 16.0 * ROWS) / count
    st_out[...] = acc[0:1, 0:1] / (count * WIDTH)

    def grad_all(rows, n):
        blocks = recv4.at[seven, rows]
        return remote(blocks, blocks, snd.at[n], rcv.at[n], patch_0=y)

    def emit(start, out):
        rows = slice(start // 16 * 16, (start // 16 + 5) * 16)
        skip = start % 16
        whole = jnp.concatenate(
            [recv4[h, rows, :].astype(F32)[skip : skip + HEAD_DIM] for h in range(HEADS)],
            axis=0,
        )
        out[0] = whole * ratio

    grad_all(qo, 11).wait_recv()
    emit(0, dq_out)
    grad_all(kvo, 12).wait_recv()
    emit(PAD, dk_out)
    emit(PAD + HEAD_DIM, dv_out)

    def y_all(n):
        blocks = yrecv.at[pl.ds(0, n)]
        return remote(blocks, blocks, snd.at[15], rcv.at[7], patch_0=y)

    @pl.when(active)
    def _():
        y_all(7).wait_recv()

    @pl.when(jnp.logical_not(active))
    def _():
        y_all(8).wait_recv()

    final = yrecv[0]
    for i in range(1, 8):
        final = final + yrecv[i]
    final = jnp.concatenate([final[:, 0:36], final[:, 36:72], final[:, 72:108]], axis=0)
    wg_out[...] = final.T[0:36, 0:36] * (ratio / (16.0 * ROWS))

    def drain(ref, n):
        remote(ref, ref, snd.at[n], rcv.at[0], patch_0=y).wait_send()

    drain(send1.at[seven, qk], 0)
    drain(send1.at[seven, vo], 1)
    drain(send1.at[:, ko], 2)
    drain(ktok.at[pl.ds(0, 8 * ROWS)], 16)
    drain(send1.at[:, mo], 3)
    drain(send2.at[seven, head], 4)
    drain(pa_s.at[0], 5)
    drain(send3.at[seven, head], 6)
    drain(pg_s, 7)
    stat_all(0, 3, 16).wait_send()
    stat_all(1, 19, nx).wait_send()
    stat_all(2, 19 + nx, nz).wait_send()
    drain(send4.at[seven, qo], 11)
    drain(send4.at[seven, kvo], 12)
    drain(drecv, 13)
    for c in xring:
        c.wait_send()

    @pl.when(active)
    def _():
        drain(zsend.at[pl.ds(0, zh - 1)], 14)
        drain(ysend.at[pl.ds(0, 15)], 15)

    @pl.when(jnp.logical_not(active))
    def _():
        drain(zsend, 14)


def write_out(*refs):
    n = len(refs) // 2
    copies = [
        pltpu.make_async_copy(refs[i], refs[n + i], refs[-1].at[i]) for i in range(n)
    ]
    for c in copies:
        c.start()
    for c in copies:
        c.wait()


def step(nx, nz, query_rows, key_rows, value_rows, out_weight, target, lengths, segments):
    part = WIDTH // (2 * nx)
    zh = nz // 2
    dma = pltpu.SemaphoreType.DMA
    scratch = [
        pltpu.VMEM((1, FEAT, ROWS), BF),
        pltpu.VMEM((1, FEAT, ROWS), BF),
        pltpu.VMEM((1, FEAT, ROWS), BF),
        pltpu.VMEM((1, ROWS), jnp.int32),
        pltpu.VMEM((FEAT, WIDTH), BF),
        pltpu.VMEM((1, ROWS, WIDTH), BF),
        pltpu.VMEM((8, 3 * HEAD_DIM + 8, ROWS), BF),
        pltpu.VMEM((2, 8, 3 * HEAD_DIM + 8, ROWS), BF),
        pltpu.VMEM((2048, PAD), BF),
        pltpu.VMEM((2048, PAD), BF),
        pltpu.VMEM((1024, PAD), BF),
        pltpu.VMEM((2, 1024, PAD), BF),
        pltpu.VMEM((4, 2048, 256), BF),
        pltpu.VMEM((4, 2048, 256), BF),
        pltpu.VMEM((2, 4, 8, 256), F32),
        pltpu.VMEM((8, PAD, ROWS), BF),
        pltpu.VMEM((8, PAD, ROWS), BF),
        pltpu.VMEM((FEAT, ROWS), F32),
        pltpu.VMEM((8, PAD, ROWS), BF),
        pltpu.VMEM((8, PAD, ROWS), BF),
        pltpu.VMEM((8, 2 * HEAD_DIM, ROWS), BF),
        pltpu.VMEM((8, 2 * HEAD_DIM, ROWS), BF),
        pltpu.VMEM((8, PAD + 2 * HEAD_DIM, ROWS), BF),
        pltpu.VMEM((8, PAD + 2 * HEAD_DIM, ROWS), BF),
        pltpu.VMEM((2, FEAT, ROWS), BF),
        pltpu.VMEM((FEAT, ROWS), BF),
        pltpu.VMEM((2, FEAT, ROWS), BF),
        pltpu.VMEM((nx, 656, ROWS), BF),
        pltpu.VMEM((656, ROWS), BF),
        pltpu.VMEM((656, ROWS), BF),
        pltpu.VMEM((2, 656, ROWS), BF),
        pltpu.VMEM((zh, 176, ROWS), BF),
        pltpu.VMEM((nz, 176, ROWS), BF),
        pltpu.VMEM((16, 16, 128), F32),
        pltpu.VMEM((8, 16, 128), F32),
        pltpu.VMEM((19 + nx + nz, 8, ROWS), F32),
        pltpu.VMEM((8, PAD, ROWS), BF),
        pltpu.VMEM((4, 8, 256), F32),
        pltpu.VMEM((4, PAD, 256), F32),
    ]
    sems = [6, 17, 13, 8, 8, 8, 8, 4, 6, 6]
    vmem = pl.BlockSpec(memory_space=pltpu.VMEM)
    hbm = pl.BlockSpec(memory_space=pltpu.HBM)
    wide = jax.ShapeDtypeStruct((1, FEAT, ROWS), F32)
    results = (
        wide,
        wide,
        wide,
        jax.ShapeDtypeStruct((36, 36), F32),
        jax.ShapeDtypeStruct((1, 1), F32),
    )
    far = lambda a: pltpu.with_memory_space_constraint(a, pltpu.HBM)
    grads = pl.pallas_call(
        functools.partial(body, nx, nz),
        out_shape=results,
        in_specs=[hbm] * 4 + [pl.BlockSpec(memory_space=pltpu.SMEM), hbm, hbm],
        out_specs=(vmem,) * 5,
        scratch_shapes=scratch + [dma((n,)) for n in sems],
        compiler_params=pltpu.CompilerParams(
            collective_id=0, has_side_effects=True, vmem_limit_bytes=40 * 1024 * 1024
        ),
    )(
        far(jnp.swapaxes(query_rows, 1, 2)),
        far(jnp.swapaxes(key_rows, 1, 2)),
        far(jnp.swapaxes(value_rows, 1, 2)),
        far(segments),
        lengths,
        far(out_weight),
        far(target),
    )
    dq, dk, dv, wg, st = pl.pallas_call(
        write_out,
        out_shape=results,
        in_specs=[pl.BlockSpec(memory_space=pl.ANY)] * 5,
        out_specs=(hbm,) * 5,
        scratch_shapes=[dma((5,))],
        compiler_params=pltpu.CompilerParams(vmem_limit_bytes=2 * 1024 * 1024),
    )(*grads)
    return (
        jnp.swapaxes(dq, 1, 2),
        jnp.swapaxes(dk, 1, 2),
        jnp.swapaxes(dv, 1, 2),
        wg,
        st[0, 0],
    )


def solution(mesh):
    torus = Mesh(mesh.devices.reshape(4, 8, 8, 2), ("dp_0", "dp_1", "patch_0", "patch_1"))
    return jax.shard_map(
        functools.partial(step, 4, 8),
        mesh=torus,
        in_specs=(
            P(DP, PATCH, None),
            P(DP, PATCH, None),
            P(DP, PATCH, None),
            P(),
            P(DP, PATCH, None),
            P(DP),
            P(DP, PATCH),
        ),
        out_specs=(P(DP, PATCH, None), P(DP, PATCH, None), P(DP, PATCH, None), P(PATCH, DP), P()),
        check_vma=False,
    )
```

```python
import functools
import math

import jax
import jax.numpy as jnp
from jax import lax
from jax.experimental import pallas as pl
from jax.experimental.pallas import tpu as pltpu
from jax.sharding import Mesh
from jax.sharding import PartitionSpec as P

WIDTH = 1152
HEADS = 8
HEAD_DIM = 72
FEAT = 576
ROWS = 128
PAD = 80
PATCH = ("patch_0", "patch_1")
DP = ("dp_0", "dp_1")
BF = jnp.bfloat16
F32 = jnp.float32
FAR = (4, 3, 5, 2, 6, 1, 7)
NEAR = (1, 7, 2, 6, 3, 5, 4)
MASK = 2.0**50


def dot(a, b, ca, cb):
    return lax.dot_general(a, b, (((ca,), (cb,)), ((), ())), preferred_element_type=F32)


def body(
    nx,
    nz,
    q_hbm,
    k_hbm,
    v_hbm,
    seg_hbm,
    len_ref,
    w_hbm,
    t_hbm,
    dq_out,
    dk_out,
    dv_out,
    wg_out,
    st_out,
    q_s,
    k_s,
    v_s,
    seg_s,
    w_s,
    t_s,
    wt_s,
    tt_s,
    send1,
    recv1,
    ktok,
    vtok,
    qtok,
    dtok,
    p_s,
    ds_s,
    w_half,
    send2,
    recv2,
    at_s,
    send3,
    recv3,
    dkv,
    drecv,
    send4,
    recv4,
    g_s,
    pg_s,
    pa_s,
    xsend,
    xrel,
    xacc,
    xin,
    zsend,
    zrecv,
    ysend,
    yrecv,
    stat_s,
    qf_s,
    top_s,
    acc_s,
    load_sem,
    snd,
    rcv,
    r1,
    r1v,
    d1r,
    r3,
    dkr,
    xs,
    xr,
):
    x = lax.axis_index("dp_0")
    z = lax.axis_index("dp_1")
    y = lax.axis_index("patch_0")
    k = lax.axis_index("patch_1")
    other = 1 - k
    p = 2 * y + k
    zh = nz // 2
    scale = 1.0 / math.sqrt(HEAD_DIM)

    loads = [
        pltpu.make_async_copy(src, dst, load_sem.at[n])
        for n, (src, dst) in enumerate(
            (
                (q_hbm, q_s),
                (k_hbm, k_s),
                (seg_hbm, seg_s),
                (v_hbm, v_s),
                (w_hbm, w_s),
                (t_hbm, t_s),
            )
        )
    ]
    for c in loads:
        c.start()

    barrier = pltpu.get_barrier_semaphore()
    for i in range(1, 8):
        peer = lax.rem(y + i, 8)
        pl.semaphore_signal(barrier, inc=1, device_id={"patch_0": peer})
        pl.semaphore_signal(barrier, inc=1, device_id={"patch_0": peer, "patch_1": other})
    pl.semaphore_signal(barrier, inc=1, device_id={"patch_1": other})
    for i in range(1, nx):
        pl.semaphore_signal(barrier, inc=1, device_id={"dp_0": lax.rem(x + i, nx)})
    for i in range(1, nz):
        pl.semaphore_signal(barrier, inc=1, device_id={"dp_1": lax.rem(z + i, nz)})

    def remote(src, dst, ssem, rsem, **where):
        return pltpu.make_async_remote_copy(
            src_ref=src, dst_ref=dst, send_sem=ssem, recv_sem=rsem, device_id=where
        )

    row = lax.broadcasted_iota(jnp.int32, (8, ROWS), 0)
    lane = lax.broadcasted_iota(jnp.int32, (8, ROWS), 1)
    for c in loads[:4]:
        c.wait()
    length = len_ref[0]
    live_t = p * ROWS + lane < length
    code = jnp.where(live_t, jnp.broadcast_to(seg_s[...], (8, ROWS)), 8)
    low = jnp.bitwise_and(row, 3)
    weight = jnp.where(low == 0, 1, jnp.where(low == 1, 2, jnp.where(low == 2, 4, 8)))
    bit = jnp.where(jnp.bitwise_and(code, weight) != 0, 1.0, 0.0).astype(F32)
    mine = jnp.where(row < 4, bit, 1.0 - bit)
    q_mask = -MASK * mine
    parts = [ref[0].astype(F32) for ref in (k_s, q_s, v_s)]
    for h in range(HEADS):
        keys, asks, vals = [a[HEAD_DIM * h : HEAD_DIM * (h + 1)] for a in parts]
        send1[h] = jnp.concatenate([keys, asks, q_mask, vals], axis=0).astype(BF)
    recv1[0, y] = send1[y]

    recv3[...] = jnp.zeros_like(recv3)
    pl.semaphore_wait(barrier, 15 + (nx - 1) + (nz - 1))

    qk = pl.ds(0, 2 * HEAD_DIM + 8)
    ko = pl.ds(0, HEAD_DIM)
    vo = pl.ds(2 * HEAD_DIM + 8, HEAD_DIM)
    mo = pl.ds(2 * HEAD_DIM, PAD)

    def spread(rows, n, rsem):
        for i in FAR:
            h = lax.rem(y + i, 8)
            remote(
                send1.at[h, rows], recv1.at[0, y, rows], snd.at[n], rsem.at[i], patch_0=h
            ).start()

    def block_in(i, rows, rsem):
        b = recv1.at[0, source(i), rows]
        remote(b, b, snd.at[0], rsem.at[i], patch_0=y).wait_recv()

    spread(qk, 0, r1)
    spread(vo, 1, r1v)

    def source(i):
        return lax.rem(y - i + 8, 8)

    def pass_on(i, rows, n, rsem):
        return remote(
            recv1.at[0, source(i), rows],
            recv1.at[1, source(i), rows],
            snd.at[n],
            rsem,
            patch_1=other,
        )

    def row_block(src, c=0):
        return pl.ds(pl.multiple_of((8 * c + src) * ROWS, ROWS), ROWS)

    def take(src):
        asks = recv1[0, src, HEAD_DIM : 2 * HEAD_DIM + 8, :].astype(F32)
        qf_s[src] = asks.astype(BF)
        keys = recv1[0, src, 0:HEAD_DIM, :].astype(F32)
        keys = jnp.concatenate([keys, MASK + asks[HEAD_DIM:]], axis=0)
        ktok[row_block(src), :] = keys.T.astype(BF)

    def pass_keys(i):
        at = pl.multiple_of(source(i) * ROWS, ROWS)
        return remote(
            ktok.at[pl.ds(at, ROWS)],
            ktok.at[pl.ds(8 * ROWS + at, ROWS)],
            snd.at[16],
            d1r.at[i],
            patch_1=other,
        )

    passed = [pass_on(i, ko, 2, rcv.at[8]) for i in range(8)]
    passed_v = [pass_on(i, mo, 3, rcv.at[9]) for i in range(8)]
    take(y)
    pass_keys(0).start()
    passed[0].start()
    passed_v[0].start()

    loads[4].wait()
    loads[5].wait()

    def turn(c, carry):
        at = pl.ds(pl.multiple_of(c * ROWS, ROWS), ROWS)
        wt_s[at, :] = w_s[:, at].astype(F32).T.astype(BF)
        tt_s[at, :] = t_s[0, :, at].astype(F32).T
        return carry

    lax.fori_loop(0, WIDTH // ROWS, turn, 0)
    for i in NEAR:
        block_in(i, qk, r1)
        take(source(i))
        pass_keys(i).start()
        passed[i].start()

    factor = scale * math.log2(math.e)
    pair = y // 2
    mate = y + 1 - 2 * lax.rem(y, 2)
    half = 8 * ROWS

    def queries(j):
        return jnp.concatenate([qf_s[2 * j], qf_s[2 * j + 1]], axis=1)

    def forward_half(j, c):
        scores = dot(ktok[half * c : half * (c + 1), :], queries(j), 1, 0)
        top = jnp.max(scores, axis=0, keepdims=True)
        p_s[j, half * c : half * (c + 1), :] = jnp.exp2((scores - top) * factor).astype(BF)
        return top

    def forward_own(j, carry):
        top_s[j] = jnp.broadcast_to(forward_half(j, 0), (8, 2 * ROWS))
        return carry

    lax.fori_loop(0, 4, forward_own, 0)
    for i in (0,) + NEAR:
        pass_keys(i).wait_recv()

    def forward_other(j, carry):
        top = forward_half(j, 1)
        mine = top_s[j, 0:1, :]
        best = jnp.maximum(mine, top)
        for c, one in enumerate((mine, top)):
            w_half[c, j] = jnp.broadcast_to(jnp.exp2((one - best) * factor), (8, 2 * ROWS))
        return carry

    lax.fori_loop(0, 4, forward_other, 0)
    for i in NEAR:
        block_in(i, vo, r1v)
        passed_v[i].start()

    def lanes(c, start, end):
        return jnp.concatenate([recv1[c, src, start:end, :] for src in range(8)], axis=1)

    def values(c):
        return lanes(c, 2 * HEAD_DIM, 3 * HEAD_DIM + 8)

    def values_own(j, carry):
        acc_s[j] = dot(values(0), p_s[j, 0:half, :], 1, 0)
        return carry

    lax.fori_loop(0, 4, values_own, 0)
    crossed = recv1.at[1, :, mo]
    remote(crossed, crossed, snd.at[3], rcv.at[9], patch_0=y).wait_recv()

    head = pl.ds(8, HEAD_DIM)

    def send_attn(s):
        return remote(
            send2.at[s, head], recv2.at[y, head], snd.at[4], rcv.at[0], patch_0=s
        )

    for step_at in (2, 1, 3, 0):
        j = lax.rem(pair + step_at, 4)
        mine, yours = w_half[0, j, 0:1, :], w_half[1, j, 0:1, :]
        accum = acc_s[j] * mine + dot(values(1), p_s[j, half : 2 * half, :], 1, 0) * yours
        rinv = -MASK / (accum[0:1, :] + accum[4:5, :])
        w_half[0, j] = jnp.broadcast_to(mine * rinv, (8, 2 * ROWS))
        w_half[1, j] = jnp.broadcast_to(yours * rinv, (8, 2 * ROWS))
        attn = (accum * rinv).astype(BF)
        send2[2 * j] = attn[:, :ROWS]
        send2[2 * j + 1] = attn[:, ROWS:]
        if step_at:
            send_attn(2 * j).start()
            send_attn(2 * j + 1).start()
        else:
            send_attn(mate).start()
    recv2[y] = send2[y]

    def backward_layouts(src, carry):
        for c in range(2):
            vals = recv1[c, src, 2 * HEAD_DIM : 3 * HEAD_DIM + 8, :]
            vtok[row_block(src, c), :] = vals.astype(F32).T.astype(BF)
        qtok[row_block(src), :] = qf_s[src].astype(F32).T.astype(BF)
        return carry

    lax.fori_loop(0, 8, backward_layouts, 0)

    seven = pl.ds(0, 7)
    remote(
        send2.at[seven, head], recv2.at[seven, head], snd.at[4], rcv.at[0], patch_0=y
    ).wait_recv()
    for h in range(HEADS):
        at_s[HEAD_DIM * h : HEAD_DIM * (h + 1), :] = recv2[h].astype(F32)[8:]
    attn_t = at_s[...].astype(BF)
    pa_s[0] = attn_t
    swap_a = remote(pa_s.at[0], pa_s.at[1], snd.at[5], rcv.at[1], patch_1=other)
    swap_a.start()
    output = dot(wt_s[...], attn_t, 1, 0)
    token = lax.broadcasted_iota(jnp.int32, (WIDTH, ROWS), 1)
    live = p * ROWS + token < length
    error = jnp.where(live, output - tt_s[...], 0.0)
    grad_t = (2.0 * error).astype(BF)
    part = WIDTH // (2 * nx)
    for zhalf in range(2):
        for xx in range(nx):
            at = (2 * xx + zhalf) * part
            g_s[zhalf, part * xx : part * (xx + 1), :] = grad_t[at : at + part]
    swap_g = remote(g_s.at[other], pg_s, snd.at[7], rcv.at[2], patch_1=other)
    swap_g.start()
    grad_attn = dot(w_s[...], grad_t, 1, 0)
    for h in range(HEADS):
        block = jnp.concatenate(
            [jnp.zeros((8, ROWS), F32), grad_attn[HEAD_DIM * h : HEAD_DIM * (h + 1)]], axis=0
        )
        send3[h] = block.astype(BF)
    for i in FAR:
        to = lax.rem(y + i, 8)
        remote(
            send3.at[to, head], recv3.at[y, head], snd.at[6], r3.at[i], patch_0=to
        ).start()
    recv3[y] = send3[y]

    swap_a.wait_recv()
    swap_g.wait_recv()
    right = jnp.concatenate([pa_s[0], pa_s[1]], axis=1)

    def x_chunk(xx):
        at = pl.ds(pl.multiple_of(part * xx, 16), part)
        chunk = dot(jnp.concatenate([g_s[k, at, :], pg_s[at, :]], axis=1), right, 1, 1)
        rest = jnp.concatenate([chunk[: part // 2, 512:], chunk[part // 2 :, 512:]], axis=1)
        for g in range(4):
            xsend[xx, part * g : part * (g + 1), :] = chunk[:, ROWS * g : ROWS * (g + 1)].astype(BF)
        xsend[xx, 4 * part :, :] = jnp.concatenate([rest, jnp.zeros((8, ROWS), F32)], axis=0).astype(BF)

    lo, hi = pl.ds(0, 336), pl.ds(336, 320)
    up, down, across = lax.rem(x + 1, 4), lax.rem(x + 3, 4), lax.rem(x + 2, 4)
    xring = [
        remote(xsend.at[across, lo], xrel.at[lo], xs.at[0], xr.at[0], dp_0=up),
        remote(xsend.at[across, hi], xrel.at[hi], xs.at[1], xr.at[1], dp_0=down),
        remote(xsend.at[up, hi], xin.at[0, hi], xs.at[2], xr.at[2], dp_0=up),
        remote(xsend.at[down, lo], xin.at[1, lo], xs.at[3], xr.at[3], dp_0=down),
        remote(xacc.at[lo], xin.at[0, lo], xs.at[4], xr.at[4], dp_0=up),
        remote(xacc.at[hi], xin.at[1, hi], xs.at[5], xr.at[5], dp_0=down),
    ]
    x_chunk(across)
    xring[0].start()
    xring[1].start()
    x_chunk(up)
    xring[2].start()
    x_chunk(down)
    xring[3].start()
    x_chunk(x)

    def x_relay():
        for n, (rows, size, to) in enumerate(((0, 336, up), (336, 320, down))):
            xring[n].wait_recv()
            xacc[rows : rows + size, :] = (
                xsend[to, rows : rows + size, :].astype(F32)
                + xrel[rows : rows + size, :].astype(F32)
            ).astype(BF)
            xring[4 + n].start()

    squares = jnp.sum(error * error)
    cell = lax.broadcasted_iota(jnp.int32, (8, ROWS), 1)
    stat_s[0] = jnp.where(
        cell == 0, squares, jnp.where(cell == 1, length.astype(F32), 0.0)
    )

    def stat_send(stage, base, n, me, to):
        for i in range(1, n):
            remote(
                stat_s.at[stage],
                stat_s.at[base + i],
                snd.at[8 + stage],
                rcv.at[3 + stage],
                **to(lax.rem(me + i, n)),
            ).start()

    def stat_all(stage, base, n):
        slots = stat_s.at[pl.ds(base + 1, n - 1)]
        return remote(slots, slots, snd.at[8 + stage], rcv.at[3 + stage], patch_0=y)

    def stat_sum(stage, base, n):
        stat_all(stage, base, n).wait_recv()
        acc = stat_s[stage]
        for i in range(1, n):
            acc = acc + stat_s[base + i]
        return acc

    stat_send(0, 3, 16, p, lambda t: {"patch_0": t // 2, "patch_1": lax.rem(t, 2)})
    crossed = recv1.at[1, :, ko]
    remote(crossed, crossed, snd.at[2], rcv.at[8], patch_0=y).wait_recv()

    def send_grad(s, rows, n):
        return remote(
            send4.at[s, rows], recv4.at[y, rows], snd.at[n], rcv.at[n], patch_0=s
        )

    qo = pl.ds(0, HEAD_DIM)
    kvo = pl.ds(PAD, 2 * HEAD_DIM)

    def third_in(s):
        i = lax.rem(y - s + 8, 8)
        remote(
            send3.at[y, head], recv3.at[s, head], snd.at[6], r3.at[i], patch_0=y
        ).wait_recv()

    for step_at in (0, 1, 3, 2):
        j = lax.rem(pair + step_at, 4)
        if step_at:
            third_in(2 * j)
            third_in(2 * j + 1)
        else:
            third_in(mate)
        grads = jnp.concatenate([recv3[2 * j], recv3[2 * j + 1]], axis=1).astype(F32)
        attn = jnp.concatenate([send2[2 * j], send2[2 * j + 1]], axis=1).astype(F32)
        at = pl.ds(pl.multiple_of(j * 2 * ROWS, 2 * ROWS), 2 * ROWS)
        for c in range(2):
            folded = grads * w_half[c, j, 0:1, :]
            dtok[c, at, :] = folded.T.astype(BF)
            folded = folded.astype(BF)
            delta = jnp.sum(folded.astype(F32) * attn, axis=0, keepdims=True)
            these = slice(half * c, half * (c + 1))
            dprobs = dot(vtok[these, :], folded, 1, 0)
            ds_s[j, these, :] = (p_s[j, these, :].astype(F32) * (dprobs - delta)).astype(BF)
        keys = jnp.concatenate([lanes(0, 0, HEAD_DIM), lanes(1, 0, HEAD_DIM)], axis=1)
        dq = dot(keys, ds_s[j], 1, 0) * scale
        dq = jnp.concatenate([dq, jnp.zeros((8, 2 * ROWS), F32)], axis=0).astype(BF)
        send4[2 * j, 0:PAD, :] = dq[:, :ROWS]
        send4[2 * j + 1, 0:PAD, :] = dq[:, ROWS:]
        if step_at:
            send_grad(2 * j, qo, 11).start()
            send_grad(2 * j + 1, qo, 11).start()
        else:
            send_grad(mate, qo, 11).start()
        if step_at == 1:
            x_relay()

    stat_s[1] = stat_sum(0, 3, 16)
    stat_send(1, 19, nx, x, lambda t: {"dp_0": t})

    def crossing(u):
        two = pl.ds(2 * u, 2)
        return remote(dkv.at[two], drecv.at[two], snd.at[13], dkr.at[u], patch_1=other)

    def key_grads(c, u):
        at = pl.ds(pl.multiple_of((8 * c + 2 * u) * ROWS, 2 * ROWS), 2 * ROWS)
        ds_rows = jnp.concatenate([ds_s[j, at, :] for j in range(4)], axis=1)
        p_rows = jnp.concatenate([p_s[j, at, :] for j in range(4)], axis=1)
        dk = (dot(ds_rows, qtok[...], 1, 0) * scale).T
        dv = dot(p_rows, dtok[c], 1, 0).T
        return jnp.concatenate([dk[:HEAD_DIM], dv[8:]], axis=0)

    cols = part // zh
    active = z // zh == k

    def x_done():
        stat_s[2] = stat_sum(1, 19, nx)
        stat_send(2, 19 + nx, nz, z, lambda t: {"dp_1": t})
        for c in xring[2:]:
            c.wait_recv()
        total = xsend[x].astype(F32) + xin[0].astype(F32) + xin[1].astype(F32)
        for j in range(zh):
            rest = total[4 * part + cols * (j % 2) : 4 * part + cols * (j % 2 + 1)]
            rest = rest[:, 64 * (j // 2) : 64 * (j // 2 + 1)]
            rows = [total[part * g + cols * j : part * g + cols * (j + 1)] for g in range(4)]
            rows += [
                jnp.concatenate([rest[: cols // 2], rest[cols // 2 :]], axis=1),
                jnp.zeros((14, ROWS), F32),
            ]
            zsend[j] = jnp.concatenate(rows, axis=0).astype(BF)
        start = z + jnp.where(active, 2, 0)
        for step_at in (0, 1, 3, 2):
            j = lax.rem(start + step_at, zh)
            to = zh * k + j
            away = lax.rem(to - z + nz, nz)

            @pl.when(to != z)
            def _():
                remote(
                    zsend.at[j], zrecv.at[away], snd.at[14], rcv.at[6], dp_1=to
                ).start()

        @pl.when(active)
        def _():
            zrecv[0] = zsend[lax.rem(z, zh)]

    def other_keys(step_at):
        u = lax.rem(pair + step_at, 4)
        both = key_grads(1, u).astype(BF)
        dkv[2 * u] = both[:, :ROWS]
        dkv[2 * u + 1] = both[:, ROWS:]
        crossing(u).start()

    def own_keys(step_at):
        u = lax.rem(pair + step_at, 4)
        both = key_grads(0, u)
        crossing(u).wait_recv()
        for c in range(2):
            mine = both[:, ROWS * c : ROWS * (c + 1)]
            send4[2 * u + c, PAD:, :] = (mine + drecv[2 * u + c].astype(F32)).astype(BF)
        if step_at:
            send_grad(2 * u, kvo, 12).start()
            send_grad(2 * u + 1, kvo, 12).start()
        else:
            send_grad(mate, kvo, 12).start()

    other_keys(2)
    other_keys(1)
    own_keys(2)
    x_done()
    other_keys(3)
    own_keys(1)
    other_keys(0)
    own_keys(3)
    own_keys(0)

    recv4[y] = send4[y]

    @pl.when(active)
    def _():
        z_all = zrecv.at[pl.ds(1, nz - 1)]
        remote(z_all, z_all, snd.at[14], rcv.at[6], patch_0=y).wait_recv()
        summed = zrecv[0].astype(F32)
        for i in range(1, nz):
            summed = summed + zrecv[i].astype(F32)
        rest = summed[4 * cols : 4 * cols + cols // 2]
        summed = jnp.concatenate(
            [summed[cols * g : cols * (g + 1)] for g in range(4)]
            + [jnp.concatenate([rest[:, :64], rest[:, 64:]], axis=0)],
            axis=1,
        )
        summed = jnp.concatenate([summed, jnp.zeros((48 - cols, FEAT), F32)], axis=0)
        for t in range(16):
            piece = summed[:, 36 * t : 36 * (t + 1)]
            ysend[t, :, 0:108] = jnp.concatenate(
                [piece[0:16], piece[16:32], piece[32:48]], axis=1
            )

    @pl.when(active)
    def _():
        for i in FAR + (0,):
            for c in range(2):
                if i == 0 and c == 1:
                    continue
                to = lax.rem(y + i, 8)
                core = c if i else other
                remote(
                    ysend.at[2 * to + core],
                    yrecv.at[y],
                    snd.at[15],
                    rcv.at[7],
                    patch_0=to,
                    patch_1=core,
                ).start()

    @pl.when(active)
    def _():
        yrecv[y] = ysend[p]

    acc = stat_sum(2, 19 + nx, nz)
    count = acc[0:1, 1:2] / 16.0
    ratio = (nx * nz * 16.0 * ROWS) / count
    st_out[...] = acc[0:1, 0:1] / (count * WIDTH)

    def grad_all(rows, n):
        blocks = recv4.at[seven, rows]
        return remote(blocks, blocks, snd.at[n], rcv.at[n], patch_0=y)

    def emit(start, out):
        rows = slice(start // 16 * 16, (start // 16 + 5) * 16)
        skip = start % 16
        whole = jnp.concatenate(
            [recv4[h, rows, :].astype(F32)[skip : skip + HEAD_DIM] for h in range(HEADS)],
            axis=0,
        )
        out[0] = whole * ratio

    grad_all(qo, 11).wait_recv()
    emit(0, dq_out)
    grad_all(kvo, 12).wait_recv()
    emit(PAD, dk_out)
    emit(PAD + HEAD_DIM, dv_out)

    def y_all(n):
        blocks = yrecv.at[pl.ds(0, n)]
        return remote(blocks, blocks, snd.at[15], rcv.at[7], patch_0=y)

    @pl.when(active)
    def _():
        y_all(7).wait_recv()

    @pl.when(jnp.logical_not(active))
    def _():
        y_all(8).wait_recv()

    final = yrecv[0]
    for i in range(1, 8):
        final = final + yrecv[i]
    final = jnp.concatenate([final[:, 0:36], final[:, 36:72], final[:, 72:108]], axis=0)
    wg_out[...] = final.T[0:36, 0:36] * (ratio / (16.0 * ROWS))

    def drain(ref, n):
        remote(ref, ref, snd.at[n], rcv.at[0], patch_0=y).wait_send()

    drain(send1.at[seven, qk], 0)
    drain(send1.at[seven, vo], 1)
    drain(send1.at[:, ko], 2)
    drain(ktok.at[pl.ds(0, 8 * ROWS)], 16)
    drain(send1.at[:, mo], 3)
    drain(send2.at[seven, head], 4)
    drain(pa_s.at[0], 5)
    drain(send3.at[seven, head], 6)
    drain(pg_s, 7)
    stat_all(0, 3, 16).wait_send()
    stat_all(1, 19, nx).wait_send()
    stat_all(2, 19 + nx, nz).wait_send()
    drain(send4.at[seven, qo], 11)
    drain(send4.at[seven, kvo], 12)
    drain(drecv, 13)
    for c in xring:
        c.wait_send()

    @pl.when(active)
    def _():
        drain(zsend.at[pl.ds(0, zh - 1)], 14)
        drain(ysend.at[pl.ds(0, 15)], 15)

    @pl.when(jnp.logical_not(active))
    def _():
        drain(zsend, 14)


def write_out(*refs):
    n = len(refs) // 2
    copies = [
        pltpu.make_async_copy(refs[i], refs[n + i], refs[-1].at[i]) for i in range(n)
    ]
    for c in copies:
        c.start()
    for c in copies:
        c.wait()


def step(nx, nz, query_rows, key_rows, value_rows, out_weight, target, lengths, segments):
    part = WIDTH // (2 * nx)
    zh = nz // 2
    dma = pltpu.SemaphoreType.DMA
    scratch = [
        pltpu.VMEM((1, FEAT, ROWS), BF),
        pltpu.VMEM((1, FEAT, ROWS), BF),
        pltpu.VMEM((1, FEAT, ROWS), BF),
        pltpu.VMEM((1, ROWS), jnp.int32),
        pltpu.VMEM((FEAT, WIDTH), BF),
        pltpu.VMEM((1, ROWS, WIDTH), BF),
        pltpu.VMEM((WIDTH, FEAT), BF),
        pltpu.VMEM((WIDTH, ROWS), F32),
        pltpu.VMEM((8, 3 * HEAD_DIM + 8, ROWS), BF),
        pltpu.VMEM((2, 8, 3 * HEAD_DIM + 8, ROWS), BF),
        pltpu.VMEM((2048, PAD), BF),
        pltpu.VMEM((2048, PAD), BF),
        pltpu.VMEM((1024, PAD), BF),
        pltpu.VMEM((2, 1024, PAD), BF),
        pltpu.VMEM((4, 2048, 256), BF),
        pltpu.VMEM((4, 2048, 256), BF),
        pltpu.VMEM((2, 4, 8, 256), F32),
        pltpu.VMEM((8, PAD, ROWS), BF),
        pltpu.VMEM((8, PAD, ROWS), BF),
        pltpu.VMEM((FEAT, ROWS), F32),
        pltpu.VMEM((8, PAD, ROWS), BF),
        pltpu.VMEM((8, PAD, ROWS), BF),
        pltpu.VMEM((8, 2 * HEAD_DIM, ROWS), BF),
        pltpu.VMEM((8, 2 * HEAD_DIM, ROWS), BF),
        pltpu.VMEM((8, PAD + 2 * HEAD_DIM, ROWS), BF),
        pltpu.VMEM((8, PAD + 2 * HEAD_DIM, ROWS), BF),
        pltpu.VMEM((2, FEAT, ROWS), BF),
        pltpu.VMEM((FEAT, ROWS), BF),
        pltpu.VMEM((2, FEAT, ROWS), BF),
        pltpu.VMEM((nx, 656, ROWS), BF),
        pltpu.VMEM((656, ROWS), BF),
        pltpu.VMEM((656, ROWS), BF),
        pltpu.VMEM((2, 656, ROWS), BF),
        pltpu.VMEM((zh, 176, ROWS), BF),
        pltpu.VMEM((nz, 176, ROWS), BF),
        pltpu.VMEM((16, 16, 128), F32),
        pltpu.VMEM((8, 16, 128), F32),
        pltpu.VMEM((19 + nx + nz, 8, ROWS), F32),
        pltpu.VMEM((8, PAD, ROWS), BF),
        pltpu.VMEM((4, 8, 256), F32),
        pltpu.VMEM((4, PAD, 256), F32),
    ]
    sems = [6, 17, 13, 8, 8, 8, 8, 4, 6, 6]
    vmem = pl.BlockSpec(memory_space=pltpu.VMEM)
    hbm = pl.BlockSpec(memory_space=pltpu.HBM)
    wide = jax.ShapeDtypeStruct((1, FEAT, ROWS), F32)
    results = (
        wide,
        wide,
        wide,
        jax.ShapeDtypeStruct((36, 36), F32),
        jax.ShapeDtypeStruct((1, 1), F32),
    )
    far = lambda a: pltpu.with_memory_space_constraint(a, pltpu.HBM)
    grads = pl.pallas_call(
        functools.partial(body, nx, nz),
        out_shape=results,
        in_specs=[hbm] * 4 + [pl.BlockSpec(memory_space=pltpu.SMEM), hbm, hbm],
        out_specs=(vmem,) * 5,
        scratch_shapes=scratch + [dma((n,)) for n in sems],
        compiler_params=pltpu.CompilerParams(
            collective_id=0, has_side_effects=True, vmem_limit_bytes=40 * 1024 * 1024
        ),
    )(
        far(jnp.swapaxes(query_rows, 1, 2)),
        far(jnp.swapaxes(key_rows, 1, 2)),
        far(jnp.swapaxes(value_rows, 1, 2)),
        far(segments),
        lengths,
        far(out_weight),
        far(target),
    )
    dq, dk, dv, wg, st = pl.pallas_call(
        write_out,
        out_shape=results,
        in_specs=[pl.BlockSpec(memory_space=pl.ANY)] * 5,
        out_specs=(hbm,) * 5,
        scratch_shapes=[dma((5,))],
        compiler_params=pltpu.CompilerParams(vmem_limit_bytes=2 * 1024 * 1024),
    )(*grads)
    return (
        jnp.swapaxes(dq, 1, 2),
        jnp.swapaxes(dk, 1, 2),
        jnp.swapaxes(dv, 1, 2),
        wg,
        st[0, 0],
    )


def solution(mesh):
    torus = Mesh(mesh.devices.reshape(4, 8, 8, 2), ("dp_0", "dp_1", "patch_0", "patch_1"))
    return jax.shard_map(
        functools.partial(step, 4, 8),
        mesh=torus,
        in_specs=(
            P(DP, PATCH, None),
            P(DP, PATCH, None),
            P(DP, PATCH, None),
            P(),
            P(DP, PATCH, None),
            P(DP),
            P(DP, PATCH),
        ),
        out_specs=(P(DP, PATCH, None), P(DP, PATCH, None), P(DP, PATCH, None), P(PATCH, DP), P()),
        check_vma=False,
    )
```

```python
import functools
import math

import jax
import jax.numpy as jnp
from jax import lax
from jax.experimental import pallas as pl
from jax.experimental.pallas import tpu as pltpu
from jax.sharding import Mesh
from jax.sharding import PartitionSpec as P

WIDTH = 1152
HEADS = 8
HEAD_DIM = 72
FEAT = 576
ROWS = 128
PAD = 80
PATCH = ("patch_0", "patch_1")
DP = ("dp_0", "dp_1")
BF = jnp.bfloat16
F32 = jnp.float32
FAR = (4, 3, 5, 2, 6, 1, 7)
NEAR = (1, 7, 2, 6, 3, 5, 4)
MASK = 2.0**50


def dot(a, b, ca, cb):
    return lax.dot_general(a, b, (((ca,), (cb,)), ((), ())), preferred_element_type=F32)


def body(
    nx,
    nz,
    q_hbm,
    k_hbm,
    v_hbm,
    seg_hbm,
    len_ref,
    w_hbm,
    t_hbm,
    dq_out,
    dk_out,
    dv_out,
    wg_out,
    st_out,
    q_s,
    k_s,
    v_s,
    seg_s,
    w_s,
    t_s,
    send1,
    recv1,
    ktok,
    vtok,
    qtok,
    dtok,
    p_s,
    ds_s,
    w_half,
    send2,
    recv2,
    at_s,
    send3,
    recv3,
    dkv,
    drecv,
    send4,
    recv4,
    g_s,
    pg_s,
    pa_s,
    xsend,
    xrel,
    xacc,
    xin,
    zsend,
    zrecv,
    ysend,
    yrecv,
    stat_s,
    qf_s,
    top_s,
    acc_s,
    load_sem,
    snd,
    rcv,
    r1,
    r1v,
    d1r,
    r3,
    dkr,
    xs,
    xr,
):
    x = lax.axis_index("dp_0")
    z = lax.axis_index("dp_1")
    y = lax.axis_index("patch_0")
    k = lax.axis_index("patch_1")
    other = 1 - k
    p = 2 * y + k
    zh = nz // 2
    scale = 1.0 / math.sqrt(HEAD_DIM)

    loads = [
        pltpu.make_async_copy(src, dst, load_sem.at[n])
        for n, (src, dst) in enumerate(
            (
                (q_hbm, q_s),
                (k_hbm, k_s),
                (seg_hbm, seg_s),
                (v_hbm, v_s),
                (w_hbm, w_s),
                (t_hbm, t_s),
            )
        )
    ]
    for c in loads:
        c.start()

    barrier = pltpu.get_barrier_semaphore()
    for i in range(1, 8):
        peer = lax.rem(y + i, 8)
        pl.semaphore_signal(barrier, inc=1, device_id={"patch_0": peer})
        pl.semaphore_signal(barrier, inc=1, device_id={"patch_0": peer, "patch_1": other})
    pl.semaphore_signal(barrier, inc=1, device_id={"patch_1": other})
    for i in range(1, nx):
        pl.semaphore_signal(barrier, inc=1, device_id={"dp_0": lax.rem(x + i, nx)})
    for i in range(1, nz):
        pl.semaphore_signal(barrier, inc=1, device_id={"dp_1": lax.rem(z + i, nz)})

    def remote(src, dst, ssem, rsem, **where):
        return pltpu.make_async_remote_copy(
            src_ref=src, dst_ref=dst, send_sem=ssem, recv_sem=rsem, device_id=where
        )

    row = lax.broadcasted_iota(jnp.int32, (8, ROWS), 0)
    lane = lax.broadcasted_iota(jnp.int32, (8, ROWS), 1)
    for c in loads[:4]:
        c.wait()
    length = len_ref[0]
    live_t = p * ROWS + lane < length
    code = jnp.where(live_t, jnp.broadcast_to(seg_s[...], (8, ROWS)), 8)
    low = jnp.bitwise_and(row, 3)
    weight = jnp.where(low == 0, 1, jnp.where(low == 1, 2, jnp.where(low == 2, 4, 8)))
    bit = jnp.where(jnp.bitwise_and(code, weight) != 0, 1.0, 0.0).astype(F32)
    mine = jnp.where(row < 4, bit, 1.0 - bit)
    q_mask = -MASK * mine
    parts = [ref[0].astype(F32) for ref in (k_s, q_s, v_s)]
    for h in range(HEADS):
        keys, asks, vals = [a[HEAD_DIM * h : HEAD_DIM * (h + 1)] for a in parts]
        send1[h] = jnp.concatenate([keys, asks, q_mask, vals], axis=0).astype(BF)
    recv1[0, y] = send1[y]

    recv3[...] = jnp.zeros_like(recv3)
    pl.semaphore_wait(barrier, 15 + (nx - 1) + (nz - 1))

    qk = pl.ds(0, 2 * HEAD_DIM + 8)
    ko = pl.ds(0, HEAD_DIM)
    vo = pl.ds(2 * HEAD_DIM + 8, HEAD_DIM)
    mo = pl.ds(2 * HEAD_DIM, PAD)

    def spread(rows, n, rsem):
        for i in FAR:
            h = lax.rem(y + i, 8)
            remote(
                send1.at[h, rows], recv1.at[0, y, rows], snd.at[n], rsem.at[i], patch_0=h
            ).start()

    def block_in(i, rows, rsem):
        b = recv1.at[0, source(i), rows]
        remote(b, b, snd.at[0], rsem.at[i], patch_0=y).wait_recv()

    spread(qk, 0, r1)
    spread(vo, 1, r1v)

    def source(i):
        return lax.rem(y - i + 8, 8)

    def pass_on(i, rows, n, rsem):
        return remote(
            recv1.at[0, source(i), rows],
            recv1.at[1, source(i), rows],
            snd.at[n],
            rsem,
            patch_1=other,
        )

    def row_block(src, c=0):
        return pl.ds(pl.multiple_of((8 * c + src) * ROWS, ROWS), ROWS)

    def take(src):
        asks = recv1[0, src, HEAD_DIM : 2 * HEAD_DIM + 8, :].astype(F32)
        qf_s[src] = asks.astype(BF)
        keys = recv1[0, src, 0:HEAD_DIM, :].astype(F32)
        keys = jnp.concatenate([keys, MASK + asks[HEAD_DIM:]], axis=0)
        ktok[row_block(src), :] = keys.T.astype(BF)

    def pass_keys(i):
        at = pl.multiple_of(source(i) * ROWS, ROWS)
        return remote(
            ktok.at[pl.ds(at, ROWS)],
            ktok.at[pl.ds(8 * ROWS + at, ROWS)],
            snd.at[16],
            d1r.at[i],
            patch_1=other,
        )

    passed = [pass_on(i, ko, 2, rcv.at[8]) for i in range(8)]
    passed_v = [pass_on(i, mo, 3, rcv.at[9]) for i in range(8)]
    take(y)
    pass_keys(0).start()
    passed[0].start()
    passed_v[0].start()
    for i in NEAR:
        block_in(i, qk, r1)
        take(source(i))
        pass_keys(i).start()
        passed[i].start()

    factor = scale * math.log2(math.e)
    pair = y // 2
    mate = y + 1 - 2 * lax.rem(y, 2)
    half = 8 * ROWS

    def queries(j):
        return jnp.concatenate([qf_s[2 * j], qf_s[2 * j + 1]], axis=1)

    def forward_half(j, c):
        scores = dot(ktok[half * c : half * (c + 1), :], queries(j), 1, 0)
        top = jnp.max(scores, axis=0, keepdims=True)
        p_s[j, half * c : half * (c + 1), :] = jnp.exp2((scores - top) * factor).astype(BF)
        return top

    def forward_own(j, carry):
        top_s[j] = jnp.broadcast_to(forward_half(j, 0), (8, 2 * ROWS))
        return carry

    lax.fori_loop(0, 4, forward_own, 0)
    for i in (0,) + NEAR:
        pass_keys(i).wait_recv()

    def forward_other(j, carry):
        top = forward_half(j, 1)
        mine = top_s[j, 0:1, :]
        best = jnp.maximum(mine, top)
        for c, one in enumerate((mine, top)):
            w_half[c, j] = jnp.broadcast_to(jnp.exp2((one - best) * factor), (8, 2 * ROWS))
        return carry

    lax.fori_loop(0, 4, forward_other, 0)
    for i in NEAR:
        block_in(i, vo, r1v)
        passed_v[i].start()

    def lanes(c, start, end):
        return jnp.concatenate([recv1[c, src, start:end, :] for src in range(8)], axis=1)

    def values(c):
        return lanes(c, 2 * HEAD_DIM, 3 * HEAD_DIM + 8)

    def values_own(j, carry):
        acc_s[j] = dot(values(0), p_s[j, 0:half, :], 1, 0)
        return carry

    lax.fori_loop(0, 4, values_own, 0)
    crossed = recv1.at[1, :, mo]
    remote(crossed, crossed, snd.at[3], rcv.at[9], patch_0=y).wait_recv()

    head = pl.ds(8, HEAD_DIM)

    def send_attn(s):
        return remote(
            send2.at[s, head], recv2.at[y, head], snd.at[4], rcv.at[0], patch_0=s
        )

    for step_at in (2, 1, 3, 0):
        j = lax.rem(pair + step_at, 4)
        mine, yours = w_half[0, j, 0:1, :], w_half[1, j, 0:1, :]
        accum = acc_s[j] * mine + dot(values(1), p_s[j, half : 2 * half, :], 1, 0) * yours
        rinv = -MASK / (accum[0:1, :] + accum[4:5, :])
        w_half[0, j] = jnp.broadcast_to(mine * rinv, (8, 2 * ROWS))
        w_half[1, j] = jnp.broadcast_to(yours * rinv, (8, 2 * ROWS))
        attn = (accum * rinv).astype(BF)
        send2[2 * j] = attn[:, :ROWS]
        send2[2 * j + 1] = attn[:, ROWS:]
        if step_at:
            send_attn(2 * j).start()
            send_attn(2 * j + 1).start()
        else:
            send_attn(mate).start()
    recv2[y] = send2[y]

    def backward_layouts(src, carry):
        for c in range(2):
            vals = recv1[c, src, 2 * HEAD_DIM : 3 * HEAD_DIM + 8, :]
            vtok[row_block(src, c), :] = vals.astype(F32).T.astype(BF)
        qtok[row_block(src), :] = qf_s[src].astype(F32).T.astype(BF)
        return carry

    lax.fori_loop(0, 8, backward_layouts, 0)

    loads[4].wait()
    loads[5].wait()
    seven = pl.ds(0, 7)
    remote(
        send2.at[seven, head], recv2.at[seven, head], snd.at[4], rcv.at[0], patch_0=y
    ).wait_recv()
    for h in range(HEADS):
        at_s[HEAD_DIM * h : HEAD_DIM * (h + 1), :] = recv2[h].astype(F32)[8:]
    attn_t = at_s[...].astype(BF)
    pa_s[0] = attn_t
    swap_a = remote(pa_s.at[0], pa_s.at[1], snd.at[5], rcv.at[1], patch_1=other)
    swap_a.start()
    output = dot(attn_t, w_s[...], 0, 0)
    token = lax.broadcasted_iota(jnp.int32, (ROWS, WIDTH), 0)
    live = p * ROWS + token < length
    error = jnp.where(live, output - t_s[0].astype(F32), 0.0)
    grad_out = (2.0 * error).astype(BF)
    grad_t = (2.0 * error).T.astype(BF)
    part = WIDTH // (2 * nx)
    for zhalf in range(2):
        for xx in range(nx):
            at = (2 * xx + zhalf) * part
            g_s[zhalf, part * xx : part * (xx + 1), :] = grad_t[at : at + part]
    swap_g = remote(g_s.at[other], pg_s, snd.at[7], rcv.at[2], patch_1=other)
    swap_g.start()
    grad_attn = dot(w_s[...], grad_t, 1, 0)
    for h in range(HEADS):
        block = jnp.concatenate(
            [jnp.zeros((8, ROWS), F32), grad_attn[HEAD_DIM * h : HEAD_DIM * (h + 1)]], axis=0
        )
        send3[h] = block.astype(BF)
    for i in FAR:
        to = lax.rem(y + i, 8)
        remote(
            send3.at[to, head], recv3.at[y, head], snd.at[6], r3.at[i], patch_0=to
        ).start()
    recv3[y] = send3[y]

    swap_a.wait_recv()
    swap_g.wait_recv()
    right = jnp.concatenate([pa_s[0], pa_s[1]], axis=1)

    def x_chunk(xx):
        at = pl.ds(pl.multiple_of(part * xx, 16), part)
        chunk = dot(jnp.concatenate([g_s[k, at, :], pg_s[at, :]], axis=1), right, 1, 1)
        rest = jnp.concatenate([chunk[: part // 2, 512:], chunk[part // 2 :, 512:]], axis=1)
        for g in range(4):
            xsend[xx, part * g : part * (g + 1), :] = chunk[:, ROWS * g : ROWS * (g + 1)].astype(BF)
        xsend[xx, 4 * part :, :] = jnp.concatenate([rest, jnp.zeros((8, ROWS), F32)], axis=0).astype(BF)

    lo, hi = pl.ds(0, 336), pl.ds(336, 320)
    up, down, across = lax.rem(x + 1, 4), lax.rem(x + 3, 4), lax.rem(x + 2, 4)
    xring = [
        remote(xsend.at[across, lo], xrel.at[lo], xs.at[0], xr.at[0], dp_0=up),
        remote(xsend.at[across, hi], xrel.at[hi], xs.at[1], xr.at[1], dp_0=down),
        remote(xsend.at[up, hi], xin.at[0, hi], xs.at[2], xr.at[2], dp_0=up),
        remote(xsend.at[down, lo], xin.at[1, lo], xs.at[3], xr.at[3], dp_0=down),
        remote(xacc.at[lo], xin.at[0, lo], xs.at[4], xr.at[4], dp_0=up),
        remote(xacc.at[hi], xin.at[1, hi], xs.at[5], xr.at[5], dp_0=down),
    ]
    x_chunk(across)
    xring[0].start()
    xring[1].start()
    x_chunk(up)
    xring[2].start()
    x_chunk(down)
    xring[3].start()
    x_chunk(x)

    def x_relay():
        for n, (rows, size, to) in enumerate(((0, 336, up), (336, 320, down))):
            xring[n].wait_recv()
            xacc[rows : rows + size, :] = (
                xsend[to, rows : rows + size, :].astype(F32)
                + xrel[rows : rows + size, :].astype(F32)
            ).astype(BF)
            xring[4 + n].start()

    squares = jnp.sum(error * error)
    cell = lax.broadcasted_iota(jnp.int32, (8, ROWS), 1)
    stat_s[0] = jnp.where(
        cell == 0, squares, jnp.where(cell == 1, length.astype(F32), 0.0)
    )

    def stat_send(stage, base, n, me, to):
        for i in range(1, n):
            remote(
                stat_s.at[stage],
                stat_s.at[base + i],
                snd.at[8 + stage],
                rcv.at[3 + stage],
                **to(lax.rem(me + i, n)),
            ).start()

    def stat_all(stage, base, n):
        slots = stat_s.at[pl.ds(base + 1, n - 1)]
        return remote(slots, slots, snd.at[8 + stage], rcv.at[3 + stage], patch_0=y)

    def stat_sum(stage, base, n):
        stat_all(stage, base, n).wait_recv()
        acc = stat_s[stage]
        for i in range(1, n):
            acc = acc + stat_s[base + i]
        return acc

    stat_send(0, 3, 16, p, lambda t: {"patch_0": t // 2, "patch_1": lax.rem(t, 2)})
    crossed = recv1.at[1, :, ko]
    remote(crossed, crossed, snd.at[2], rcv.at[8], patch_0=y).wait_recv()

    def send_grad(s, rows, n):
        return remote(
            send4.at[s, rows], recv4.at[y, rows], snd.at[n], rcv.at[n], patch_0=s
        )

    qo = pl.ds(0, HEAD_DIM)
    kvo = pl.ds(PAD, 2 * HEAD_DIM)

    def third_in(s):
        i = lax.rem(y - s + 8, 8)
        remote(
            send3.at[y, head], recv3.at[s, head], snd.at[6], r3.at[i], patch_0=y
        ).wait_recv()

    for step_at in (0, 1, 3, 2):
        j = lax.rem(pair + step_at, 4)
        if step_at:
            third_in(2 * j)
            third_in(2 * j + 1)
        else:
            third_in(mate)
        grads = jnp.concatenate([recv3[2 * j], recv3[2 * j + 1]], axis=1).astype(F32)
        attn = jnp.concatenate([send2[2 * j], send2[2 * j + 1]], axis=1).astype(F32)
        at = pl.ds(pl.multiple_of(j * 2 * ROWS, 2 * ROWS), 2 * ROWS)
        for c in range(2):
            folded = grads * w_half[c, j, 0:1, :]
            dtok[c, at, :] = folded.T.astype(BF)
            folded = folded.astype(BF)
            delta = jnp.sum(folded.astype(F32) * attn, axis=0, keepdims=True)
            these = slice(half * c, half * (c + 1))
            dprobs = dot(vtok[these, :], folded, 1, 0)
            ds_s[j, these, :] = (p_s[j, these, :].astype(F32) * (dprobs - delta)).astype(BF)
        keys = jnp.concatenate([lanes(0, 0, HEAD_DIM), lanes(1, 0, HEAD_DIM)], axis=1)
        dq = dot(keys, ds_s[j], 1, 0) * scale
        dq = jnp.concatenate([dq, jnp.zeros((8, 2 * ROWS), F32)], axis=0).astype(BF)
        send4[2 * j, 0:PAD, :] = dq[:, :ROWS]
        send4[2 * j + 1, 0:PAD, :] = dq[:, ROWS:]
        if step_at:
            send_grad(2 * j, qo, 11).start()
            send_grad(2 * j + 1, qo, 11).start()
        else:
            send_grad(mate, qo, 11).start()
        if step_at == 0:
            x_relay()

    stat_s[1] = stat_sum(0, 3, 16)
    stat_send(1, 19, nx, x, lambda t: {"dp_0": t})

    def crossing(u):
        two = pl.ds(2 * u, 2)
        return remote(dkv.at[two], drecv.at[two], snd.at[13], dkr.at[u], patch_1=other)

    def key_grads(c, u):
        at = pl.ds(pl.multiple_of((8 * c + 2 * u) * ROWS, 2 * ROWS), 2 * ROWS)
        ds_rows = jnp.concatenate([ds_s[j, at, :] for j in range(4)], axis=1)
        p_rows = jnp.concatenate([p_s[j, at, :] for j in range(4)], axis=1)
        dk = (dot(ds_rows, qtok[...], 1, 0) * scale).T
        dv = dot(p_rows, dtok[c], 1, 0).T
        return jnp.concatenate([dk[:HEAD_DIM], dv[8:]], axis=0)

    cols = part // zh
    active = z // zh == k

    def x_done():
        for c in xring[2:]:
            c.wait_recv()
        total = xsend[x].astype(F32) + xin[0].astype(F32) + xin[1].astype(F32)
        for j in range(zh):
            rest = total[4 * part + cols * (j % 2) : 4 * part + cols * (j % 2 + 1)]
            rest = rest[:, 64 * (j // 2) : 64 * (j // 2 + 1)]
            rows = [total[part * g + cols * j : part * g + cols * (j + 1)] for g in range(4)]
            rows += [
                jnp.concatenate([rest[: cols // 2], rest[cols // 2 :]], axis=1),
                jnp.zeros((14, ROWS), F32),
            ]
            zsend[j] = jnp.concatenate(rows, axis=0).astype(BF)
        start = z + jnp.where(active, 2, 0)
        for step_at in (0, 1, 3, 2):
            j = lax.rem(start + step_at, zh)
            to = zh * k + j
            away = lax.rem(to - z + nz, nz)

            @pl.when(to != z)
            def _():
                remote(
                    zsend.at[j], zrecv.at[away], snd.at[14], rcv.at[6], dp_1=to
                ).start()

        @pl.when(active)
        def _():
            zrecv[0] = zsend[lax.rem(z, zh)]

    def other_keys(step_at):
        u = lax.rem(pair + step_at, 4)
        both = key_grads(1, u).astype(BF)
        dkv[2 * u] = both[:, :ROWS]
        dkv[2 * u + 1] = both[:, ROWS:]
        crossing(u).start()

    def own_keys(step_at):
        u = lax.rem(pair + step_at, 4)
        both = key_grads(0, u)
        crossing(u).wait_recv()
        for c in range(2):
            mine = both[:, ROWS * c : ROWS * (c + 1)]
            send4[2 * u + c, PAD:, :] = (mine + drecv[2 * u + c].astype(F32)).astype(BF)
        if step_at:
            send_grad(2 * u, kvo, 12).start()
            send_grad(2 * u + 1, kvo, 12).start()
        else:
            send_grad(mate, kvo, 12).start()

    x_done()
    other_keys(2)
    other_keys(1)
    own_keys(2)
    stat_s[2] = stat_sum(1, 19, nx)
    stat_send(2, 19 + nx, nz, z, lambda t: {"dp_1": t})
    other_keys(3)
    own_keys(1)
    other_keys(0)
    own_keys(3)
    own_keys(0)

    recv4[y] = send4[y]

    @pl.when(active)
    def _():
        z_all = zrecv.at[pl.ds(1, nz - 1)]
        remote(z_all, z_all, snd.at[14], rcv.at[6], patch_0=y).wait_recv()
        summed = zrecv[0].astype(F32)
        for i in range(1, nz):
            summed = summed + zrecv[i].astype(F32)
        rest = summed[4 * cols : 4 * cols + cols // 2]
        summed = jnp.concatenate(
            [summed[cols * g : cols * (g + 1)] for g in range(4)]
            + [jnp.concatenate([rest[:, :64], rest[:, 64:]], axis=0)],
            axis=1,
        )
        summed = jnp.concatenate([summed, jnp.zeros((48 - cols, FEAT), F32)], axis=0)
        for t in range(16):
            piece = summed[:, 36 * t : 36 * (t + 1)]
            ysend[t, :, 0:108] = jnp.concatenate(
                [piece[0:16], piece[16:32], piece[32:48]], axis=1
            )

    @pl.when(active)
    def _():
        for i in FAR + (0,):
            for c in range(2):
                if i == 0 and c == 1:
                    continue
                to = lax.rem(y + i, 8)
                core = c if i else other
                remote(
                    ysend.at[2 * to + core],
                    yrecv.at[y],
                    snd.at[15],
                    rcv.at[7],
                    patch_0=to,
                    patch_1=core,
                ).start()

    @pl.when(active)
    def _():
        yrecv[y] = ysend[p]

    acc = stat_sum(2, 19 + nx, nz)
    count = acc[0:1, 1:2] / 16.0
    ratio = (nx * nz * 16.0 * ROWS) / count
    st_out[...] = acc[0:1, 0:1] / (count * WIDTH)

    def grad_all(rows, n):
        blocks = recv4.at[seven, rows]
        return remote(blocks, blocks, snd.at[n], rcv.at[n], patch_0=y)

    def emit(start, out):
        rows = slice(start // 16 * 16, (start // 16 + 5) * 16)
        skip = start % 16
        whole = jnp.concatenate(
            [recv4[h, rows, :].astype(F32)[skip : skip + HEAD_DIM] for h in range(HEADS)],
            axis=0,
        )
        out[0] = whole * ratio

    grad_all(qo, 11).wait_recv()
    emit(0, dq_out)
    grad_all(kvo, 12).wait_recv()
    emit(PAD, dk_out)
    emit(PAD + HEAD_DIM, dv_out)

    def y_all(n):
        blocks = yrecv.at[pl.ds(0, n)]
        return remote(blocks, blocks, snd.at[15], rcv.at[7], patch_0=y)

    @pl.when(active)
    def _():
        y_all(7).wait_recv()

    @pl.when(jnp.logical_not(active))
    def _():
        y_all(8).wait_recv()

    final = yrecv[0]
    for i in range(1, 8):
        final = final + yrecv[i]
    final = jnp.concatenate([final[:, 0:36], final[:, 36:72], final[:, 72:108]], axis=0)
    wg_out[...] = final.T[0:36, 0:36] * (ratio / (16.0 * ROWS))

    def drain(ref, n):
        remote(ref, ref, snd.at[n], rcv.at[0], patch_0=y).wait_send()

    drain(send1.at[seven, qk], 0)
    drain(send1.at[seven, vo], 1)
    drain(send1.at[:, ko], 2)
    drain(ktok.at[pl.ds(0, 8 * ROWS)], 16)
    drain(send1.at[:, mo], 3)
    drain(send2.at[seven, head], 4)
    drain(pa_s.at[0], 5)
    drain(send3.at[seven, head], 6)
    drain(pg_s, 7)
    stat_all(0, 3, 16).wait_send()
    stat_all(1, 19, nx).wait_send()
    stat_all(2, 19 + nx, nz).wait_send()
    drain(send4.at[seven, qo], 11)
    drain(send4.at[seven, kvo], 12)
    drain(drecv, 13)
    for c in xring:
        c.wait_send()

    @pl.when(active)
    def _():
        drain(zsend.at[pl.ds(0, zh - 1)], 14)
        drain(ysend.at[pl.ds(0, 15)], 15)

    @pl.when(jnp.logical_not(active))
    def _():
        drain(zsend, 14)


def write_out(*refs):
    n = len(refs) // 2
    copies = [
        pltpu.make_async_copy(refs[i], refs[n + i], refs[-1].at[i]) for i in range(n)
    ]
    for c in copies:
        c.start()
    for c in copies:
        c.wait()


def step(nx, nz, query_rows, key_rows, value_rows, out_weight, target, lengths, segments):
    part = WIDTH // (2 * nx)
    zh = nz // 2
    dma = pltpu.SemaphoreType.DMA
    scratch = [
        pltpu.VMEM((1, FEAT, ROWS), BF),
        pltpu.VMEM((1, FEAT, ROWS), BF),
        pltpu.VMEM((1, FEAT, ROWS), BF),
        pltpu.VMEM((1, ROWS), jnp.int32),
        pltpu.VMEM((FEAT, WIDTH), BF),
        pltpu.VMEM((1, ROWS, WIDTH), BF),
        pltpu.VMEM((8, 3 * HEAD_DIM + 8, ROWS), BF),
        pltpu.VMEM((2, 8, 3 * HEAD_DIM + 8, ROWS), BF),
        pltpu.VMEM((2048, PAD), BF),
        pltpu.VMEM((2048, PAD), BF),
        pltpu.VMEM((1024, PAD), BF),
        pltpu.VMEM((2, 1024, PAD), BF),
        pltpu.VMEM((4, 2048, 256), BF),
        pltpu.VMEM((4, 2048, 256), BF),
        pltpu.VMEM((2, 4, 8, 256), F32),
        pltpu.VMEM((8, PAD, ROWS), BF),
        pltpu.VMEM((8, PAD, ROWS), BF),
        pltpu.VMEM((FEAT, ROWS), F32),
        pltpu.VMEM((8, PAD, ROWS), BF),
        pltpu.VMEM((8, PAD, ROWS), BF),
        pltpu.VMEM((8, 2 * HEAD_DIM, ROWS), BF),
        pltpu.VMEM((8, 2 * HEAD_DIM, ROWS), BF),
        pltpu.VMEM((8, PAD + 2 * HEAD_DIM, ROWS), BF),
        pltpu.VMEM((8, PAD + 2 * HEAD_DIM, ROWS), BF),
        pltpu.VMEM((2, FEAT, ROWS), BF),
        pltpu.VMEM((FEAT, ROWS), BF),
        pltpu.VMEM((2, FEAT, ROWS), BF),
        pltpu.VMEM((nx, 656, ROWS), BF),
        pltpu.VMEM((656, ROWS), BF),
        pltpu.VMEM((656, ROWS), BF),
        pltpu.VMEM((2, 656, ROWS), BF),
        pltpu.VMEM((zh, 176, ROWS), BF),
        pltpu.VMEM((nz, 176, ROWS), BF),
        pltpu.VMEM((16, 16, 128), F32),
        pltpu.VMEM((8, 16, 128), F32),
        pltpu.VMEM((19 + nx + nz, 8, ROWS), F32),
        pltpu.VMEM((8, PAD, ROWS), BF),
        pltpu.VMEM((4, 8, 256), F32),
        pltpu.VMEM((4, PAD, 256), F32),
    ]
    sems = [6, 17, 13, 8, 8, 8, 8, 4, 6, 6]
    vmem = pl.BlockSpec(memory_space=pltpu.VMEM)
    hbm = pl.BlockSpec(memory_space=pltpu.HBM)
    wide = jax.ShapeDtypeStruct((1, FEAT, ROWS), F32)
    results = (
        wide,
        wide,
        wide,
        jax.ShapeDtypeStruct((36, 36), F32),
        jax.ShapeDtypeStruct((1, 1), F32),
    )
    far = lambda a: pltpu.with_memory_space_constraint(a, pltpu.HBM)
    grads = pl.pallas_call(
        functools.partial(body, nx, nz),
        out_shape=results,
        in_specs=[hbm] * 4 + [pl.BlockSpec(memory_space=pltpu.SMEM), hbm, hbm],
        out_specs=(vmem,) * 5,
        scratch_shapes=scratch + [dma((n,)) for n in sems],
        compiler_params=pltpu.CompilerParams(
            collective_id=0, has_side_effects=True, vmem_limit_bytes=40 * 1024 * 1024
        ),
    )(
        far(jnp.swapaxes(query_rows, 1, 2)),
        far(jnp.swapaxes(key_rows, 1, 2)),
        far(jnp.swapaxes(value_rows, 1, 2)),
        far(segments),
        lengths,
        far(out_weight),
        far(target),
    )
    dq, dk, dv, wg, st = pl.pallas_call(
        write_out,
        out_shape=results,
        in_specs=[pl.BlockSpec(memory_space=pl.ANY)] * 5,
        out_specs=(hbm,) * 5,
        scratch_shapes=[dma((5,))],
        compiler_params=pltpu.CompilerParams(vmem_limit_bytes=2 * 1024 * 1024),
    )(*grads)
    return (
        jnp.swapaxes(dq, 1, 2),
        jnp.swapaxes(dk, 1, 2),
        jnp.swapaxes(dv, 1, 2),
        wg,
        st[0, 0],
    )


def solution(mesh):
    torus = Mesh(mesh.devices.reshape(4, 8, 8, 2), ("dp_0", "dp_1", "patch_0", "patch_1"))
    return jax.shard_map(
        functools.partial(step, 4, 8),
        mesh=torus,
        in_specs=(
            P(DP, PATCH, None),
            P(DP, PATCH, None),
            P(DP, PATCH, None),
            P(),
            P(DP, PATCH, None),
            P(DP),
            P(DP, PATCH),
        ),
        out_specs=(P(DP, PATCH, None), P(DP, PATCH, None), P(DP, PATCH, None), P(PATCH, DP), P()),
        check_vma=False,
    )
```

```python
import functools
import math

import jax
import jax.numpy as jnp
from jax import lax
from jax.experimental import pallas as pl
from jax.experimental.pallas import tpu as pltpu
from jax.sharding import Mesh
from jax.sharding import PartitionSpec as P

WIDTH = 1152
HEADS = 8
HEAD_DIM = 72
FEAT = 576
ROWS = 128
PAD = 80
PATCH = ("patch_0", "patch_1")
DP = ("dp_0", "dp_1")
BF = jnp.bfloat16
F32 = jnp.float32
FAR = (4, 3, 5, 2, 6, 1, 7)
NEAR = (1, 7, 2, 6, 3, 5, 4)
MASK = 2.0**50


def dot(a, b, ca, cb):
    return lax.dot_general(a, b, (((ca,), (cb,)), ((), ())), preferred_element_type=F32)


def body(
    nx,
    nz,
    q_hbm,
    k_hbm,
    v_hbm,
    seg_hbm,
    len_ref,
    w_hbm,
    t_hbm,
    dq_out,
    dk_out,
    dv_out,
    wg_out,
    st_out,
    q_s,
    k_s,
    v_s,
    seg_s,
    w_s,
    t_s,
    send1,
    recv1,
    ktok,
    vtok,
    qtok,
    dtok,
    p_s,
    ds_s,
    w_half,
    send2,
    recv2,
    at_s,
    send3,
    recv3,
    dkv,
    drecv,
    send4,
    recv4,
    g_s,
    pg_s,
    pa_s,
    xsend,
    xrel,
    xacc,
    xin,
    zsend,
    zrecv,
    ysend,
    yrecv,
    stat_s,
    qf_s,
    top_s,
    acc_s,
    load_sem,
    snd,
    rcv,
    r1,
    r1v,
    d1r,
    r3,
    dkr,
    xs,
    xr,
):
    x = lax.axis_index("dp_0")
    z = lax.axis_index("dp_1")
    y = lax.axis_index("patch_0")
    k = lax.axis_index("patch_1")
    other = 1 - k
    p = 2 * y + k
    zh = nz // 2
    scale = 1.0 / math.sqrt(HEAD_DIM)

    loads = [
        pltpu.make_async_copy(src, dst, load_sem.at[n])
        for n, (src, dst) in enumerate(
            (
                (q_hbm, q_s),
                (k_hbm, k_s),
                (seg_hbm, seg_s),
                (v_hbm, v_s),
                (w_hbm, w_s),
                (t_hbm, t_s),
            )
        )
    ]
    for c in loads:
        c.start()

    barrier = pltpu.get_barrier_semaphore()
    for i in range(1, 8):
        peer = lax.rem(y + i, 8)
        pl.semaphore_signal(barrier, inc=1, device_id={"patch_0": peer})
        pl.semaphore_signal(barrier, inc=1, device_id={"patch_0": peer, "patch_1": other})
    pl.semaphore_signal(barrier, inc=1, device_id={"patch_1": other})
    for i in range(1, nx):
        pl.semaphore_signal(barrier, inc=1, device_id={"dp_0": lax.rem(x + i, nx)})
    for i in range(1, nz):
        pl.semaphore_signal(barrier, inc=1, device_id={"dp_1": lax.rem(z + i, nz)})

    def remote(src, dst, ssem, rsem, **where):
        return pltpu.make_async_remote_copy(
            src_ref=src, dst_ref=dst, send_sem=ssem, recv_sem=rsem, device_id=where
        )

    row = lax.broadcasted_iota(jnp.int32, (8, ROWS), 0)
    lane = lax.broadcasted_iota(jnp.int32, (8, ROWS), 1)
    for c in loads[:4]:
        c.wait()
    length = len_ref[0]
    live_t = p * ROWS + lane < length
    code = jnp.where(live_t, jnp.broadcast_to(seg_s[...], (8, ROWS)), 8)
    low = jnp.bitwise_and(row, 3)
    weight = jnp.where(low == 0, 1, jnp.where(low == 1, 2, jnp.where(low == 2, 4, 8)))
    bit = jnp.where(jnp.bitwise_and(code, weight) != 0, 1.0, 0.0).astype(F32)
    mine = jnp.where(row < 4, bit, 1.0 - bit)
    q_mask = -MASK * mine
    parts = [ref[0].astype(F32) for ref in (k_s, q_s, v_s)]
    for h in range(HEADS):
        keys, asks, vals = [a[HEAD_DIM * h : HEAD_DIM * (h + 1)] for a in parts]
        send1[h] = jnp.concatenate([keys, asks, q_mask, vals], axis=0).astype(BF)
    recv1[0, y] = send1[y]

    recv3[...] = jnp.zeros_like(recv3)
    pl.semaphore_wait(barrier, 15 + (nx - 1) + (nz - 1))

    qk = pl.ds(0, 2 * HEAD_DIM + 8)
    ko = pl.ds(0, HEAD_DIM)
    vo = pl.ds(2 * HEAD_DIM + 8, HEAD_DIM)
    mo = pl.ds(2 * HEAD_DIM, PAD)

    def spread(rows, n, rsem):
        for i in FAR:
            h = lax.rem(y + i, 8)
            remote(
                send1.at[h, rows], recv1.at[0, y, rows], snd.at[n], rsem.at[i], patch_0=h
            ).start()

    def block_in(i, rows, rsem):
        b = recv1.at[0, source(i), rows]
        remote(b, b, snd.at[0], rsem.at[i], patch_0=y).wait_recv()

    spread(qk, 0, r1)
    spread(vo, 1, r1v)

    def source(i):
        return lax.rem(y - i + 8, 8)

    def pass_on(i, rows, n, rsem):
        return remote(
            recv1.at[0, source(i), rows],
            recv1.at[1, source(i), rows],
            snd.at[n],
            rsem,
            patch_1=other,
        )

    def row_block(src, c=0):
        return pl.ds(pl.multiple_of((8 * c + src) * ROWS, ROWS), ROWS)

    def take(src):
        asks = recv1[0, src, HEAD_DIM : 2 * HEAD_DIM + 8, :].astype(F32)
        qf_s[src] = asks.astype(BF)
        keys = recv1[0, src, 0:HEAD_DIM, :].astype(F32)
        keys = jnp.concatenate([keys, MASK + asks[HEAD_DIM:]], axis=0)
        ktok[row_block(src), :] = keys.T.astype(BF)

    def pass_keys(i):
        at = pl.multiple_of(source(i) * ROWS, ROWS)
        return remote(
            ktok.at[pl.ds(at, ROWS)],
            ktok.at[pl.ds(8 * ROWS + at, ROWS)],
            snd.at[16],
            d1r.at[i],
            patch_1=other,
        )

    passed = [pass_on(i, ko, 2, rcv.at[8]) for i in range(8)]
    passed_v = [pass_on(i, mo, 3, rcv.at[9]) for i in range(8)]
    take(y)
    pass_keys(0).start()
    passed[0].start()
    passed_v[0].start()
    for i in NEAR:
        block_in(i, qk, r1)
        take(source(i))
        pass_keys(i).start()
        passed[i].start()

    factor = scale * math.log2(math.e)
    pair = y // 2
    mate = y + 1 - 2 * lax.rem(y, 2)
    half = 8 * ROWS

    def queries(j):
        return jnp.concatenate([qf_s[2 * j], qf_s[2 * j + 1]], axis=1)

    def forward_half(j, c):
        scores = dot(ktok[half * c : half * (c + 1), :], queries(j), 1, 0)
        top = jnp.max(scores, axis=0, keepdims=True)
        p_s[j, half * c : half * (c + 1), :] = jnp.exp2((scores - top) * factor).astype(BF)
        return top

    def forward_own(j, carry):
        top_s[j] = jnp.broadcast_to(forward_half(j, 0), (8, 2 * ROWS))
        return carry

    lax.fori_loop(0, 4, forward_own, 0)
    for i in (0,) + NEAR:
        pass_keys(i).wait_recv()

    def forward_other(j, carry):
        top = forward_half(j, 1)
        mine = top_s[j, 0:1, :]
        best = jnp.maximum(mine, top)
        for c, one in enumerate((mine, top)):
            w_half[c, j] = jnp.broadcast_to(jnp.exp2((one - best) * factor), (8, 2 * ROWS))
        return carry

    lax.fori_loop(0, 4, forward_other, 0)
    for i in NEAR:
        block_in(i, vo, r1v)
        passed_v[i].start()

    def lanes(c, start, end):
        return jnp.concatenate([recv1[c, src, start:end, :] for src in range(8)], axis=1)

    def values(c):
        return lanes(c, 2 * HEAD_DIM, 3 * HEAD_DIM + 8)

    def values_own(j, carry):
        acc_s[j] = dot(values(0), p_s[j, 0:half, :], 1, 0)
        return carry

    lax.fori_loop(0, 4, values_own, 0)
    crossed = recv1.at[1, :, mo]
    remote(crossed, crossed, snd.at[3], rcv.at[9], patch_0=y).wait_recv()

    head = pl.ds(8, HEAD_DIM)

    def send_attn(s):
        return remote(
            send2.at[s, head], recv2.at[y, head], snd.at[4], rcv.at[0], patch_0=s
        )

    for step_at in (2, 1, 3, 0):
        j = lax.rem(pair + step_at, 4)
        mine, yours = w_half[0, j, 0:1, :], w_half[1, j, 0:1, :]
        accum = acc_s[j] * mine + dot(values(1), p_s[j, half : 2 * half, :], 1, 0) * yours
        rinv = -MASK / (accum[0:1, :] + accum[4:5, :])
        w_half[0, j] = jnp.broadcast_to(mine * rinv, (8, 2 * ROWS))
        w_half[1, j] = jnp.broadcast_to(yours * rinv, (8, 2 * ROWS))
        attn = (accum * rinv).astype(BF)
        send2[2 * j] = attn[:, :ROWS]
        send2[2 * j + 1] = attn[:, ROWS:]
        if step_at:
            send_attn(2 * j).start()
            send_attn(2 * j + 1).start()
        else:
            send_attn(mate).start()
    recv2[y] = send2[y]

    def backward_layouts(src, carry):
        for c in range(2):
            vals = recv1[c, src, 2 * HEAD_DIM : 3 * HEAD_DIM + 8, :]
            vtok[row_block(src, c), :] = vals.astype(F32).T.astype(BF)
        qtok[row_block(src), :] = qf_s[src].astype(F32).T.astype(BF)
        return carry

    lax.fori_loop(0, 8, backward_layouts, 0)

    loads[4].wait()
    loads[5].wait()
    seven = pl.ds(0, 7)
    remote(
        send2.at[seven, head], recv2.at[seven, head], snd.at[4], rcv.at[0], patch_0=y
    ).wait_recv()
    for h in range(HEADS):
        at_s[HEAD_DIM * h : HEAD_DIM * (h + 1), :] = recv2[h].astype(F32)[8:]
    attn_t = at_s[...].astype(BF)
    pa_s[0] = attn_t
    swap_a = remote(pa_s.at[0], pa_s.at[1], snd.at[5], rcv.at[1], patch_1=other)
    swap_a.start()
    output = dot(attn_t, w_s[...], 0, 0)
    token = lax.broadcasted_iota(jnp.int32, (ROWS, WIDTH), 0)
    live = p * ROWS + token < length
    error = jnp.where(live, output - t_s[0].astype(F32), 0.0)
    grad_out = (2.0 * error).astype(BF)
    grad_t = (2.0 * error).T.astype(BF)
    part = WIDTH // (2 * nx)
    for zhalf in range(2):
        for xx in range(nx):
            at = (2 * xx + zhalf) * part
            g_s[zhalf, part * xx : part * (xx + 1), :] = grad_t[at : at + part]
    swap_g = remote(g_s.at[other], pg_s, snd.at[7], rcv.at[2], patch_1=other)
    swap_g.start()
    grad_attn = dot(w_s[...], grad_t, 1, 0)
    for h in range(HEADS):
        block = jnp.concatenate(
            [jnp.zeros((8, ROWS), F32), grad_attn[HEAD_DIM * h : HEAD_DIM * (h + 1)]], axis=0
        )
        send3[h] = block.astype(BF)
    for i in FAR:
        to = lax.rem(y + i, 8)
        remote(
            send3.at[to, head], recv3.at[y, head], snd.at[6], r3.at[i], patch_0=to
        ).start()
    recv3[y] = send3[y]

    swap_a.wait_recv()
    swap_g.wait_recv()
    right = jnp.concatenate([pa_s[0], pa_s[1]], axis=1)

    def x_chunk(xx):
        at = pl.ds(pl.multiple_of(part * xx, 16), part)
        chunk = dot(jnp.concatenate([g_s[k, at, :], pg_s[at, :]], axis=1), right, 1, 1)
        rest = jnp.concatenate([chunk[: part // 2, 512:], chunk[part // 2 :, 512:]], axis=1)
        for g in range(4):
            xsend[xx, part * g : part * (g + 1), :] = chunk[:, ROWS * g : ROWS * (g + 1)].astype(BF)
        xsend[xx, 4 * part :, :] = jnp.concatenate([rest, jnp.zeros((8, ROWS), F32)], axis=0).astype(BF)

    lo, hi = pl.ds(0, 336), pl.ds(336, 320)
    up, down, across = lax.rem(x + 1, 4), lax.rem(x + 3, 4), lax.rem(x + 2, 4)
    xring = [
        remote(xsend.at[across, lo], xrel.at[lo], xs.at[0], xr.at[0], dp_0=up),
        remote(xsend.at[across, hi], xrel.at[hi], xs.at[1], xr.at[1], dp_0=down),
        remote(xsend.at[up, hi], xin.at[0, hi], xs.at[2], xr.at[2], dp_0=up),
        remote(xsend.at[down, lo], xin.at[1, lo], xs.at[3], xr.at[3], dp_0=down),
        remote(xacc.at[lo], xin.at[0, lo], xs.at[4], xr.at[4], dp_0=up),
        remote(xacc.at[hi], xin.at[1, hi], xs.at[5], xr.at[5], dp_0=down),
    ]
    x_chunk(across)
    xring[0].start()
    xring[1].start()
    x_chunk(up)
    xring[2].start()
    x_chunk(down)
    xring[3].start()
    x_chunk(x)

    def x_relay():
        for n, (rows, size, to) in enumerate(((0, 336, up), (336, 320, down))):
            xring[n].wait_recv()
            xacc[rows : rows + size, :] = (
                xsend[to, rows : rows + size, :].astype(F32)
                + xrel[rows : rows + size, :].astype(F32)
            ).astype(BF)
            xring[4 + n].start()

    squares = jnp.sum(error * error)
    cell = lax.broadcasted_iota(jnp.int32, (8, ROWS), 1)
    stat_s[0] = jnp.where(
        cell == 0, squares, jnp.where(cell == 1, length.astype(F32), 0.0)
    )

    def stat_send(stage, base, n, me, to):
        for i in range(1, n):
            remote(
                stat_s.at[stage],
                stat_s.at[base + i],
                snd.at[8 + stage],
                rcv.at[3 + stage],
                **to(lax.rem(me + i, n)),
            ).start()

    def stat_all(stage, base, n):
        slots = stat_s.at[pl.ds(base + 1, n - 1)]
        return remote(slots, slots, snd.at[8 + stage], rcv.at[3 + stage], patch_0=y)

    def stat_sum(stage, base, n):
        stat_all(stage, base, n).wait_recv()
        acc = stat_s[stage]
        for i in range(1, n):
            acc = acc + stat_s[base + i]
        return acc

    stat_send(0, 3, 16, p, lambda t: {"patch_0": t // 2, "patch_1": lax.rem(t, 2)})
    crossed = recv1.at[1, :, ko]
    remote(crossed, crossed, snd.at[2], rcv.at[8], patch_0=y).wait_recv()

    def send_grad(s, rows, n):
        return remote(
            send4.at[s, rows], recv4.at[y, rows], snd.at[n], rcv.at[n], patch_0=s
        )

    qo = pl.ds(0, HEAD_DIM)
    kvo = pl.ds(PAD, 2 * HEAD_DIM)

    def third_in(s):
        i = lax.rem(y - s + 8, 8)
        remote(
            send3.at[y, head], recv3.at[s, head], snd.at[6], r3.at[i], patch_0=y
        ).wait_recv()

    x_relay()
    for step_at in (0, 1, 3, 2):
        j = lax.rem(pair + step_at, 4)
        if step_at:
            third_in(2 * j)
            third_in(2 * j + 1)
        else:
            third_in(mate)
        grads = jnp.concatenate([recv3[2 * j], recv3[2 * j + 1]], axis=1).astype(F32)
        attn = jnp.concatenate([send2[2 * j], send2[2 * j + 1]], axis=1).astype(F32)
        at = pl.ds(pl.multiple_of(j * 2 * ROWS, 2 * ROWS), 2 * ROWS)
        for c in range(2):
            folded = grads * w_half[c, j, 0:1, :]
            dtok[c, at, :] = folded.T.astype(BF)
            folded = folded.astype(BF)
            delta = jnp.sum(folded.astype(F32) * attn, axis=0, keepdims=True)
            these = slice(half * c, half * (c + 1))
            dprobs = dot(vtok[these, :], folded, 1, 0)
            ds_s[j, these, :] = (p_s[j, these, :].astype(F32) * (dprobs - delta)).astype(BF)
        keys = jnp.concatenate([lanes(0, 0, HEAD_DIM), lanes(1, 0, HEAD_DIM)], axis=1)
        dq = dot(keys, ds_s[j], 1, 0) * scale
        dq = jnp.concatenate([dq, jnp.zeros((8, 2 * ROWS), F32)], axis=0).astype(BF)
        send4[2 * j, 0:PAD, :] = dq[:, :ROWS]
        send4[2 * j + 1, 0:PAD, :] = dq[:, ROWS:]
        if step_at:
            send_grad(2 * j, qo, 11).start()
            send_grad(2 * j + 1, qo, 11).start()
        else:
            send_grad(mate, qo, 11).start()

    stat_s[1] = stat_sum(0, 3, 16)
    stat_send(1, 19, nx, x, lambda t: {"dp_0": t})

    def crossing(u):
        two = pl.ds(2 * u, 2)
        return remote(dkv.at[two], drecv.at[two], snd.at[13], dkr.at[u], patch_1=other)

    def key_grads(c, u):
        at = pl.ds(pl.multiple_of((8 * c + 2 * u) * ROWS, 2 * ROWS), 2 * ROWS)
        ds_rows = jnp.concatenate([ds_s[j, at, :] for j in range(4)], axis=1)
        p_rows = jnp.concatenate([p_s[j, at, :] for j in range(4)], axis=1)
        dk = (dot(ds_rows, qtok[...], 1, 0) * scale).T
        dv = dot(p_rows, dtok[c], 1, 0).T
        return jnp.concatenate([dk[:HEAD_DIM], dv[8:]], axis=0)

    cols = part // zh
    active = z // zh == k

    def x_done():
        for c in xring[2:]:
            c.wait_recv()
        total = xsend[x].astype(F32) + xin[0].astype(F32) + xin[1].astype(F32)
        for j in range(zh):
            rest = total[4 * part + cols * (j % 2) : 4 * part + cols * (j % 2 + 1)]
            rest = rest[:, 64 * (j // 2) : 64 * (j // 2 + 1)]
            rows = [total[part * g + cols * j : part * g + cols * (j + 1)] for g in range(4)]
            rows += [
                jnp.concatenate([rest[: cols // 2], rest[cols // 2 :]], axis=1),
                jnp.zeros((14, ROWS), F32),
            ]
            zsend[j] = jnp.concatenate(rows, axis=0).astype(BF)
        start = z + jnp.where(active, 2, 0)
        for step_at in (0, 1, 3, 2):
            j = lax.rem(start + step_at, zh)
            to = zh * k + j
            away = lax.rem(to - z + nz, nz)

            @pl.when(to != z)
            def _():
                remote(
                    zsend.at[j], zrecv.at[away], snd.at[14], rcv.at[6], dp_1=to
                ).start()

        @pl.when(active)
        def _():
            zrecv[0] = zsend[lax.rem(z, zh)]

    def other_keys(step_at):
        u = lax.rem(pair + step_at, 4)
        both = key_grads(1, u).astype(BF)
        dkv[2 * u] = both[:, :ROWS]
        dkv[2 * u + 1] = both[:, ROWS:]
        crossing(u).start()

    def own_keys(step_at):
        u = lax.rem(pair + step_at, 4)
        both = key_grads(0, u)
        crossing(u).wait_recv()
        for c in range(2):
            mine = both[:, ROWS * c : ROWS * (c + 1)]
            send4[2 * u + c, PAD:, :] = (mine + drecv[2 * u + c].astype(F32)).astype(BF)
        if step_at:
            send_grad(2 * u, kvo, 12).start()
            send_grad(2 * u + 1, kvo, 12).start()
        else:
            send_grad(mate, kvo, 12).start()

    x_done()
    other_keys(2)
    other_keys(1)
    own_keys(2)
    stat_s[2] = stat_sum(1, 19, nx)
    stat_send(2, 19 + nx, nz, z, lambda t: {"dp_1": t})
    other_keys(3)
    own_keys(1)
    other_keys(0)
    own_keys(3)
    own_keys(0)

    recv4[y] = send4[y]

    @pl.when(active)
    def _():
        z_all = zrecv.at[pl.ds(1, nz - 1)]
        remote(z_all, z_all, snd.at[14], rcv.at[6], patch_0=y).wait_recv()
        summed = zrecv[0].astype(F32)
        for i in range(1, nz):
            summed = summed + zrecv[i].astype(F32)
        rest = summed[4 * cols : 4 * cols + cols // 2]
        summed = jnp.concatenate(
            [summed[cols * g : cols * (g + 1)] for g in range(4)]
            + [jnp.concatenate([rest[:, :64], rest[:, 64:]], axis=0)],
            axis=1,
        )
        summed = jnp.concatenate([summed, jnp.zeros((48 - cols, FEAT), F32)], axis=0)
        for t in range(16):
            piece = summed[:, 36 * t : 36 * (t + 1)]
            ysend[t, :, 0:108] = jnp.concatenate(
                [piece[0:16], piece[16:32], piece[32:48]], axis=1
            )

    @pl.when(active)
    def _():
        for i in FAR + (0,):
            for c in range(2):
                if i == 0 and c == 1:
                    continue
                to = lax.rem(y + i, 8)
                core = c if i else other
                remote(
                    ysend.at[2 * to + core],
                    yrecv.at[y],
                    snd.at[15],
                    rcv.at[7],
                    patch_0=to,
                    patch_1=core,
                ).start()

    @pl.when(active)
    def _():
        yrecv[y] = ysend[p]

    acc = stat_sum(2, 19 + nx, nz)
    count = acc[0:1, 1:2] / 16.0
    ratio = (nx * nz * 16.0 * ROWS) / count
    st_out[...] = acc[0:1, 0:1] / (count * WIDTH)

    def grad_all(rows, n):
        blocks = recv4.at[seven, rows]
        return remote(blocks, blocks, snd.at[n], rcv.at[n], patch_0=y)

    def emit(start, out):
        rows = slice(start // 16 * 16, (start // 16 + 5) * 16)
        skip = start % 16
        whole = jnp.concatenate(
            [recv4[h, rows, :].astype(F32)[skip : skip + HEAD_DIM] for h in range(HEADS)],
            axis=0,
        )
        out[0] = whole * ratio

    grad_all(qo, 11).wait_recv()
    emit(0, dq_out)
    grad_all(kvo, 12).wait_recv()
    emit(PAD, dk_out)
    emit(PAD + HEAD_DIM, dv_out)

    def y_all(n):
        blocks = yrecv.at[pl.ds(0, n)]
        return remote(blocks, blocks, snd.at[15], rcv.at[7], patch_0=y)

    @pl.when(active)
    def _():
        y_all(7).wait_recv()

    @pl.when(jnp.logical_not(active))
    def _():
        y_all(8).wait_recv()

    final = yrecv[0]
    for i in range(1, 8):
        final = final + yrecv[i]
    final = jnp.concatenate([final[:, 0:36], final[:, 36:72], final[:, 72:108]], axis=0)
    wg_out[...] = final.T[0:36, 0:36] * (ratio / (16.0 * ROWS))

    def drain(ref, n):
        remote(ref, ref, snd.at[n], rcv.at[0], patch_0=y).wait_send()

    drain(send1.at[seven, qk], 0)
    drain(send1.at[seven, vo], 1)
    drain(send1.at[:, ko], 2)
    drain(ktok.at[pl.ds(0, 8 * ROWS)], 16)
    drain(send1.at[:, mo], 3)
    drain(send2.at[seven, head], 4)
    drain(pa_s.at[0], 5)
    drain(send3.at[seven, head], 6)
    drain(pg_s, 7)
    stat_all(0, 3, 16).wait_send()
    stat_all(1, 19, nx).wait_send()
    stat_all(2, 19 + nx, nz).wait_send()
    drain(send4.at[seven, qo], 11)
    drain(send4.at[seven, kvo], 12)
    drain(drecv, 13)
    for c in xring:
        c.wait_send()

    @pl.when(active)
    def _():
        drain(zsend.at[pl.ds(0, zh - 1)], 14)
        drain(ysend.at[pl.ds(0, 15)], 15)

    @pl.when(jnp.logical_not(active))
    def _():
        drain(zsend, 14)


def write_out(*refs):
    n = len(refs) // 2
    copies = [
        pltpu.make_async_copy(refs[i], refs[n + i], refs[-1].at[i]) for i in range(n)
    ]
    for c in copies:
        c.start()
    for c in copies:
        c.wait()


def step(nx, nz, query_rows, key_rows, value_rows, out_weight, target, lengths, segments):
    part = WIDTH // (2 * nx)
    zh = nz // 2
    dma = pltpu.SemaphoreType.DMA
    scratch = [
        pltpu.VMEM((1, FEAT, ROWS), BF),
        pltpu.VMEM((1, FEAT, ROWS), BF),
        pltpu.VMEM((1, FEAT, ROWS), BF),
        pltpu.VMEM((1, ROWS), jnp.int32),
        pltpu.VMEM((FEAT, WIDTH), BF),
        pltpu.VMEM((1, ROWS, WIDTH), BF),
        pltpu.VMEM((8, 3 * HEAD_DIM + 8, ROWS), BF),
        pltpu.VMEM((2, 8, 3 * HEAD_DIM + 8, ROWS), BF),
        pltpu.VMEM((2048, PAD), BF),
        pltpu.VMEM((2048, PAD), BF),
        pltpu.VMEM((1024, PAD), BF),
        pltpu.VMEM((2, 1024, PAD), BF),
        pltpu.VMEM((4, 2048, 256), BF),
        pltpu.VMEM((4, 2048, 256), BF),
        pltpu.VMEM((2, 4, 8, 256), F32),
        pltpu.VMEM((8, PAD, ROWS), BF),
        pltpu.VMEM((8, PAD, ROWS), BF),
        pltpu.VMEM((FEAT, ROWS), F32),
        pltpu.VMEM((8, PAD, ROWS), BF),
        pltpu.VMEM((8, PAD, ROWS), BF),
        pltpu.VMEM((8, 2 * HEAD_DIM, ROWS), BF),
        pltpu.VMEM((8, 2 * HEAD_DIM, ROWS), BF),
        pltpu.VMEM((8, PAD + 2 * HEAD_DIM, ROWS), BF),
        pltpu.VMEM((8, PAD + 2 * HEAD_DIM, ROWS), BF),
        pltpu.VMEM((2, FEAT, ROWS), BF),
        pltpu.VMEM((FEAT, ROWS), BF),
        pltpu.VMEM((2, FEAT, ROWS), BF),
        pltpu.VMEM((nx, 656, ROWS), BF),
        pltpu.VMEM((656, ROWS), BF),
        pltpu.VMEM((656, ROWS), BF),
        pltpu.VMEM((2, 656, ROWS), BF),
        pltpu.VMEM((zh, 176, ROWS), BF),
        pltpu.VMEM((nz, 176, ROWS), BF),
        pltpu.VMEM((16, 16, 128), F32),
        pltpu.VMEM((8, 16, 128), F32),
        pltpu.VMEM((19 + nx + nz, 8, ROWS), F32),
        pltpu.VMEM((8, PAD, ROWS), BF),
        pltpu.VMEM((4, 8, 256), F32),
        pltpu.VMEM((4, PAD, 256), F32),
    ]
    sems = [6, 17, 13, 8, 8, 8, 8, 4, 6, 6]
    vmem = pl.BlockSpec(memory_space=pltpu.VMEM)
    hbm = pl.BlockSpec(memory_space=pltpu.HBM)
    wide = jax.ShapeDtypeStruct((1, FEAT, ROWS), F32)
    results = (
        wide,
        wide,
        wide,
        jax.ShapeDtypeStruct((36, 36), F32),
        jax.ShapeDtypeStruct((1, 1), F32),
    )
    far = lambda a: pltpu.with_memory_space_constraint(a, pltpu.HBM)
    grads = pl.pallas_call(
        functools.partial(body, nx, nz),
        out_shape=results,
        in_specs=[hbm] * 4 + [pl.BlockSpec(memory_space=pltpu.SMEM), hbm, hbm],
        out_specs=(vmem,) * 5,
        scratch_shapes=scratch + [dma((n,)) for n in sems],
        compiler_params=pltpu.CompilerParams(
            collective_id=0, has_side_effects=True, vmem_limit_bytes=40 * 1024 * 1024
        ),
    )(
        far(jnp.swapaxes(query_rows, 1, 2)),
        far(jnp.swapaxes(key_rows, 1, 2)),
        far(jnp.swapaxes(value_rows, 1, 2)),
        far(segments),
        lengths,
        far(out_weight),
        far(target),
    )
    dq, dk, dv, wg, st = pl.pallas_call(
        write_out,
        out_shape=results,
        in_specs=[pl.BlockSpec(memory_space=pl.ANY)] * 5,
        out_specs=(hbm,) * 5,
        scratch_shapes=[dma((5,))],
        compiler_params=pltpu.CompilerParams(vmem_limit_bytes=2 * 1024 * 1024),
    )(*grads)
    return (
        jnp.swapaxes(dq, 1, 2),
        jnp.swapaxes(dk, 1, 2),
        jnp.swapaxes(dv, 1, 2),
        wg,
        st[0, 0],
    )


def solution(mesh):
    torus = Mesh(mesh.devices.reshape(4, 8, 8, 2), ("dp_0", "dp_1", "patch_0", "patch_1"))
    return jax.shard_map(
        functools.partial(step, 4, 8),
        mesh=torus,
        in_specs=(
            P(DP, PATCH, None),
            P(DP, PATCH, None),
            P(DP, PATCH, None),
            P(),
            P(DP, PATCH, None),
            P(DP),
            P(DP, PATCH),
        ),
        out_specs=(P(DP, PATCH, None), P(DP, PATCH, None), P(DP, PATCH, None), P(PATCH, DP), P()),
        check_vma=False,
    )
```
